32 devices in a mesh: dp: 4 (over y, z), tp: 8 (over x, core).
Axes of the slice: x: 4, y: 2, z: 2, core: 2. Of those that a mesh axis runs over, the one named last changes fastest.
The devices are a block of a 4x4x8 slice.
Arguments:
- hidden: bfloat16 [8192, 2048], P(('dp', 'tp')), parts along dimension 0
- w_two: bfloat16 [2048, 2048], replicated
- ln_scale: float32 [2, 2048], replicated
- ln_shift: float32 [2, 2048], replicated
- embed: bfloat16 [32768, 2048], P('tp')
- targets: int32 [2, 8192], P(None, ('dp', 'tp')), parts along dimension 1
- loss_mask: int32 [2, 8192], P(None, ('dp', 'tp')), parts along dimension 1
Outputs:
- output 1: float32 [2, 8192], P(None, ('dp', 'tp')), parts along dimension 1
- output 2: float32 [4], P('dp'), parts along dimension 0
- output 3: bfloat16 [8192, 2048], P(('dp', 'tp')), parts along dimension 0
- output 4: float32 [131072, 2048], P(('dp', 'tp')), parts along dimension 0
- output 5: float32 [8192, 2048], P('dp'), parts along dimension 0
- output 6: float32 [8, 2048], P('dp'), parts along dimension 0
- output 7: float32 [8, 2048], P('dp'), parts along dimension 0
There are 4 independent parts. The reference program is written for one: setup_inputs(seed, part) draws one part's arguments, and reference() takes and returns one part's arrays. A program takes and returns all parts, laid end to end along the dimension named above; an argument that names none is the same for every part.
All inputs are finite; a program needn't handle non-finite values.
Results may differ from the reference program's by a relative error of at most 0.00168.
Values are sent between devices in bfloat16 or wider.
A program may use at most 768 MiB of HBM per device.

```python
import math
import jax
import jax.numpy as jnp
from jax import lax

TOKENS_DEV = 256
GROUP_SIZE = 8
D_MODEL = 2048
VOCAB_SIZE = 32000
TABLE_ROWS = 32768

TOKENS = TOKENS_DEV * GROUP_SIZE
ROW_BLOCK = math.gcd(TOKENS, 128)
BLOCKS = TOKENS // ROW_BLOCK
LN_EPS = 1e-5


def setup_inputs(seed: int = 0, part: int = 0) -> dict:
    base = jax.random.key(seed)
    k_w, k_g, k_b, k_e = jax.random.split(base, 4)
    part_key = jax.random.fold_in(base, part)
    k_h, k_t, k_m, k_l = jax.random.split(part_key, 4)
    hidden = jax.random.normal(k_h, (TOKENS, D_MODEL), jnp.float32).astype(jnp.bfloat16)
    w_two = (jax.random.normal(k_w, (D_MODEL, D_MODEL), jnp.float32) * D_MODEL ** -0.5).astype(jnp.bfloat16)
    ln_scale = 1.0 + 0.3 * jax.random.normal(k_g, (2, D_MODEL), jnp.float32)
    ln_shift = 0.3 * jax.random.normal(k_b, (2, D_MODEL), jnp.float32)
    embed = (jax.random.normal(k_e, (TABLE_ROWS, D_MODEL), jnp.float32) * (2.5 * D_MODEL ** -0.5)).astype(jnp.bfloat16)
    targets = jax.random.randint(k_t, (2, TOKENS), 0, VOCAB_SIZE, jnp.int32)
    keep_len = jax.random.randint(k_l, (2, GROUP_SIZE, 1), TOKENS_DEV // 4, TOKENS_DEV + 1, jnp.int32)
    keep_draw = jax.random.randint(k_m, (2, GROUP_SIZE, TOKENS_DEV), 0, 8, jnp.int32)
    position = jnp.arange(TOKENS_DEV, dtype=jnp.int32)
    keep = (position < keep_len) & ((keep_draw != 0) | (position == 0))
    loss_mask = keep.astype(jnp.int32).reshape(2, TOKENS)
    return {'hidden': hidden, 'w_two': w_two, 'ln_scale': ln_scale, 'ln_shift': ln_shift,
            'embed': embed, 'targets': targets, 'loss_mask': loss_mask}


def layer_norm(values, gain, bias):
    mean_val = jnp.mean(values, axis=-1, keepdims=True)
    centered = values - mean_val
    variance = jnp.mean(centered * centered, axis=-1, keepdims=True)
    return centered * lax.rsqrt(variance + LN_EPS) * gain + bias


def reference(hidden, w_two, ln_scale, ln_shift, embed, targets, loss_mask):
    proj_out = jnp.dot(hidden, w_two, preferred_element_type=jnp.float32).astype(jnp.bfloat16)
    norm_input = jnp.stack([hidden.astype(jnp.float32), proj_out.astype(jnp.float32)])
    normed, ln_back = jax.vjp(jax.vmap(layer_norm), norm_input, ln_scale, ln_shift)
    x_both = normed.astype(jnp.bfloat16)
    mask_f = loss_mask.astype(jnp.float32)
    token_count = jnp.sum(mask_f, axis=1)
    weight = mask_f / token_count[:, None]
    x_blocks = jnp.swapaxes(x_both.reshape(2, BLOCKS, ROW_BLOCK, D_MODEL), 0, 1)
    t_blocks = jnp.swapaxes(targets.reshape(2, BLOCKS, ROW_BLOCK), 0, 1)
    w_blocks = jnp.swapaxes(weight.reshape(2, BLOCKS, ROW_BLOCK), 0, 1)
    col_ids = jnp.arange(TABLE_ROWS, dtype=jnp.int32)

    def block_step(d_embed, block):
        x_blk, t_blk, w_blk = block
        raw_rows = []
        dx_rows = []
        for head_idx in range(2):
            logits = jnp.dot(x_blk[head_idx], embed.T, preferred_element_type=jnp.float32)
            log_norm = jax.nn.logsumexp(logits, axis=-1)
            is_target = col_ids[None, :] == t_blk[head_idx][:, None]
            tgt_logit = jnp.sum(jnp.where(is_target, logits, 0.0), axis=-1)
            probs_val = jnp.exp(logits - log_norm[:, None])
            d_logits = ((probs_val - is_target.astype(jnp.float32)) * w_blk[head_idx][:, None]).astype(jnp.bfloat16)
            d_embed = d_embed + jnp.dot(d_logits.T, x_blk[head_idx], preferred_element_type=jnp.float32)
            dx_rows.append(jnp.dot(d_logits, embed, preferred_element_type=jnp.float32))
            raw_rows.append(log_norm - tgt_logit)
        return d_embed, (jnp.stack(raw_rows), jnp.stack(dx_rows))

    d_embed, (raw_loss, d_x) = lax.scan(block_step, jnp.zeros((TABLE_ROWS, D_MODEL), jnp.float32),
                                        (x_blocks, t_blocks, w_blocks))
    raw_loss = jnp.swapaxes(raw_loss, 0, 1).reshape(2, TOKENS)
    d_x = jnp.swapaxes(d_x, 0, 1).reshape(2, TOKENS, D_MODEL)
    token_loss = raw_loss * mask_f
    total_loss = jnp.sum(token_loss / token_count[:, None]).reshape(1)
    d_norm_in, d_ln_scale, d_ln_shift = ln_back(d_x)
    d_proj = d_norm_in[1].astype(jnp.bfloat16)
    d_hidden = (d_norm_in[0] + jnp.dot(d_proj, w_two.T, preferred_element_type=jnp.float32)).astype(jnp.bfloat16)
    d_w_two = jnp.dot(hidden.T, d_proj, preferred_element_type=jnp.float32)
    return token_loss, total_loss, d_hidden, d_embed, d_w_two, d_ln_scale, d_ln_shift
```

```python
import functools

import jax
import jax.numpy as jnp
from jax import lax
from jax.experimental import pallas as pl
from jax.experimental.pallas import tpu as pltpu
from jax.sharding import PartitionSpec as P

LN_EPS = 1e-5
CHIPS = 4
BLOCKS = 8
F32 = jnp.float32
BF16 = jnp.bfloat16


def to(idx):
    return dict(device_id={'tp': idx}, device_id_type=pl.DeviceIdType.MESH)


def remote(src, dst, send, recv, idx):
    return pltpu.make_async_remote_copy(src_ref=src, dst_ref=dst, send_sem=send, recv_sem=recv, **to(idx))


def stream_kernel(dims, h_ref, w_ref, gain_ref, bias_ref, e_ref, code_ref,
                  hall_ref, xall_ref, dzt_ref, dgall_ref, da1_ref, dgown_ref, loss_ref, total_ref, dgb_ref,
                  e_v, w_v, a_v, x_v, z_v, dz_v, dx_v, pr_v, mg_v, ow_v, hown_v, a2own_v, dg_v, da_v,
                  stsrc_v, strcv_v, crcv_v, tgt_v, msk_v, wgt_v, ms_v, row_v, tot_v, gsrc_v, grcv_v,
                  ld_sem, h_send, h_recv, h_loc, g_send, g_recv, g_loc,
                  st_send, st_recv, pr_send, pr_recv, r2_send, r3_send, mg_recv, ow_recv, pair_free,
                  cd_send, cd_recv, x_sem, dz_sem, a_sem, out_sem, gb_send, gb_recv):
    n, q, depth, rows, rc, nc = dims
    half = CHIPS * q
    tok = 2 * half
    cols = 2 * tok
    me = lax.axis_index('tp')
    chip = me // 2
    core = me % 2
    peer = me + 1 - 2 * core
    right_chip = (chip + 1) % CHIPS
    left_chip = (chip + CHIPS - 1) % CHIPS
    far_chip = (chip + 2) % CHIPS
    right = right_chip * 2 + core
    left = left_chip * 2 + core

    ld_e = pltpu.make_async_copy(e_ref, e_v, ld_sem.at[0])
    ld_w = pltpu.make_async_copy(w_ref, w_v, ld_sem.at[1])
    ld_h = pltpu.make_async_copy(h_ref, hown_v, ld_sem.at[2])
    ld_h.start()
    ld_w.start()
    ld_e.start()

    barrier = pltpu.get_barrier_semaphore()
    for r in range(1, n):
        pl.semaphore_signal(barrier, inc=1, **to((me + r) % n))
    pl.semaphore_wait(barrier, n - 1)

    def code_copy(r):
        return remote(code_ref, crcv_v.at[r], cd_send.at[r], cd_recv.at[r], (me + r) % n)

    for r in range(1, n):
        code_copy(r).start()

    def g1_copies(src, dst, b, send, recv):
        piece = dst.at[b, core, chip]
        return (remote(src, piece, send.at[b, 0], recv.at[b, 0], right),
                remote(src, piece, send.at[b, 1], recv.at[b, 1], left),
                remote(src, piece, send.at[b, 2], recv.at[b, 4], peer))

    def g2_copies(dst, b, send, recv):
        fl = dst.at[b, core, left_chip]
        fr = dst.at[b, core, right_chip]
        lo, hi = pl.ds(0, q // 2), pl.ds(q // 2, q // 2)
        return (remote(fl.at[lo], fl.at[lo], send.at[b, 3], recv.at[b, 2], right),
                remote(fr.at[hi], fr.at[hi], send.at[b, 4], recv.at[b, 3], left),
                remote(fl, fl, send.at[b, 5], recv.at[b, 5], peer),
                remote(fr, fr, send.at[b, 6], recv.at[b, 6], peer))

    def g3_copies(dst, b, send, recv):
        far = dst.at[b, core, far_chip]
        return (remote(far, far, send.at[b, 7], recv.at[b, 7], peer),)

    def gather1(src, dst, b, send, recv, loc):
        for c in g1_copies(src, dst, b, send, recv):
            c.start()
        pltpu.make_async_copy(src, dst.at[b, core, chip], loc.at[b]).start()

    def gather2(src, dst, b, send, recv, loc):
        c1 = g1_copies(src, dst, b, send, recv)
        remote(src, dst.at[b, core, left_chip], send.at[b, 0], recv.at[b, 0], right).wait_recv()
        remote(src, dst.at[b, core, right_chip], send.at[b, 1], recv.at[b, 1], left).wait_recv()
        for c in g2_copies(dst, b, send, recv):
            c.start()
        for c in c1:
            c.wait_send()
        pltpu.make_async_copy(src, dst.at[b, core, chip], loc.at[b]).wait()

    def gather3(dst, b, send, recv):
        far = dst.at[b, core, far_chip]
        lo, hi = pl.ds(0, q // 2), pl.ds(q // 2, q // 2)
        remote(far.at[lo], far.at[lo], send.at[b, 3], recv.at[b, 2], right).wait_recv()
        remote(far.at[hi], far.at[hi], send.at[b, 4], recv.at[b, 3], left).wait_recv()
        for c in g3_copies(dst, b, send, recv):
            c.start()
        for c in g2_copies(dst, b, send, recv):
            c.wait_send()

    def gather4(dst, b, send, recv):
        for i, c in enumerate((chip, left_chip, right_chip, far_chip)):
            piece = dst.at[b, 1 - core, c]
            remote(piece, piece, send.at[b, 7], recv.at[b, 4 + i], peer).wait_recv()
        for c in g3_copies(dst, b, send, recv):
            c.wait_send()

    def hpiece(b):
        return hown_v.at[pl.ds(b * q, q)]

    def a_copy(b, i, kk):
        return pltpu.make_async_copy(hall_ref.at[b, kk, i], a_v.at[pl.ds((kk * CHIPS + i) * q, q)],
                                     a_sem.at[kk * CHIPS + i])

    def load_block(b):
        gather4(hall_ref, b, h_send, h_recv)
        for kk in range(2):
            for i in range(CHIPS):
                a_copy(b, i, kk).start()
        for kk in range(2):
            for i in range(CHIPS):
                a_copy(b, i, kk).wait()

        def proj(i, _):
            sl = pl.ds(pl.multiple_of(i * nc, nc), nc)
            a_v[tok:, sl] = jnp.dot(a_v[:tok, :], w_v[:, sl], preferred_element_type=F32).astype(BF16)
            return 0
        lax.fori_loop(0, depth // nc, proj, 0)
        a2own_v[b % 4] = a_v[pl.ds(pl.multiple_of(tok + core * half + chip * q, q), q), :]

    def norm_rows(start, head):
        a = a_v[pl.ds(start, 16), :].astype(F32)
        mean = jnp.mean(a, axis=-1, keepdims=True)
        cent = a - mean
        var = jnp.mean(cent * cent, axis=-1, keepdims=True)
        y = cent * lax.rsqrt(var + LN_EPS) * gain_ref[pl.ds(head, 1), :] + bias_ref[pl.ds(head, 1), :]
        x_v[pl.ds(start, 16), :] = y.astype(BF16)

    npart = depth // nc
    lrows = cols // npart

    def norm_part(i):
        head = (i * lrows) // tok
        for s in range(lrows // 16):
            norm_rows(pl.multiple_of(i * lrows + s * 16, 16), head)

    def dx_part(i, slot):
        sl = pl.ds(pl.multiple_of(i * nc, nc), nc)
        val = lax.dot_general(dz_v[...], e_v[:, sl], (((0,), (0,)), ((), ())), preferred_element_type=F32)
        for h in range(2):
            for kk in range(2):
                base = h * tok + kk * half
                dx_v[slot, kk, h, :, sl] = val[base:base + half, :]

    nr = rows // rc

    def z_part(i):
        rsl = pl.ds(pl.multiple_of(i * rc, rc), rc)
        z_v[rsl, :] = lax.dot_general(e_v[rsl, :], x_v[...], (((1,), (1,)), ((), ())), preferred_element_type=F32)

    iota16 = lambda: lax.broadcasted_iota(jnp.int32, (16, cols), 0)

    def back_part(i):
        lse = row_v[0:1, :]
        w = row_v[1:2, :]
        td = tgt_v[pl.ds(8, 1), :] - i * rc - iota16()
        for s in range(rc // 16):
            sl = pl.ds(pl.multiple_of(i * rc + s * 16, 16), 16)
            p = jnp.exp(z_v[sl, :] - lse)
            d = jnp.where(td == s * 16, p - 1.0, p) * w
            dz_v[sl, :] = d.astype(BF16)

    def stat_part(i):
        base = i * rc
        m_old = ms_v[0]
        m = m_old
        for s in range(rc // 8):
            m = jnp.maximum(m, z_v[pl.ds(pl.multiple_of(base + s * 8, 8), 8), :])
        acc = ms_v[1] * jnp.exp(m_old - m)
        tl = ms_v[2]
        td = tgt_v[pl.ds(9, 1), :] - base - lax.broadcasted_iota(jnp.int32, (8, cols), 0)
        for s in range(rc // 8):
            z = z_v[pl.ds(pl.multiple_of(base + s * 8, 8), 8), :]
            acc = acc + jnp.exp(z - m)
            tl = tl + jnp.where(td == s * 8, z, 0.0)
        ms_v[0] = m
        ms_v[1] = acc
        ms_v[2] = tl

    def stat_copy(slot, r):
        return remote(stsrc_v.at[slot], strcv_v.at[slot, r], st_send.at[slot, r], st_recv.at[slot, r], (me + r) % n)

    def send_stats(b):
        slot = b % 2
        m = ms_v[0]
        top = jnp.max(m, axis=0, keepdims=True)
        stsrc_v[slot, 0:1, :] = top
        stsrc_v[slot, 1:2, :] = jnp.sum(ms_v[1] * jnp.exp(m - top), axis=0, keepdims=True)
        stsrc_v[slot, 2:3, :] = jnp.sum(ms_v[2], axis=0, keepdims=True)
        for r in range(1, n):
            stat_copy(slot, r).start()

    def join_stats(b):
        slot = b % 2
        for r in range(1, n):
            stat_copy(slot, r).wait()
        parts = [stsrc_v[slot]] + [strcv_v[slot, r] for r in range(1, n)]
        top = parts[0][0:1]
        for p in parts[1:]:
            top = jnp.maximum(top, p[0:1])
        total = jnp.zeros_like(top)
        hit = jnp.zeros_like(top)
        for p in parts:
            total = total + p[1:2] * jnp.exp(p[0:1] - top)
            hit = hit + p[2:3]
        lse = top + jnp.log(total)
        row_v[0:1, :] = lse
        row_v[1:2, :] = wgt_v[pl.ds(b, 1), :]
        tgt_v[pl.ds(8, 1), :] = tgt_v[pl.ds(b, 1), :]
        loss = (lse - hit) * msk_v[pl.ds(b, 1), :]
        loss_ref[pl.ds(b, 1), :] = loss
        tot_v[0:1, :] = tot_v[0:1, :] + loss / tot_v[1:2, :]

    def pair_copy(b):
        slot = b % 2
        return remote(dx_v.at[slot, 1 - core], pr_v.at[slot], pr_send.at[slot], pr_recv.at[slot], peer)

    def rs1(b):
        @pl.when(b >= 2)
        def _():
            pl.semaphore_wait(pair_free, 1)
        pair_copy(b).start()

    def crow(c):
        return pl.ds(pl.multiple_of(c * q, q), q)

    def r2_copies(b):
        s2, s3 = b % 2, b % 3
        mine = dx_v.at[s2, core]
        return (remote(mine.at[0, crow(far_chip)], mg_v.at[s2, 0], r2_send.at[s2, 0], mg_recv.at[s2, 0], right),
                remote(mine.at[1, crow(far_chip)], mg_v.at[s2, 1], r2_send.at[s2, 1], mg_recv.at[s2, 1], left),
                remote(mine.at[1, crow(right_chip)], ow_v.at[s3, 0, 1], r2_send.at[s2, 2], ow_recv.at[s3, 0, 1], right),
                remote(mine.at[0, crow(left_chip)], ow_v.at[s3, 1, 0], r2_send.at[s2, 3], ow_recv.at[s3, 1, 0], left))

    def rs2(b):
        slot = b % 2
        pair_copy(b).wait()

        def add(i, _):
            h = i // CHIPS
            c = i % CHIPS
            dx_v[slot, core, h, crow(c), :] += pr_v[slot, h, crow(c), :]
            return 0
        lax.fori_loop(0, 2 * CHIPS, add, 0)

        @pl.when(b < BLOCKS - 2)
        def _():
            pl.semaphore_signal(pair_free, inc=1, **to(peer))
        for c in r2_copies(b):
            c.start()

    def r3_copies(b):
        s2, s3 = b % 2, b % 3
        mine = dx_v.at[s2, core]
        return (remote(mine.at[0, crow(right_chip)], ow_v.at[s3, 0, 0], r3_send.at[s2, 0], ow_recv.at[s3, 0, 0], right),
                remote(mine.at[1, crow(left_chip)], ow_v.at[s3, 1, 1], r3_send.at[s2, 1], ow_recv.at[s3, 1, 1], left))

    def rs3(b):
        s2 = b % 2
        c2 = r2_copies(b)
        c2[0].wait_recv()
        c2[1].wait_recv()
        dx_v[s2, core, 0, crow(right_chip), :] += mg_v[s2, 0]
        dx_v[s2, core, 1, crow(left_chip), :] += mg_v[s2, 1]
        for c in r3_copies(b):
            c.start()
        for c in c2:
            c.wait_send()

    def rs4(b):
        s2, s3 = b % 2, b % 3
        c2, c3 = r2_copies(b), r3_copies(b)
        c2[2].wait_recv()
        c2[3].wait_recv()
        c3[0].wait_recv()
        c3[1].wait_recv()

        @pl.when(b >= 1)
        def _():
            out_copies(b - 1)[0].wait()
            out_copies(b - 1)[1].wait()
        for h in range(2):
            dy = dx_v[s2, core, h, crow(chip), :] + ow_v[s3, 0, h] + ow_v[s3, 1, h]
            a = (hown_v[pl.ds(pl.multiple_of(b * q, q), q), :] if h == 0 else a2own_v[b % 4]).astype(F32)
            mean = jnp.mean(a, axis=-1, keepdims=True)
            cent = a - mean
            rstd = lax.rsqrt(jnp.mean(cent * cent, axis=-1, keepdims=True) + LN_EPS)
            xhat = cent * rstd
            gsrc_v[h:h + 1, :] += jnp.sum(dy * xhat, axis=0, keepdims=True)
            gsrc_v[2 + h:3 + h, :] += jnp.sum(dy, axis=0, keepdims=True)
            dxh = dy * gain_ref[h:h + 1, :]
            c1 = jnp.mean(dxh, axis=-1, keepdims=True)
            c2_ = jnp.mean(dxh * xhat, axis=-1, keepdims=True)
            da = rstd * (dxh - c1 - xhat * c2_)
            if h == 0:
                da_v[...] = da
            else:
                dg_v[b % 4] = da.astype(BF16)
        for c in out_copies(b):
            c.start()
        for c in c3:
            c.wait_send()

    def out_copies(b):
        return (pltpu.make_async_copy(da_v, da1_ref.at[b], out_sem.at[0]),
                pltpu.make_async_copy(dg_v.at[b % 4], dgown_ref.at[b], out_sem.at[1]))

    def inside(b, fn):
        @pl.when(jnp.logical_and(b >= 0, b < BLOCKS))
        def _():
            fn(b)

    def between(j, lo, hi, fn):
        @pl.when(jnp.logical_and(j >= lo, j <= hi))
        def _():
            fn()

    def x_copy(b):
        return pltpu.make_async_copy(x_v, xall_ref.at[pl.ds(pl.multiple_of(b * cols, cols), cols)], x_sem)

    def dz_copy(b):
        return pltpu.make_async_copy(dz_v, dzt_ref.at[:, pl.ds(pl.multiple_of(b * cols, cols), cols)], dz_sem)

    def loop(k, fn):
        def body(i, _):
            fn(i)
            return 0
        lax.fori_loop(0, k, body, 0)

    ld_h.wait()
    gather1(hpiece(0), hall_ref, 0, h_send, h_recv, h_loc)
    gather1(hpiece(1), hall_ref, 1, h_send, h_recv, h_loc)
    for r in range(1, n):
        code_copy(r).wait()
    code = code_ref[...]
    for r in range(1, n):
        code = code + crcv_v[r]
    mask = (code >= 65536).astype(jnp.int32)
    tgt_v[0:BLOCKS, :] = code - mask * 65536 - me * rows
    maskf = mask.astype(F32)
    msk_v[...] = maskf
    per_col = jnp.sum(maskf, axis=0, keepdims=True)
    n0 = jnp.sum(per_col[:, :tok], axis=1, keepdims=True)
    n1 = jnp.sum(per_col[:, tok:], axis=1, keepdims=True)
    counts = jnp.concatenate([jnp.broadcast_to(n0, (1, tok)), jnp.broadcast_to(n1, (1, tok))], axis=1)
    wgt_v[...] = maskf / counts
    tot_v[0:1, :] = jnp.zeros((1, cols), F32)
    tot_v[1:2, :] = counts
    gsrc_v[...] = jnp.zeros_like(gsrc_v)
    gather2(hpiece(0), hall_ref, 0, h_send, h_recv, h_loc)
    gather3(hall_ref, 0, h_send, h_recv)
    gather2(hpiece(1), hall_ref, 1, h_send, h_recv, h_loc)
    ld_w.wait()
    load_block(0)
    ld_e.wait()

    def step(t, _):
        j = t - 1
        between(j, 1, BLOCKS, lambda: x_wait(j))

        def full_a():
            def body(i):
                dx_part(i, (j - 1) % 2)
                norm_part(i)
            loop(npart, body)
        between(j, -1, 0, lambda: loop(npart, norm_part))
        between(j, 1, BLOCKS - 2, full_a)
        between(j, BLOCKS - 1, BLOCKS, lambda: loop(npart, lambda i: dx_part(i, (j - 1) % 2)))
        inside(j - 1, rs1)
        between(j, -1, BLOCKS - 2, lambda: x_copy(j + 1).start())
        inside(j - 2, rs3)
        between(j, -1, BLOCKS - 4, lambda: gather1(hpiece(j + 3), hall_ref, j + 3, h_send, h_recv, h_loc))
        between(j, -1, BLOCKS - 3, lambda: gather3(hall_ref, j + 2, h_send, h_recv))
        inside(j - 3, lambda b: gather2(dg_v.at[b % 4], dgall_ref, b, g_send, g_recv, g_loc))
        inside(j, join_stats)
        between(j, 1, BLOCKS, lambda: dz_copy(j - 1).wait())

        def start_stats():
            ms_v[0] = jnp.full((8, cols), -3.0e38, F32)
            ms_v[1] = jnp.zeros((8, cols), F32)
            ms_v[2] = jnp.zeros((8, cols), F32)
            tgt_v[pl.ds(9, 1), :] = tgt_v[pl.ds(j + 1, 1), :]
        between(j, -1, BLOCKS - 2, start_stats)

        def full_d(i):
            back_part(i)
            z_part(i)
            stat_part(i)

        def only_z(i):
            z_part(i)
            stat_part(i)
        between(j, -1, -1, lambda: loop(nr, only_z))
        between(j, 0, BLOCKS - 2, lambda: loop(nr, full_d))
        between(j, BLOCKS - 1, BLOCKS - 1, lambda: loop(nr, back_part))
        between(j, -1, BLOCKS - 2, lambda: send_stats(j + 1))
        inside(j, lambda b: dz_copy(b).start())
        inside(j - 1, rs2)

        def finish(b):
            rs4(b)
            gather1(dg_v.at[b % 4], dgall_ref, b, g_send, g_recv, g_loc)
        inside(j - 2, finish)
        between(j, -1, BLOCKS - 4, lambda: gather2(hpiece(j + 3), hall_ref, j + 3, h_send, h_recv, h_loc))
        inside(j - 3, lambda b: gather3(dgall_ref, b, g_send, g_recv))
        between(j, -1, BLOCKS - 3, lambda: load_block(j + 2))
        return 0

    def x_wait(j):
        @pl.when(j <= BLOCKS - 1)
        def _():
            x_copy(j).wait()

    def first_x(j):
        x_copy(j).wait()

    def step_outer(t, c):
        @pl.when(t == 1)
        def _():
            first_x(0)
        return step(t, c)

    lax.fori_loop(0, BLOCKS + 4, step_outer, 0)

    for b in range(BLOCKS):
        gather4(dgall_ref, b, g_send, g_recv)
    for c in out_copies(BLOCKS - 1):
        c.wait()
    total_ref[...] = jnp.broadcast_to(jnp.sum(tot_v[0:1, :], axis=1, keepdims=True), total_ref.shape)

    def gb_copy(r):
        return remote(gsrc_v, grcv_v.at[r], gb_send.at[r], gb_recv.at[r], (me + r) % n)
    for r in range(1, n):
        gb_copy(r).start()
    for r in range(1, n):
        gb_copy(r).wait()
    acc = gsrc_v[...]
    for r in range(1, n):
        acc = acc + grcv_v[r]
    dgb_ref[...] = acc


def stream(n, hidden, w_two, gain, bias, embed, code):
    tokens, depth = hidden.shape
    rows = embed.shape[0]
    q = tokens // BLOCKS
    half = CHIPS * q
    tok = 2 * half
    cols = 2 * tok
    nc = min(512, depth // 4)
    rc = min(512, rows // 4)
    dims = (n, q, depth, rows, rc, nc)
    any_spec = pl.BlockSpec(memory_space=pl.ANY)
    vmem = pl.BlockSpec(memory_space=pltpu.VMEM)
    dma = pltpu.SemaphoreType.DMA
    sds = jax.ShapeDtypeStruct
    return pl.pallas_call(
        functools.partial(stream_kernel, dims),
        out_shape=(sds((BLOCKS, 2, CHIPS, q, depth), BF16), sds((BLOCKS * cols, depth), BF16),
                   sds((rows, BLOCKS * cols), BF16), sds((BLOCKS, 2, CHIPS, q, depth), BF16),
                   sds((BLOCKS, q, depth), F32), sds((BLOCKS, q, depth), BF16),
                   sds((BLOCKS, cols), F32), sds((8, 128), F32), sds((8, depth), F32)),
        in_specs=[any_spec, any_spec, vmem, vmem, any_spec, vmem],
        out_specs=(any_spec,) * 6 + (vmem,) * 3,
        scratch_shapes=[
            pltpu.VMEM((rows, depth), BF16), pltpu.VMEM((depth, depth), BF16),
            pltpu.VMEM((cols, depth), BF16), pltpu.VMEM((cols, depth), BF16),
            pltpu.VMEM((rows, cols), F32), pltpu.VMEM((rows, cols), BF16),
            pltpu.VMEM((2, 2, 2, half, depth), F32), pltpu.VMEM((2, 2, half, depth), F32),
            pltpu.VMEM((2, 2, q, depth), F32), pltpu.VMEM((3, 2, 2, q, depth), F32),
            pltpu.VMEM((tokens, depth), BF16), pltpu.VMEM((4, q, depth), BF16),
            pltpu.VMEM((4, q, depth), BF16), pltpu.VMEM((q, depth), F32),
            pltpu.VMEM((2, 8, cols), F32), pltpu.VMEM((2, n, 8, cols), F32),
            pltpu.VMEM((n, BLOCKS, cols), jnp.int32), pltpu.VMEM((16, cols), jnp.int32),
            pltpu.VMEM((BLOCKS, cols), F32), pltpu.VMEM((BLOCKS, cols), F32),
            pltpu.VMEM((3, 8, cols), F32), pltpu.VMEM((8, cols), F32), pltpu.VMEM((8, cols), F32),
            pltpu.VMEM((8, depth), F32), pltpu.VMEM((n, 8, depth), F32),
            dma((3,)), dma((BLOCKS, 8)), dma((BLOCKS, 8)), dma((BLOCKS,)), dma((BLOCKS, 8)), dma((BLOCKS, 8)),
            dma((BLOCKS,)), dma((2, n)), dma((2, n)), dma((2,)), dma((2,)), dma((2, 4)), dma((2, 2)),
            dma((2, 2)), dma((3, 2, 2)), pltpu.SemaphoreType.REGULAR,
            dma((n,)), dma((n,)), dma, dma, dma((8,)), dma((2,)), dma((n,)), dma((n,)),
        ],
        compiler_params=pltpu.CompilerParams(collective_id=0, has_side_effects=True, vmem_limit_bytes=67043328),
        name='stream',
    )(hidden, w_two, gain, bias, embed, code)


def solution(mesh):
    n = mesh.shape['tp']
    tok_spec = P(('dp', 'tp'), None)
    row_spec = P(None, ('dp', 'tp'))

    def device_step(hidden, w_two, ln_scale, ln_shift, embed, targets, loss_mask):
        tokens, depth = hidden.shape
        q = tokens // BLOCKS
        me = lax.axis_index('tp')
        code = (targets + 65536 * loss_mask).reshape(2, BLOCKS, q).transpose(1, 0, 2)
        place = (me % 2) * CHIPS + me // 2
        seat = lax.broadcasted_iota(jnp.int32, (1, 1, 2 * CHIPS, 1), 2) == place
        code = jnp.where(seat, code[:, :, None, :], 0).reshape(BLOCKS, 2 * 2 * CHIPS * q)
        hall, xall, dzt, dgall, da1, dgown, loss, total, dgb = stream(n, hidden, w_two, ln_scale, ln_shift, embed, code)
        d_embed = jnp.dot(dzt, xall, preferred_element_type=F32)
        d_w = lax.dot_general(hall.reshape(n * tokens, depth), dgall.reshape(n * tokens, depth),
                              (((0,), (0,)), ((), ())), preferred_element_type=F32)
        d_proj = dgown.reshape(tokens, depth)
        back = lax.dot_general(d_proj, w_two, (((1,), (1,)), ((), ())), preferred_element_type=F32)
        d_hidden = (da1.reshape(tokens, depth) + back).astype(BF16)
        loss = loss.reshape(BLOCKS, 2, 2 * CHIPS, q)
        mine = lax.dynamic_index_in_dim(loss, place, axis=2, keepdims=False)
        token_loss = mine.transpose(1, 0, 2).reshape(2, tokens)
        return token_loss, total[0, :1], d_hidden, d_embed, d_w, dgb[0:2], dgb[2:4]

    return jax.shard_map(device_step, mesh=mesh,
                         in_specs=(tok_spec, P(), P(), P(), P('tp', None), row_spec, row_spec),
                         out_specs=(row_spec, P('dp'), tok_spec, tok_spec, P('dp', None), P('dp', None), P('dp', None)),
                         check_vma=False)
```

```python
import functools

import jax
import jax.numpy as jnp
from jax import lax
from jax.experimental import pallas as pl
from jax.experimental.pallas import tpu as pltpu
from jax.sharding import PartitionSpec as P

LN_EPS = 1e-5
CHIPS = 4
BLOCKS = 8
KEEP = 5
WAYS = 4
LANES = 2
F32 = jnp.float32
BF16 = jnp.bfloat16


def to(idx):
    return dict(device_id={'tp': idx}, device_id_type=pl.DeviceIdType.MESH)


def remote(src, dst, send, recv, idx):
    return pltpu.make_async_remote_copy(src_ref=src, dst_ref=dst, send_sem=send, recv_sem=recv, **to(idx))


def stream_kernel(dims, h_ref, w_ref, gain_ref, bias_ref, e_ref, code_ref,
                  hall_ref, xall_ref, dzt_ref, dgall_ref, da1_ref, dgown_ref, loss_ref, total_ref, dgb_ref, de_ref,
                  e_v, w_v, a_v, x_v, z_v, dz_v, dx_v, pr_v, mg_v, ow_v, hown_v, a2own_v, dg_v, da_v,
                  stsrc_v, strcv_v, crcv_v, tgt_v, msk_v, wgt_v, ms_v, row_v, tot_v, gsrc_v, grcv_v,
                  ld_sem, h_send, h_recv, h_loc, g_send, g_recv, g_loc,
                  st_send, st_recv, pr_send, pr_recv, r2_send, r3_send, mg_recv, ow_recv, pair_free,
                  cd_send, cd_recv, x_sem, dz_sem, a_sem, out_sem, gb_send, gb_recv, xin_sem, dzin_sem, de_sem):
    n, q, depth, rows, rc, nc, sub = dims
    re = rows // BLOCKS
    half = CHIPS * q
    tok = 2 * half
    cols = 2 * tok
    me = lax.axis_index('tp')
    chip = me // 2
    core = me % 2
    peer = me + 1 - 2 * core
    right_chip = (chip + 1) % CHIPS
    left_chip = (chip + CHIPS - 1) % CHIPS
    far_chip = (chip + 2) % CHIPS
    right = right_chip * 2 + core
    left = left_chip * 2 + core

    ld_e = pltpu.make_async_copy(e_ref, e_v, ld_sem.at[0])
    ld_w = pltpu.make_async_copy(w_ref, w_v, ld_sem.at[1])
    ld_h = pltpu.make_async_copy(h_ref, hown_v, ld_sem.at[2])
    ld_h.start()
    ld_w.start()
    ld_e.start()

    barrier = pltpu.get_barrier_semaphore()
    for r in range(1, n):
        pl.semaphore_signal(barrier, inc=1, **to((me + r) % n))
    pl.semaphore_wait(barrier, n - 1)

    def code_copy(r):
        return remote(code_ref, crcv_v.at[r], cd_send.at[r], cd_recv.at[r], (me + r) % n)

    for r in range(1, n):
        code_copy(r).start()

    def g1_copies(src, dst, b, send, recv):
        piece = dst.at[b, core, chip]
        return (remote(src, piece, send.at[b, 0], recv.at[b, 0], right),
                remote(src, piece, send.at[b, 1], recv.at[b, 1], left),
                remote(src, piece, send.at[b, 2], recv.at[b, 4], peer))

    def g2_copies(dst, b, send, recv):
        fl = dst.at[b, core, left_chip]
        fr = dst.at[b, core, right_chip]
        lo, hi = pl.ds(0, q // 2), pl.ds(q // 2, q // 2)
        return (remote(fl.at[lo], fl.at[lo], send.at[b, 3], recv.at[b, 2], right),
                remote(fr.at[hi], fr.at[hi], send.at[b, 4], recv.at[b, 3], left),
                remote(fl, fl, send.at[b, 5], recv.at[b, 5], peer),
                remote(fr, fr, send.at[b, 6], recv.at[b, 6], peer))

    def g3_copies(dst, b, send, recv):
        far = dst.at[b, core, far_chip]
        return (remote(far, far, send.at[b, 7], recv.at[b, 7], peer),)

    def gather1(src, dst, b, send, recv, loc):
        for c in g1_copies(src, dst, b, send, recv):
            c.start()
        pltpu.make_async_copy(src, dst.at[b, core, chip], loc.at[b]).start()

    def gather2(src, dst, b, send, recv, loc):
        c1 = g1_copies(src, dst, b, send, recv)
        remote(src, dst.at[b, core, left_chip], send.at[b, 0], recv.at[b, 0], right).wait_recv()
        remote(src, dst.at[b, core, right_chip], send.at[b, 1], recv.at[b, 1], left).wait_recv()
        for c in g2_copies(dst, b, send, recv):
            c.start()
        for c in c1:
            c.wait_send()
        pltpu.make_async_copy(src, dst.at[b, core, chip], loc.at[b]).wait()

    def gather3(dst, b, send, recv):
        far = dst.at[b, core, far_chip]
        lo, hi = pl.ds(0, q // 2), pl.ds(q // 2, q // 2)
        remote(far.at[lo], far.at[lo], send.at[b, 3], recv.at[b, 2], right).wait_recv()
        remote(far.at[hi], far.at[hi], send.at[b, 4], recv.at[b, 3], left).wait_recv()
        for c in g3_copies(dst, b, send, recv):
            c.start()
        for c in g2_copies(dst, b, send, recv):
            c.wait_send()

    def gather4(dst, b, send, recv):
        for i, c in enumerate((chip, left_chip, right_chip, far_chip)):
            piece = dst.at[b, 1 - core, c]
            remote(piece, piece, send.at[b, 7], recv.at[b, 4 + i], peer).wait_recv()
        for c in g3_copies(dst, b, send, recv):
            c.wait_send()

    def hpiece(b):
        return hown_v.at[pl.ds(b * q, q)]

    def a_copy(b, i, kk):
        return pltpu.make_async_copy(hall_ref.at[b, kk, i], a_v.at[pl.ds((kk * CHIPS + i) * q, q)],
                                     a_sem.at[kk * CHIPS + i])

    def fetch_block(b):
        gather4(hall_ref, b, h_send, h_recv)
        for kk in range(2):
            for i in range(CHIPS):
                a_copy(b, i, kk).start()

    def project_block(b):
        for kk in range(2):
            for i in range(CHIPS):
                a_copy(b, i, kk).wait()

        def proj(i, _):
            sl = pl.ds(pl.multiple_of(i * nc, nc), nc)
            a_v[tok:, sl] = jnp.dot(a_v[:tok, :], w_v[:, sl], preferred_element_type=F32).astype(BF16)
            return 0
        lax.fori_loop(0, depth // nc, proj, 0)
        a2own_v[b % 4] = a_v[pl.ds(pl.multiple_of(tok + core * half + chip * q, q), q), :]

    def norm_rows(start, head):
        a = a_v[pl.ds(start, 16), :].astype(F32)
        mean = jnp.mean(a, axis=-1, keepdims=True)
        cent = a - mean
        var = jnp.mean(cent * cent, axis=-1, keepdims=True)
        y = cent * lax.rsqrt(var + LN_EPS) * gain_ref[pl.ds(head, 1), :] + bias_ref[pl.ds(head, 1), :]
        x_v[pl.ds(start, 16), :] = y.astype(BF16)

    npart = depth // nc
    lrows = cols // npart

    def norm_part(i):
        head = (i * lrows) // tok
        for s in range(lrows // 16):
            norm_rows(pl.multiple_of(i * lrows + s * 16, 16), head)

    def dx_part(i, slot):
        sl = pl.ds(pl.multiple_of(i * nc, nc), nc)
        val = lax.dot_general(dz_v[...], e_v[:, sl], (((0,), (0,)), ((), ())), preferred_element_type=F32)
        for h in range(2):
            for kk in range(2):
                base = h * tok + kk * half
                dx_v[slot, kk, h, :, sl] = val[base:base + half, :]

    nr = rows // rc

    def tree(parts, op):
        while len(parts) > 1:
            parts = [op(a, b) for a, b in zip(parts[::2], parts[1::2])]
        return parts[0]

    def part_view(ref, i):
        return ref.at[pl.ds(pl.multiple_of(i * rc, rc), rc)]

    def back_part(i, p, lanes, td):
        shift, w = row_v[0:1, lanes], row_v[1:2, lanes]
        zc, dc = part_view(z_v, i), part_view(dz_v, i)
        for s in range(p * sub, p * sub + sub, 16):
            both = []
            for t in (s, s + 8):
                pw = jnp.exp(zc[t:t + 8, lanes] - shift)
                both.append(jnp.where(td == t, pw - w, pw))
            dc[s:s + 16, lanes] = jnp.concatenate(both, axis=0).astype(BF16)

    def z_part(i, p):
        ec = part_view(e_v, i)
        part_view(z_v, i)[p * sub:p * sub + sub, :] = lax.dot_general(
            ec[p * sub:p * sub + sub, :], x_v[...], (((1,), (1,)), ((), ())), preferred_element_type=F32)

    def stat_part(i, p, lanes, td, state):
        zc = part_view(z_v, i)
        m_old, acc, tl = state
        at = range(p * sub, p * sub + sub, 8)
        tops = [zc[s:s + 8, lanes] for s in at[:WAYS]]
        for k, s in enumerate(at[WAYS:]):
            tops[k % WAYS] = jnp.maximum(tops[k % WAYS], zc[s:s + 8, lanes])
        m = jnp.maximum(m_old, tree(tops, jnp.maximum))
        accs = [None] * WAYS
        for k, s in enumerate(at):
            z = zc[s:s + 8, lanes]
            e = jnp.exp(z - m)
            accs[k % WAYS] = e if accs[k % WAYS] is None else accs[k % WAYS] + e
            tl = jnp.where(td == s, z, tl)
        return m, acc * jnp.exp(m_old - m) + tree(accs, jnp.add), tl

    def d_body(i, back, new):
        span = cols // LANES
        iota = lax.broadcasted_iota(jnp.int32, (8, span), 0)
        cut = [slice(k * span, k * span + span) for k in range(LANES)]
        td_old = [tgt_v[pl.ds(8, 1), c] - i * rc - iota for c in cut]
        td_new = [tgt_v[pl.ds(9, 1), c] - i * rc - iota for c in cut]
        state = [tuple(ms_v[k, :, c] for k in range(3)) for c in cut]
        for p in range(rc // sub):
            if back:
                for k in range(LANES):
                    back_part(i, p, cut[k], td_old[k])
            if new:
                z_part(i, p)
                for k in range(LANES):
                    state[k] = stat_part(i, p, cut[k], td_new[k], state[k])
        if new:
            for k in range(LANES):
                for q_ in range(3):
                    ms_v[q_, :, cut[k]] = state[k][q_]

    def stat_copy(slot, r):
        return remote(stsrc_v.at[slot], strcv_v.at[slot, r], st_send.at[slot, r], st_recv.at[slot, r], (me + r) % n)

    def send_stats(b):
        slot = b % 2
        m = ms_v[0]
        top = jnp.max(m, axis=0, keepdims=True)
        stsrc_v[slot, 0:1, :] = top
        stsrc_v[slot, 1:2, :] = jnp.sum(ms_v[1] * jnp.exp(m - top), axis=0, keepdims=True)
        stsrc_v[slot, 2:3, :] = jnp.sum(ms_v[2], axis=0, keepdims=True)
        for r in range(1, n):
            stat_copy(slot, r).start()

    def join_stats(b):
        slot = b % 2
        for r in range(1, n):
            stat_copy(slot, r).wait()
        parts = [stsrc_v[slot]] + [strcv_v[slot, r] for r in range(1, n)]
        top = parts[0][0:1]
        for p in parts[1:]:
            top = jnp.maximum(top, p[0:1])
        total = jnp.zeros_like(top)
        hit = jnp.zeros_like(top)
        for p in parts:
            total = total + p[1:2] * jnp.exp(p[0:1] - top)
            hit = hit + p[2:3]
        lse = top + jnp.log(total)
        w = wgt_v[pl.ds(b, 1), :]
        row_v[0:1, :] = jnp.where(w > 0.0, lse - jnp.log(jnp.where(w > 0.0, w, 1.0)), 3.0e38)
        row_v[1:2, :] = w
        tgt_v[pl.ds(8, 1), :] = tgt_v[pl.ds(b, 1), :]
        loss = (lse - hit) * msk_v[pl.ds(b, 1), :]
        loss_ref[pl.ds(b, 1), :] = loss
        tot_v[0:1, :] = tot_v[0:1, :] + loss / tot_v[1:2, :]

    def pair_copy(b):
        slot = b % 2
        return remote(dx_v.at[slot, 1 - core], pr_v.at[slot], pr_send.at[slot], pr_recv.at[slot], peer)

    def rs1(b):
        @pl.when(b >= 2)
        def _():
            pl.semaphore_wait(pair_free, 1)
        pair_copy(b).start()

    def crow(c):
        return pl.ds(pl.multiple_of(c * q, q), q)

    def r2_copies(b):
        s2, s3 = b % 2, b % 3
        mine = dx_v.at[s2, core]
        return (remote(mine.at[0, crow(far_chip)], mg_v.at[s2, 0], r2_send.at[s2, 0], mg_recv.at[s2, 0], right),
                remote(mine.at[1, crow(far_chip)], mg_v.at[s2, 1], r2_send.at[s2, 1], mg_recv.at[s2, 1], left),
                remote(mine.at[1, crow(right_chip)], ow_v.at[s3, 0, 1], r2_send.at[s2, 2], ow_recv.at[s3, 0, 1], right),
                remote(mine.at[0, crow(left_chip)], ow_v.at[s3, 1, 0], r2_send.at[s2, 3], ow_recv.at[s3, 1, 0], left))

    def rs2(b):
        slot = b % 2
        pair_copy(b).wait()

        def add(i, _):
            h = i // CHIPS
            c = i % CHIPS
            dx_v[slot, core, h, crow(c), :] += pr_v[slot, h, crow(c), :]
            return 0
        lax.fori_loop(0, 2 * CHIPS, add, 0)

        @pl.when(b < BLOCKS - 2)
        def _():
            pl.semaphore_signal(pair_free, inc=1, **to(peer))
        for c in r2_copies(b):
            c.start()

    def r3_copies(b):
        s2, s3 = b % 2, b % 3
        mine = dx_v.at[s2, core]
        return (remote(mine.at[0, crow(right_chip)], ow_v.at[s3, 0, 0], r3_send.at[s2, 0], ow_recv.at[s3, 0, 0], right),
                remote(mine.at[1, crow(left_chip)], ow_v.at[s3, 1, 1], r3_send.at[s2, 1], ow_recv.at[s3, 1, 1], left))

    def rs3(b):
        s2 = b % 2
        c2 = r2_copies(b)
        c2[0].wait_recv()
        c2[1].wait_recv()
        dx_v[s2, core, 0, crow(right_chip), :] += mg_v[s2, 0]
        dx_v[s2, core, 1, crow(left_chip), :] += mg_v[s2, 1]
        for c in r3_copies(b):
            c.start()

    def rs4(b):
        s2, s3 = b % 2, b % 3
        c2, c3 = r2_copies(b), r3_copies(b)
        c2[2].wait_recv()
        c2[3].wait_recv()
        c3[0].wait_recv()
        c3[1].wait_recv()

        @pl.when(b >= 1)
        def _():
            out_copies(b - 1)[0].wait()
            out_copies(b - 1)[1].wait()
        for h in range(2):
            dy = dx_v[s2, core, h, crow(chip), :] + ow_v[s3, 0, h] + ow_v[s3, 1, h]
            a = (hown_v[pl.ds(pl.multiple_of(b * q, q), q), :] if h == 0 else a2own_v[b % 4]).astype(F32)
            mean = jnp.mean(a, axis=-1, keepdims=True)
            cent = a - mean
            rstd = lax.rsqrt(jnp.mean(cent * cent, axis=-1, keepdims=True) + LN_EPS)
            xhat = cent * rstd
            gsrc_v[h:h + 1, :] += jnp.sum(dy * xhat, axis=0, keepdims=True)
            gsrc_v[2 + h:3 + h, :] += jnp.sum(dy, axis=0, keepdims=True)
            dxh = dy * gain_ref[h:h + 1, :]
            c1 = jnp.mean(dxh, axis=-1, keepdims=True)
            c2_ = jnp.mean(dxh * xhat, axis=-1, keepdims=True)
            da = rstd * (dxh - c1 - xhat * c2_)
            if h == 0:
                da_v[...] = da
            else:
                dg_v[b % 4] = da.astype(BF16)
        for c in out_copies(b):
            c.start()
        for c in c2 + c3:
            c.wait_send()

    def out_copies(b):
        return (pltpu.make_async_copy(da_v, da1_ref.at[b], out_sem.at[0]),
                pltpu.make_async_copy(dg_v.at[b % 4], dgown_ref.at[b], out_sem.at[1]))

    def xin_copy(i):
        sl = pl.ds(pl.multiple_of(i * nc, nc), nc)
        return pltpu.make_async_copy(xall_ref.at[:, sl], e_v.at[:, sl], xin_sem.at[i])

    def dzin_copy(c, hf):
        return pltpu.make_async_copy(
            dzt_ref.at[pl.ds(pl.multiple_of(c * re, re), re), pl.ds(hf * depth, depth)],
            w_v.at[pl.ds(pl.multiple_of((c % 2) * 2 * re + hf * re, re), re)], dzin_sem.at[c % 2, hf])

    def de_copy(c, i):
        return pltpu.make_async_copy(
            z_v.at[pl.ds(pl.multiple_of(i * re, re), re)],
            de_ref.at[pl.ds(pl.multiple_of(c * re, re), re), pl.ds(pl.multiple_of(i * nc, nc), nc)], de_sem.at[i])

    def de_chunk(c):
        for hf in range(2):
            dzin_copy(c, hf).wait()
        base = (c % 2) * 2 * re
        lo = w_v.at[pl.ds(pl.multiple_of(base, re), re)]
        hi = w_v.at[pl.ds(pl.multiple_of(base + re, re), re)]

        def part(i, _):
            sl = pl.ds(pl.multiple_of(i * nc, nc), nc)

            @pl.when(c == 0)
            def _():
                xin_copy(i).wait()

            @pl.when(c >= 1)
            def _():
                de_copy(c - 1, i).wait()
            val = jnp.dot(lo[...], e_v[:depth, sl], preferred_element_type=F32)
            val = val + jnp.dot(hi[...], e_v[depth:, sl], preferred_element_type=F32)
            z_v[pl.ds(pl.multiple_of(i * re, re), re), :] = val
            de_copy(c, i).start()
            return 0
        lax.fori_loop(0, npart, part, 0)

        @pl.when(c + 2 < KEEP)
        def _():
            for hf in range(2):
                dzin_copy(c + 2, hf).start()

    def inside(b, fn):
        @pl.when(jnp.logical_and(b >= 0, b < BLOCKS))
        def _():
            fn(b)

    def between(j, lo, hi, fn):
        @pl.when(jnp.logical_and(j >= lo, j <= hi))
        def _():
            fn()

    def x_copy(b):
        return pltpu.make_async_copy(x_v, xall_ref.at[pl.ds(pl.multiple_of(b * cols, cols), cols)], x_sem)

    def dz_copy(b):
        return pltpu.make_async_copy(dz_v, dzt_ref.at[:, pl.ds(pl.multiple_of(b * cols, cols), cols)], dz_sem)

    def loop(k, fn):
        def body(i, _):
            fn(i)
            return 0
        lax.fori_loop(0, k, body, 0)

    ld_h.wait()
    gather1(hpiece(0), hall_ref, 0, h_send, h_recv, h_loc)
    gather1(hpiece(1), hall_ref, 1, h_send, h_recv, h_loc)
    for r in range(1, n):
        code_copy(r).wait()
    code = code_ref[...]
    for r in range(1, n):
        code = code + crcv_v[r]
    mask = (code >= 65536).astype(jnp.int32)
    local = code - mask * 65536 - me * rows
    tgt_v[0:BLOCKS, :] = jnp.where(jnp.logical_and(local >= 0, local < rows), local, -(1 << 24))
    maskf = mask.astype(F32)
    msk_v[...] = maskf
    per_col = jnp.sum(maskf, axis=0, keepdims=True)
    n0 = jnp.sum(per_col[:, :tok], axis=1, keepdims=True)
    n1 = jnp.sum(per_col[:, tok:], axis=1, keepdims=True)
    counts = jnp.concatenate([jnp.broadcast_to(n0, (1, tok)), jnp.broadcast_to(n1, (1, tok))], axis=1)
    wgt_v[...] = maskf / counts
    tot_v[0:1, :] = jnp.zeros((1, cols), F32)
    tot_v[1:2, :] = counts
    gsrc_v[...] = jnp.zeros_like(gsrc_v)
    gather2(hpiece(0), hall_ref, 0, h_send, h_recv, h_loc)
    gather3(hall_ref, 0, h_send, h_recv)
    gather2(hpiece(1), hall_ref, 1, h_send, h_recv, h_loc)
    ld_w.wait()
    fetch_block(0)
    project_block(0)
    ld_e.wait()

    def step(t, _):
        j = t - 1
        between(j, 1, BLOCKS, lambda: x_wait(j))

        def full_a():
            def body(i):
                dx_part(i, (j - 1) % 2)
                norm_part(i)
            loop(npart, body)
        between(j, -1, 0, lambda: loop(npart, norm_part))
        between(j, 1, BLOCKS - 2, full_a)
        between(j, BLOCKS, BLOCKS, start_tail)

        def last_a(i):
            dx_part(i, (j - 1) % 2)

            @pl.when(j == BLOCKS)
            def _():
                xin_copy(i).start()
        between(j, BLOCKS - 1, BLOCKS, lambda: loop(npart, last_a))
        between(j, BLOCKS + 1, BLOCKS + 2, lambda: de_chunk(2 * (j - BLOCKS) - 1))
        inside(j - 1, rs1)
        between(j, -1, BLOCKS - 2, lambda: x_copy(j + 1).start())
        inside(j - 2, rs3)
        between(j, -1, BLOCKS - 4, lambda: gather1(hpiece(j + 3), hall_ref, j + 3, h_send, h_recv, h_loc))
        between(j, -1, BLOCKS - 3, lambda: gather3(hall_ref, j + 2, h_send, h_recv))
        inside(j - 3, lambda b: gather2(dg_v.at[b % 4], dgall_ref, b, g_send, g_recv, g_loc))
        between(j, BLOCKS + 2, BLOCKS + 2, gb_start)
        inside(j, join_stats)
        between(j, 1, BLOCKS - 1, lambda: dz_copy(j - 1).wait())
        between(j, BLOCKS, BLOCKS + 2, lambda: de_chunk(2 * (j - BLOCKS)))

        def start_stats():
            ms_v[0] = jnp.full((8, cols), -3.0e38, F32)
            ms_v[1] = jnp.zeros((8, cols), F32)
            ms_v[2] = jnp.zeros((8, cols), F32)
            tgt_v[pl.ds(9, 1), :] = tgt_v[pl.ds(j + 1, 1), :]
        between(j, -1, BLOCKS - 2, start_stats)

        between(j, -1, -1, lambda: loop(nr, lambda i: d_body(i, False, True)))
        between(j, 0, BLOCKS - 2, lambda: loop(nr, lambda i: d_body(i, True, True)))
        between(j, BLOCKS - 1, BLOCKS - 1, lambda: loop(nr, lambda i: d_body(i, True, False)))
        between(j, -1, BLOCKS - 2, lambda: send_stats(j + 1))
        between(j, -1, BLOCKS - 3, lambda: fetch_block(j + 2))
        inside(j, lambda b: dz_copy(b).start())
        inside(j - 1, rs2)

        def finish(b):
            rs4(b)
            gather1(dg_v.at[b % 4], dgall_ref, b, g_send, g_recv, g_loc)
        inside(j - 2, finish)
        between(j, -1, BLOCKS - 4, lambda: gather2(hpiece(j + 3), hall_ref, j + 3, h_send, h_recv, h_loc))
        inside(j - 3, lambda b: gather3(dgall_ref, b, g_send, g_recv))
        between(j, -1, BLOCKS - 3, lambda: project_block(j + 2))
        return 0

    def gb_copy(r):
        return remote(gsrc_v, grcv_v.at[r], gb_send.at[r], gb_recv.at[r], (me + r) % n)

    def gb_start():
        for r in range(1, n):
            gb_copy(r).start()

    def start_tail():
        dz_copy(BLOCKS - 1).wait()
        for c in range(2):
            for hf in range(2):
                dzin_copy(c, hf).start()

    def x_wait(j):
        @pl.when(j <= BLOCKS - 1)
        def _():
            x_copy(j).wait()

    def first_x(j):
        x_copy(j).wait()

    def step_outer(t, c):
        @pl.when(t == 1)
        def _():
            first_x(0)
        return step(t, c)

    lax.fori_loop(0, BLOCKS + 4, step_outer, 0)

    for b in range(BLOCKS):
        gather4(dgall_ref, b, g_send, g_recv)
    for c in out_copies(BLOCKS - 1):
        c.wait()
    total_ref[...] = jnp.broadcast_to(jnp.sum(tot_v[0:1, :], axis=1, keepdims=True), total_ref.shape)

    for i in range(npart):
        de_copy(KEEP - 1, i).wait()
    for r in range(1, n):
        gb_copy(r).wait()
    acc = gsrc_v[...]
    for r in range(1, n):
        acc = acc + grcv_v[r]
    dgb_ref[...] = acc


def stream(n, hidden, w_two, gain, bias, embed, code):
    tokens, depth = hidden.shape
    rows = embed.shape[0]
    q = tokens // BLOCKS
    half = CHIPS * q
    tok = 2 * half
    cols = 2 * tok
    nc = depth // 4
    rc, sub = rows // 2, rows // 8
    assert BLOCKS * cols == rows == 2 * depth and nc == cols
    dims = (n, q, depth, rows, rc, nc, sub)
    any_spec = pl.BlockSpec(memory_space=pl.ANY)
    vmem = pl.BlockSpec(memory_space=pltpu.VMEM)
    dma = pltpu.SemaphoreType.DMA
    sds = jax.ShapeDtypeStruct
    return pl.pallas_call(
        functools.partial(stream_kernel, dims),
        out_shape=(sds((BLOCKS, 2, CHIPS, q, depth), BF16), sds((BLOCKS * cols, depth), BF16),
                   sds((rows, BLOCKS * cols), BF16), sds((BLOCKS, 2, CHIPS, q, depth), BF16),
                   sds((BLOCKS, q, depth), F32), sds((BLOCKS, q, depth), BF16),
                   sds((BLOCKS, cols), F32), sds((8, 128), F32), sds((8, depth), F32),
                   sds((KEEP * (rows // BLOCKS), depth), F32)),
        in_specs=[any_spec, any_spec, vmem, vmem, any_spec, vmem],
        out_specs=(any_spec,) * 6 + (vmem,) * 3 + (any_spec,),
        scratch_shapes=[
            pltpu.VMEM((rows, depth), BF16), pltpu.VMEM((depth, depth), BF16),
            pltpu.VMEM((cols, depth), BF16), pltpu.VMEM((cols, depth), BF16),
            pltpu.VMEM((rows, cols), F32), pltpu.VMEM((rows, cols), BF16),
            pltpu.VMEM((2, 2, 2, half, depth), F32), pltpu.VMEM((2, 2, half, depth), F32),
            pltpu.VMEM((2, 2, q, depth), F32), pltpu.VMEM((3, 2, 2, q, depth), F32),
            pltpu.VMEM((tokens, depth), BF16), pltpu.VMEM((4, q, depth), BF16),
            pltpu.VMEM((4, q, depth), BF16), pltpu.VMEM((q, depth), F32),
            pltpu.VMEM((2, 8, cols), F32), pltpu.VMEM((2, n, 8, cols), F32),
            pltpu.VMEM((n, BLOCKS, cols), jnp.int32), pltpu.VMEM((16, cols), jnp.int32),
            pltpu.VMEM((BLOCKS, cols), F32), pltpu.VMEM((BLOCKS, cols), F32),
            pltpu.VMEM((3, 8, cols), F32), pltpu.VMEM((8, cols), F32), pltpu.VMEM((8, cols), F32),
            pltpu.VMEM((8, depth), F32), pltpu.VMEM((n, 8, depth), F32),
            dma((3,)), dma((BLOCKS, 8)), dma((BLOCKS, 8)), dma((BLOCKS,)), dma((BLOCKS, 8)), dma((BLOCKS, 8)),
            dma((BLOCKS,)), dma((2, n)), dma((2, n)), dma((2,)), dma((2,)), dma((2, 4)), dma((2, 2)),
            dma((2, 2)), dma((3, 2, 2)), pltpu.SemaphoreType.REGULAR,
            dma((n,)), dma((n,)), dma, dma, dma((8,)), dma((2,)), dma((n,)), dma((n,)),
            dma((depth // nc,)), dma((2, 2)), dma((depth // nc,)),
        ],
        compiler_params=pltpu.CompilerParams(collective_id=0, has_side_effects=True, vmem_limit_bytes=67043328),
        name='stream',
    )(hidden, w_two, gain, bias, embed, code)


def dense_kernel(part_ref, dz_ref, x_ref, h_ref, g_ref, da_ref, go_ref, w_ref, de_ref, dw_ref, dh_ref, x_v, x_sem):
    i = pl.program_id(0)
    depth = x_v.shape[1]
    nc = depth // 4
    load = pltpu.make_async_copy(x_ref, x_v, x_sem)

    @pl.when(i == 0)
    def _():
        load.start()

    @pl.when(i < KEEP)
    def _():
        de_ref[...] = part_ref[...]

    @pl.when(i == KEEP)
    def _():
        load.wait()

    @pl.when(i >= KEEP)
    def _():
        def part(p, _):
            sl = pl.ds(pl.multiple_of(p * nc, nc), nc)
            de_ref[:, sl] = jnp.dot(dz_ref[...], x_v[:, sl], preferred_element_type=F32)
            return 0
        lax.fori_loop(0, 4, part, 0)
    dw_ref[...] = lax.dot_general(h_ref[...], g_ref[...], (((0,), (0,)), ((), ())), preferred_element_type=F32)
    back = lax.dot_general(go_ref[...], w_ref[...], (((1,), (1,)), ((), ())), preferred_element_type=F32)
    dh_ref[...] = (da_ref[...] + back).astype(BF16)


def dense(part, dzt, xall, hall, dgall, da1, dgown, w_two):
    rows, kk = dzt.shape
    depth = xall.shape[1]
    total, tokens = hall.shape[0], da1.shape[0]
    re, wb = rows // BLOCKS, depth // BLOCKS
    sds = jax.ShapeDtypeStruct
    one = pl.Buffered(buffer_count=1)
    return pl.pallas_call(
        dense_kernel,
        grid=(BLOCKS,),
        out_shape=(sds((rows, depth), F32), sds((depth, depth), F32), sds((tokens, depth), BF16)),
        in_specs=[pl.BlockSpec((re, depth), lambda i: (jnp.minimum(i, KEEP - 1), 0)),
                  pl.BlockSpec((re, kk), lambda i: (jnp.maximum(i, KEEP), 0)),
                  pl.BlockSpec(memory_space=pl.ANY),
                  pl.BlockSpec((total, wb), lambda i: (0, i)),
                  pl.BlockSpec((total, depth), lambda i: (0, 0), pipeline_mode=one),
                  pl.BlockSpec((tokens, wb), lambda i: (0, i)),
                  pl.BlockSpec((tokens, depth), lambda i: (0, 0), pipeline_mode=one),
                  pl.BlockSpec((wb, depth), lambda i: (i, 0))],
        out_specs=(pl.BlockSpec((re, depth), lambda i: (i, 0)), pl.BlockSpec((wb, depth), lambda i: (i, 0)),
                   pl.BlockSpec((tokens, wb), lambda i: (0, i))),
        scratch_shapes=[pltpu.VMEM((kk, depth), BF16), pltpu.SemaphoreType.DMA],
        compiler_params=pltpu.CompilerParams(vmem_limit_bytes=67043328),
        name='dense',
    )(part, dzt, xall, hall, dgall, da1, dgown, w_two)


def solution(mesh):
    n = mesh.shape['tp']
    tok_spec = P(('dp', 'tp'), None)
    row_spec = P(None, ('dp', 'tp'))

    def device_step(hidden, w_two, ln_scale, ln_shift, embed, targets, loss_mask):
        tokens, depth = hidden.shape
        q = tokens // BLOCKS
        me = lax.axis_index('tp')
        code = (targets + 65536 * loss_mask).reshape(2, BLOCKS, q).transpose(1, 0, 2)
        place = (me % 2) * CHIPS + me // 2
        seat = lax.broadcasted_iota(jnp.int32, (1, 1, 2 * CHIPS, 1), 2) == place
        code = jnp.where(seat, code[:, :, None, :], 0).reshape(BLOCKS, 2 * 2 * CHIPS * q)
        hall, xall, dzt, dgall, da1, dgown, loss, total, dgb, part = stream(
            n, hidden, w_two, ln_scale, ln_shift, embed, code)
        d_embed, d_w, d_hidden = dense(part, dzt, xall, hall.reshape(n * tokens, depth), dgall.reshape(n * tokens, depth),
                                       da1.reshape(tokens, depth), dgown.reshape(tokens, depth), w_two)
        loss = loss.reshape(BLOCKS, 2, 2 * CHIPS, q)
        mine = lax.dynamic_index_in_dim(loss, place, axis=2, keepdims=False)
        token_loss = mine.transpose(1, 0, 2).reshape(2, tokens)
        return token_loss, total[0, :1], d_hidden, d_embed, d_w, dgb[0:2], dgb[2:4]

    return jax.shard_map(device_step, mesh=mesh,
                         in_specs=(tok_spec, P(), P(), P(), P('tp', None), row_spec, row_spec),
                         out_specs=(row_spec, P('dp'), tok_spec, tok_spec, P('dp', None), P('dp', None), P('dp', None)),
                         check_vma=False)
```

```python
import functools

import jax
import jax.numpy as jnp
from jax import lax
from jax.experimental import pallas as pl
from jax.experimental.pallas import tpu as pltpu
from jax.sharding import PartitionSpec as P

LN_EPS = 1e-5
CHIPS = 4
BLOCKS = 8
KEEP = 5
WAYS = 4
LANES = 2
F32 = jnp.float32
BF16 = jnp.bfloat16


def to(idx):
    return dict(device_id={'tp': idx}, device_id_type=pl.DeviceIdType.MESH)


def remote(src, dst, send, recv, idx):
    return pltpu.make_async_remote_copy(src_ref=src, dst_ref=dst, send_sem=send, recv_sem=recv, **to(idx))


def stream_kernel(dims, h_ref, w_ref, gain_ref, bias_ref, e_ref, code_ref,
                  aall_ref, xall_ref, dzt_ref, dgall_ref, da1_ref, dgown_ref, loss_ref, total_ref, dgb_ref, de_ref,
                  e_v, w_v, a_v, x_v, z_v, dz_v, dx_v, pr_v, mg_v, ow_v, hown_v, a2own_v, dg_v, da_v,
                  stsrc_v, strcv_v, crcv_v, tgt_v, msk_v, wgt_v, ms_v, row_v, tot_v, gsrc_v, grcv_v,
                  ld_sem, h_send, h_recv, h_loc, g_send, g_recv, g_loc,
                  st_send, st_recv, pr_send, pr_recv, r2_send, r3_send, mg_recv, ow_recv, pair_free,
                  cd_send, cd_recv, x_sem, dz_sem, a_sem, out_sem, gb_send, gb_recv, xin_sem, dzin_sem, de_sem):
    n, q, depth, rows, rc, nc, sub = dims
    re = rows // BLOCKS
    half = CHIPS * q
    tok = 2 * half
    cols = 2 * tok
    me = lax.axis_index('tp')
    chip = me // 2
    core = me % 2
    peer = me + 1 - 2 * core
    right_chip = (chip + 1) % CHIPS
    left_chip = (chip + CHIPS - 1) % CHIPS
    far_chip = (chip + 2) % CHIPS
    right = right_chip * 2 + core
    left = left_chip * 2 + core

    ld_e = pltpu.make_async_copy(e_ref, e_v, ld_sem.at[0])
    ld_w = pltpu.make_async_copy(w_ref, w_v, ld_sem.at[1])
    ld_h = pltpu.make_async_copy(h_ref, hown_v, ld_sem.at[2])
    ld_h.start()
    ld_w.start()
    ld_e.start()

    barrier = pltpu.get_barrier_semaphore()
    for r in range(1, n):
        pl.semaphore_signal(barrier, inc=1, **to((me + r) % n))
    pl.semaphore_wait(barrier, n - 1)

    def code_copy(r):
        return remote(code_ref, crcv_v.at[r], cd_send.at[r], cd_recv.at[r], (me + r) % n)

    for r in range(1, n):
        code_copy(r).start()

    lo, hi = pl.ds(0, q // 2), pl.ds(q // 2, q // 2)

    def g1_copies(src, dst, send, recv):
        piece = dst.at[core, chip]
        return (remote(src, piece, send.at[0], recv.at[0], right),
                remote(src, piece, send.at[1], recv.at[1], left),
                remote(src, piece, send.at[2], recv.at[4], peer))

    def g2_copies(dst, send, recv):
        fl, fr = dst.at[core, left_chip], dst.at[core, right_chip]
        return (remote(fl.at[lo], fl.at[lo], send.at[3], recv.at[2], right),
                remote(fr.at[hi], fr.at[hi], send.at[4], recv.at[3], left),
                remote(fl, fl, send.at[5], recv.at[5], peer),
                remote(fr, fr, send.at[6], recv.at[6], peer))

    def g3_copies(dst, send, recv):
        far = dst.at[core, far_chip]
        return (remote(far, far, send.at[7], recv.at[7], peer),)

    def gather1(src, dst, send, recv, loc):
        for c in g1_copies(src, dst, send, recv):
            c.start()
        pltpu.make_async_copy(src, dst.at[core, chip], loc).start()

    def gather2(src, dst, send, recv, loc):
        remote(src, dst.at[core, left_chip], send.at[0], recv.at[0], right).wait_recv()
        remote(src, dst.at[core, right_chip], send.at[1], recv.at[1], left).wait_recv()
        for c in g2_copies(dst, send, recv):
            c.start()
        for c in g1_copies(src, dst, send, recv):
            c.wait_send()
        pltpu.make_async_copy(src, dst.at[core, chip], loc).wait()

    def gather3(dst, send, recv):
        far = dst.at[core, far_chip]
        remote(far.at[lo], far.at[lo], send.at[3], recv.at[2], right).wait_recv()
        remote(far.at[hi], far.at[hi], send.at[4], recv.at[3], left).wait_recv()
        for c in g3_copies(dst, send, recv):
            c.start()
        for c in g2_copies(dst, send, recv):
            c.wait_send()

    def gather4(dst, send, recv):
        for i, c in enumerate((chip, left_chip, right_chip, far_chip)):
            piece = dst.at[1 - core, c]
            remote(piece, piece, send.at[7], recv.at[4 + i], peer).wait_recv()
        for c in g3_copies(dst, send, recv):
            c.wait_send()

    def own(b, h):
        return (hown_v if h == 0 else a2own_v).at[pl.ds(pl.multiple_of(b * q, q), q)]

    def in1(b, h):
        gather1(own(b, h), aall_ref.at[b, h], h_send.at[b, h], h_recv.at[b, h], h_loc.at[b, h])

    def in2(b, h):
        gather2(own(b, h), aall_ref.at[b, h], h_send.at[b, h], h_recv.at[b, h], h_loc.at[b, h])

    def in3(b, h):
        gather3(aall_ref.at[b, h], h_send.at[b, h], h_recv.at[b, h])

    def dg1(b):
        gather1(dg_v.at[b % 4], dgall_ref.at[b], g_send.at[b], g_recv.at[b], g_loc.at[b])

    def dg2(b):
        gather2(dg_v.at[b % 4], dgall_ref.at[b], g_send.at[b], g_recv.at[b], g_loc.at[b])

    def dg3(b):
        gather3(dgall_ref.at[b], g_send.at[b], g_recv.at[b])

    def a_copy(b, h, kk, c):
        at = pl.ds(((h * 2 + kk) * CHIPS + c) * q, q)
        return pltpu.make_async_copy(aall_ref.at[b, h, kk, c], a_v.at[at], a_sem.at[(h * 2 + kk) * CHIPS + c])

    def block_copies(b):
        return [a_copy(b, h, kk, c) for h in range(2) for kk in range(2) for c in range(CHIPS)]

    def fetch_block(b):
        for h in range(2):
            gather4(aall_ref.at[b, h], h_send.at[b, h], h_recv.at[b, h])
        for c in block_copies(b):
            c.start()

    def project_own():
        def proj(i, _):
            sl = pl.ds(pl.multiple_of(i * nc, nc), nc)
            a2own_v[:, sl] = jnp.dot(hown_v[...], w_v[:, sl], preferred_element_type=F32).astype(BF16)
            return 0
        lax.fori_loop(0, depth // nc, proj, 0)

    def norm_rows(start, head):
        a = a_v[pl.ds(start, 16), :].astype(F32)
        mean = jnp.mean(a, axis=-1, keepdims=True)
        cent = a - mean
        var = jnp.mean(cent * cent, axis=-1, keepdims=True)
        y = cent * lax.rsqrt(var + LN_EPS) * gain_ref[pl.ds(head, 1), :] + bias_ref[pl.ds(head, 1), :]
        x_v[pl.ds(start, 16), :] = y.astype(BF16)

    npart = depth // nc
    lrows = cols // npart

    def norm_part(i):
        head = (i * lrows) // tok
        for s in range(lrows // 16):
            norm_rows(pl.multiple_of(i * lrows + s * 16, 16), head)

    def dx_part(i, slot):
        sl = pl.ds(pl.multiple_of(i * nc, nc), nc)
        val = lax.dot_general(dz_v[...], e_v[:, sl], (((0,), (0,)), ((), ())), preferred_element_type=F32)
        for h in range(2):
            for kk in range(2):
                base = h * tok + kk * half
                dx_v[slot, kk, h, :, sl] = val[base:base + half, :]

    nr = rows // rc

    def tree(parts, op):
        while len(parts) > 1:
            parts = [op(a, b) for a, b in zip(parts[::2], parts[1::2])]
        return parts[0]

    def part_view(ref, i):
        return ref.at[pl.ds(pl.multiple_of(i * rc, rc), rc)]

    def back_part(i, p, lanes, td):
        shift, w = row_v[0:1, lanes], row_v[1:2, lanes]
        zc, dc = part_view(z_v, i), part_view(dz_v, i)
        for s in range(p * sub, p * sub + sub, 16):
            both = []
            for t in (s, s + 8):
                pw = jnp.exp(zc[t:t + 8, lanes] - shift)
                both.append(jnp.where(td == t, pw - w, pw))
            dc[s:s + 16, lanes] = jnp.concatenate(both, axis=0).astype(BF16)

    def z_part(i, p):
        ec = part_view(e_v, i)
        part_view(z_v, i)[p * sub:p * sub + sub, :] = lax.dot_general(
            ec[p * sub:p * sub + sub, :], x_v[...], (((1,), (1,)), ((), ())), preferred_element_type=F32)

    def stat_part(i, p, lanes, td, state):
        zc = part_view(z_v, i)
        m_old, acc, tl = state
        at = range(p * sub, p * sub + sub, 8)
        tops = [zc[s:s + 8, lanes] for s in at[:WAYS]]
        for k, s in enumerate(at[WAYS:]):
            tops[k % WAYS] = jnp.maximum(tops[k % WAYS], zc[s:s + 8, lanes])
        m = jnp.maximum(m_old, tree(tops, jnp.maximum))
        accs = [None] * WAYS
        for k, s in enumerate(at):
            z = zc[s:s + 8, lanes]
            e = jnp.exp(z - m)
            accs[k % WAYS] = e if accs[k % WAYS] is None else accs[k % WAYS] + e
            tl = jnp.where(td == s, z, tl)
        return m, acc * jnp.exp(m_old - m) + tree(accs, jnp.add), tl

    def d_body(i, back, new):
        span = cols // LANES
        iota = lax.broadcasted_iota(jnp.int32, (8, span), 0)
        cut = [slice(k * span, k * span + span) for k in range(LANES)]
        td_old = [tgt_v[pl.ds(8, 1), c] - i * rc - iota for c in cut]
        td_new = [tgt_v[pl.ds(9, 1), c] - i * rc - iota for c in cut]
        state = [tuple(ms_v[k, :, c] for k in range(3)) for c in cut]
        for p in range(rc // sub):
            if back:
                for k in range(LANES):
                    back_part(i, p, cut[k], td_old[k])
            if new:
                z_part(i, p)
                for k in range(LANES):
                    state[k] = stat_part(i, p, cut[k], td_new[k], state[k])
        if new:
            for k in range(LANES):
                for q_ in range(3):
                    ms_v[q_, :, cut[k]] = state[k][q_]

    def stat_copy(slot, r):
        return remote(stsrc_v.at[slot], strcv_v.at[slot, r], st_send.at[slot, r], st_recv.at[slot, r], (me + r) % n)

    def send_stats(b):
        slot = b % 2
        m = ms_v[0]
        top = jnp.max(m, axis=0, keepdims=True)
        stsrc_v[slot, 0:1, :] = top
        stsrc_v[slot, 1:2, :] = jnp.sum(ms_v[1] * jnp.exp(m - top), axis=0, keepdims=True)
        stsrc_v[slot, 2:3, :] = jnp.sum(ms_v[2], axis=0, keepdims=True)
        for r in range(1, n):
            stat_copy(slot, r).start()

    def join_stats(b):
        slot = b % 2
        for r in range(1, n):
            stat_copy(slot, r).wait()
        parts = [stsrc_v[slot]] + [strcv_v[slot, r] for r in range(1, n)]
        top = parts[0][0:1]
        for p in parts[1:]:
            top = jnp.maximum(top, p[0:1])
        total = jnp.zeros_like(top)
        hit = jnp.zeros_like(top)
        for p in parts:
            total = total + p[1:2] * jnp.exp(p[0:1] - top)
            hit = hit + p[2:3]
        lse = top + jnp.log(total)
        w = wgt_v[pl.ds(b, 1), :]
        row_v[0:1, :] = jnp.where(w > 0.0, lse - jnp.log(jnp.where(w > 0.0, w, 1.0)), 3.0e38)
        row_v[1:2, :] = w
        tgt_v[pl.ds(8, 1), :] = tgt_v[pl.ds(b, 1), :]
        loss = (lse - hit) * msk_v[pl.ds(b, 1), :]
        loss_ref[pl.ds(b, 1), :] = loss
        tot_v[0:1, :] = tot_v[0:1, :] + loss / tot_v[1:2, :]

    def pair_copy(b):
        slot = b % 2
        return remote(dx_v.at[slot, 1 - core], pr_v.at[slot], pr_send.at[slot], pr_recv.at[slot], peer)

    def rs1(b):
        @pl.when(b >= 2)
        def _():
            pl.semaphore_wait(pair_free, 1)
        pair_copy(b).start()

    def crow(c):
        return pl.ds(pl.multiple_of(c * q, q), q)

    def r2_copies(b):
        s2, s3 = b % 2, b % 3
        mine = dx_v.at[s2, core]
        return (remote(mine.at[0, crow(far_chip)], mg_v.at[s2, 0], r2_send.at[s2, 0], mg_recv.at[s2, 0], right),
                remote(mine.at[1, crow(far_chip)], mg_v.at[s2, 1], r2_send.at[s2, 1], mg_recv.at[s2, 1], left),
                remote(mine.at[1, crow(right_chip)], ow_v.at[s3, 0, 1], r2_send.at[s2, 2], ow_recv.at[s3, 0, 1], right),
                remote(mine.at[0, crow(left_chip)], ow_v.at[s3, 1, 0], r2_send.at[s2, 3], ow_recv.at[s3, 1, 0], left))

    def rs2(b):
        slot = b % 2
        pair_copy(b).wait()

        def add(i, _):
            h = i // CHIPS
            c = i % CHIPS
            dx_v[slot, core, h, crow(c), :] += pr_v[slot, h, crow(c), :]
            return 0
        lax.fori_loop(0, 2 * CHIPS, add, 0)

        @pl.when(b < BLOCKS - 2)
        def _():
            pl.semaphore_signal(pair_free, inc=1, **to(peer))
        for c in r2_copies(b):
            c.start()

    def r3_copies(b):
        s2, s3 = b % 2, b % 3
        mine = dx_v.at[s2, core]
        return (remote(mine.at[0, crow(right_chip)], ow_v.at[s3, 0, 0], r3_send.at[s2, 0], ow_recv.at[s3, 0, 0], right),
                remote(mine.at[1, crow(left_chip)], ow_v.at[s3, 1, 1], r3_send.at[s2, 1], ow_recv.at[s3, 1, 1], left))

    def rs3(b):
        s2 = b % 2
        c2 = r2_copies(b)
        c2[0].wait_recv()
        c2[1].wait_recv()
        dx_v[s2, core, 0, crow(right_chip), :] += mg_v[s2, 0]
        dx_v[s2, core, 1, crow(left_chip), :] += mg_v[s2, 1]
        for c in r3_copies(b):
            c.start()

    def rs4(b):
        s2, s3 = b % 2, b % 3
        c2, c3 = r2_copies(b), r3_copies(b)
        c2[2].wait_recv()
        c2[3].wait_recv()
        c3[0].wait_recv()
        c3[1].wait_recv()

        @pl.when(b >= 1)
        def _():
            out_copies(b - 1)[0].wait()
            out_copies(b - 1)[1].wait()
        for h in range(2):
            dy = dx_v[s2, core, h, crow(chip), :] + ow_v[s3, 0, h] + ow_v[s3, 1, h]
            a = own(b, h)[...].astype(F32)
            mean = jnp.mean(a, axis=-1, keepdims=True)
            cent = a - mean
            rstd = lax.rsqrt(jnp.mean(cent * cent, axis=-1, keepdims=True) + LN_EPS)
            xhat = cent * rstd
            gsrc_v[h:h + 1, :] += jnp.sum(dy * xhat, axis=0, keepdims=True)
            gsrc_v[2 + h:3 + h, :] += jnp.sum(dy, axis=0, keepdims=True)
            dxh = dy * gain_ref[h:h + 1, :]
            c1 = jnp.mean(dxh, axis=-1, keepdims=True)
            c2_ = jnp.mean(dxh * xhat, axis=-1, keepdims=True)
            da = rstd * (dxh - c1 - xhat * c2_)
            if h == 0:
                da_v[...] = da
            else:
                dg_v[b % 4] = da.astype(BF16)
        for c in out_copies(b):
            c.start()
        for c in c2 + c3:
            c.wait_send()

    def out_copies(b):
        return (pltpu.make_async_copy(da_v, da1_ref.at[b], out_sem.at[0]),
                pltpu.make_async_copy(dg_v.at[b % 4], dgown_ref.at[b], out_sem.at[1]))

    def xin_copy(i):
        sl = pl.ds(pl.multiple_of(i * nc, nc), nc)
        return pltpu.make_async_copy(xall_ref.at[:, sl], e_v.at[:, sl], xin_sem.at[i])

    def dzin_copy(c, hf):
        return pltpu.make_async_copy(
            dzt_ref.at[pl.ds(pl.multiple_of(c * re, re), re), pl.ds(hf * depth, depth)],
            w_v.at[pl.ds(pl.multiple_of((c % 2) * 2 * re + hf * re, re), re)], dzin_sem.at[c % 2, hf])

    def de_copy(c, i):
        return pltpu.make_async_copy(
            z_v.at[pl.ds(pl.multiple_of(i * re, re), re)],
            de_ref.at[pl.ds(pl.multiple_of(c * re, re), re), pl.ds(pl.multiple_of(i * nc, nc), nc)], de_sem.at[i])

    def de_chunk(c):
        for hf in range(2):
            dzin_copy(c, hf).wait()
        base = (c % 2) * 2 * re
        lo = w_v.at[pl.ds(pl.multiple_of(base, re), re)]
        hi = w_v.at[pl.ds(pl.multiple_of(base + re, re), re)]

        def part(i, _):
            sl = pl.ds(pl.multiple_of(i * nc, nc), nc)

            @pl.when(c == 0)
            def _():
                xin_copy(i).wait()

            @pl.when(c >= 1)
            def _():
                de_copy(c - 1, i).wait()
            val = jnp.dot(lo[...], e_v[:depth, sl], preferred_element_type=F32)
            val = val + jnp.dot(hi[...], e_v[depth:, sl], preferred_element_type=F32)
            z_v[pl.ds(pl.multiple_of(i * re, re), re), :] = val
            de_copy(c, i).start()
            return 0
        lax.fori_loop(0, npart, part, 0)

        @pl.when(c + 2 < KEEP)
        def _():
            for hf in range(2):
                dzin_copy(c + 2, hf).start()

    def inside(b, fn, name='svc'):
        @pl.when(jnp.logical_and(b >= 0, b < BLOCKS))
        def _():
            with jax.named_scope(name):
                fn(b)

    def between(j, lo, hi, fn, name='svc'):
        @pl.when(jnp.logical_and(j >= lo, j <= hi))
        def _():
            with jax.named_scope(name):
                fn()

    def x_copy(b):
        return pltpu.make_async_copy(x_v, xall_ref.at[pl.ds(pl.multiple_of(b * cols, cols), cols)], x_sem)

    def dz_copy(b):
        return pltpu.make_async_copy(dz_v, dzt_ref.at[:, pl.ds(pl.multiple_of(b * cols, cols), cols)], dz_sem)

    def loop(k, fn):
        def body(i, _):
            fn(i)
            return 0
        lax.fori_loop(0, k, body, 0)

    ld_h.wait()
    in1(0, 0)
    in1(1, 0)
    ld_w.wait()
    project_own()
    in1(0, 1)
    in1(1, 1)
    in2(0, 0)
    in2(1, 0)
    for r in range(1, n):
        code_copy(r).wait()
    code = code_ref[...]
    for r in range(1, n):
        code = code + crcv_v[r]
    mask = (code >= 65536).astype(jnp.int32)
    local = code - mask * 65536 - me * rows
    tgt_v[0:BLOCKS, :] = jnp.where(jnp.logical_and(local >= 0, local < rows), local, -(1 << 24))
    maskf = mask.astype(F32)
    msk_v[...] = maskf
    per_col = jnp.sum(maskf, axis=0, keepdims=True)
    n0 = jnp.sum(per_col[:, :tok], axis=1, keepdims=True)
    n1 = jnp.sum(per_col[:, tok:], axis=1, keepdims=True)
    counts = jnp.concatenate([jnp.broadcast_to(n0, (1, tok)), jnp.broadcast_to(n1, (1, tok))], axis=1)
    wgt_v[...] = maskf / counts
    tot_v[0:1, :] = jnp.zeros((1, cols), F32)
    tot_v[1:2, :] = counts
    gsrc_v[...] = jnp.zeros_like(gsrc_v)
    in3(0, 0)
    in2(0, 1)
    in3(0, 1)
    in2(1, 1)
    fetch_block(0)
    ld_e.wait()

    def both(fn):
        def run(b):
            fn(b, 0)
            fn(b, 1)
        return run

    def last_stage(b):
        rs4(b)
        dg1(b)

    def gather_in(h):
        between(h, -2, BLOCKS - 5, lambda: both(in1)(h + 4), 'in1')
        between(h, -1, BLOCKS - 4, lambda: both(in2)(h + 3), 'in2')
        between(h, 0, BLOCKS - 3, lambda: both(in3)(h + 2), 'in3')

    def step(t, _):
        j = t - 1
        def block_wait():
            for c in block_copies(j + 1):
                c.wait()
        between(j, -1, BLOCKS - 2, block_wait, 'bwait')
        between(j, 1, BLOCKS, lambda: x_wait(j), 'xwait')

        def full_a():
            def body(i):
                dx_part(i, (j - 1) % 2)
                norm_part(i)
            loop(npart, body)
        between(j, -1, 0, lambda: loop(npart, norm_part), 'norm')
        between(j, 1, BLOCKS - 2, full_a, 'full_a')
        between(j, BLOCKS, BLOCKS, start_tail, 'start_tail')

        def last_a(i):
            dx_part(i, (j - 1) % 2)

            @pl.when(j == BLOCKS)
            def _():
                xin_copy(i).start()

            @pl.when(jnp.logical_and(j == BLOCKS - 1, i == npart - 2))
            def _():
                rs3(BLOCKS - 3)
        between(j, BLOCKS - 1, BLOCKS, lambda: loop(npart, last_a), 'last_a')
        between(j, BLOCKS + 1, BLOCKS + 2, lambda: de_chunk(2 * (j - BLOCKS) - 1), 'de_a')
        between(j, -1, BLOCKS - 2, lambda: x_copy(j + 1).start(), 'xstart')
        inside(j - 1, rs1, 'rs1')
        between(j, 2, BLOCKS - 2, lambda: rs3(j - 2), 'rs3')
        between(j, BLOCKS, BLOCKS + 1, lambda: rs3(j - 2), 'rs3')
        between(j, -1, -1, lambda: both(in3)(1), 'in3p')
        gather_in(2 * j)
        inside(j - 3, dg2, 'dg2')
        between(j, BLOCKS + 2, BLOCKS + 2, gb_start, 'gbstart')
        inside(j, join_stats, 'join')
        between(j, 1, BLOCKS - 1, lambda: dz_copy(j - 1).wait(), 'dzwait')
        between(j, BLOCKS, BLOCKS + 2, lambda: de_chunk(2 * (j - BLOCKS)), 'de_d')

        def start_stats():
            ms_v[0] = jnp.full((8, cols), -3.0e38, F32)
            ms_v[1] = jnp.zeros((8, cols), F32)
            ms_v[2] = jnp.zeros((8, cols), F32)
            tgt_v[pl.ds(9, 1), :] = tgt_v[pl.ds(j + 1, 1), :]
        between(j, -1, BLOCKS - 2, start_stats)

        between(j, -1, -1, lambda: loop(nr, lambda i: d_body(i, False, True)), 'only_z')
        between(j, 0, BLOCKS - 2, lambda: loop(nr, lambda i: d_body(i, True, True)), 'full_d')
        between(j, BLOCKS - 1, BLOCKS - 1, lambda: loop(nr, lambda i: d_body(i, True, False)), 'back')
        between(j, -1, BLOCKS - 3, lambda: fetch_block(j + 2), 'fetch')
        between(j, -1, BLOCKS - 2, lambda: send_stats(j + 1), 'stats')
        inside(j, lambda b: dz_copy(b).start(), 'dzstart')
        inside(j - 2, last_stage, 'rs4g1')
        gather_in(2 * j + 1)
        inside(j - 1, rs2, 'rs2')
        inside(j - 3, dg3, 'dg3')
        return 0

    def gb_copy(r):
        return remote(gsrc_v, grcv_v.at[r], gb_send.at[r], gb_recv.at[r], (me + r) % n)

    def gb_start():
        for r in range(1, n):
            gb_copy(r).start()

    def start_tail():
        dz_copy(BLOCKS - 1).wait()
        for c in range(2):
            for hf in range(2):
                dzin_copy(c, hf).start()

    def x_wait(j):
        @pl.when(j <= BLOCKS - 1)
        def _():
            x_copy(j).wait()

    def first_x(j):
        x_copy(j).wait()

    def step_outer(t, c):
        @pl.when(t == 1)
        def _():
            first_x(0)
        return step(t, c)

    lax.fori_loop(0, BLOCKS + 4, step_outer, 0)

    for b in range(BLOCKS):
        gather4(dgall_ref.at[b], g_send.at[b], g_recv.at[b])
    for c in out_copies(BLOCKS - 1):
        c.wait()
    total_ref[...] = jnp.broadcast_to(jnp.sum(tot_v[0:1, :], axis=1, keepdims=True), total_ref.shape)

    for i in range(npart):
        de_copy(KEEP - 1, i).wait()
    for r in range(1, n):
        gb_copy(r).wait()
    acc = gsrc_v[...]
    for r in range(1, n):
        acc = acc + grcv_v[r]
    dgb_ref[...] = acc


def stream(n, hidden, w_two, gain, bias, embed, code):
    tokens, depth = hidden.shape
    rows = embed.shape[0]
    q = tokens // BLOCKS
    half = CHIPS * q
    tok = 2 * half
    cols = 2 * tok
    nc = depth // 4
    rc, sub = rows // 2, rows // 8
    assert BLOCKS * cols == rows == 2 * depth and nc == cols
    dims = (n, q, depth, rows, rc, nc, sub)
    any_spec = pl.BlockSpec(memory_space=pl.ANY)
    vmem = pl.BlockSpec(memory_space=pltpu.VMEM)
    dma = pltpu.SemaphoreType.DMA
    sds = jax.ShapeDtypeStruct
    return pl.pallas_call(
        functools.partial(stream_kernel, dims),
        out_shape=(sds((BLOCKS, 2, 2, CHIPS, q, depth), BF16), sds((BLOCKS * cols, depth), BF16),
                   sds((rows, BLOCKS * cols), BF16), sds((BLOCKS, 2, CHIPS, q, depth), BF16),
                   sds((BLOCKS, q, depth), F32), sds((BLOCKS, q, depth), BF16),
                   sds((BLOCKS, cols), F32), sds((8, 128), F32), sds((8, depth), F32),
                   sds((KEEP * (rows // BLOCKS), depth), F32)),
        in_specs=[any_spec, any_spec, vmem, vmem, any_spec, vmem],
        out_specs=(any_spec,) * 6 + (vmem,) * 3 + (any_spec,),
        scratch_shapes=[
            pltpu.VMEM((rows, depth), BF16), pltpu.VMEM((depth, depth), BF16),
            pltpu.VMEM((cols, depth), BF16), pltpu.VMEM((cols, depth), BF16),
            pltpu.VMEM((rows, cols), F32), pltpu.VMEM((rows, cols), BF16),
            pltpu.VMEM((2, 2, 2, half, depth), F32), pltpu.VMEM((2, 2, half, depth), F32),
            pltpu.VMEM((2, 2, q, depth), F32), pltpu.VMEM((3, 2, 2, q, depth), F32),
            pltpu.VMEM((tokens, depth), BF16), pltpu.VMEM((tokens, depth), BF16),
            pltpu.VMEM((4, q, depth), BF16), pltpu.VMEM((q, depth), F32),
            pltpu.VMEM((2, 8, cols), F32), pltpu.VMEM((2, n, 8, cols), F32),
            pltpu.VMEM((n, BLOCKS, cols), jnp.int32), pltpu.VMEM((16, cols), jnp.int32),
            pltpu.VMEM((BLOCKS, cols), F32), pltpu.VMEM((BLOCKS, cols), F32),
            pltpu.VMEM((3, 8, cols), F32), pltpu.VMEM((8, cols), F32), pltpu.VMEM((8, cols), F32),
            pltpu.VMEM((8, depth), F32), pltpu.VMEM((n, 8, depth), F32),
            dma((3,)), dma((BLOCKS, 2, 8)), dma((BLOCKS, 2, 8)), dma((BLOCKS, 2)), dma((BLOCKS, 8)), dma((BLOCKS, 8)),
            dma((BLOCKS,)), dma((2, n)), dma((2, n)), dma((2,)), dma((2,)), dma((2, 4)), dma((2, 2)),
            dma((2, 2)), dma((3, 2, 2)), pltpu.SemaphoreType.REGULAR,
            dma((n,)), dma((n,)), dma, dma, dma((4 * CHIPS,)), dma((2,)), dma((n,)), dma((n,)),
            dma((depth // nc,)), dma((2, 2)), dma((depth // nc,)),
        ],
        compiler_params=pltpu.CompilerParams(collective_id=0, has_side_effects=True, vmem_limit_bytes=67043328),
        name='stream',
    )(hidden, w_two, gain, bias, embed, code)


def dense_kernel(part_ref, dzt_ref, xall_ref, aall_ref, gall_ref, da_ref, go_ref, w_ref, de_ref, dw_ref, dh_ref,
                 w_v, g_v, x_v, h_v, dw_v, dz_v, de_v, st_v, w_sem, g_sem, x_sem, h_sem, dw_sem, dz_sem, de_sem, in_sem, out_sem):
    depth = x_v.shape[1]
    nc, wb = depth // 4, depth // BLOCKS
    re = dzt_ref.shape[0] // BLOCKS
    xr = x_v.shape[0] // BLOCKS
    todo = BLOCKS - KEEP
    pieces = BLOCKS + 4 * todo
    pr = KEEP * re // pieces

    def at(i, size):
        return pl.ds(pl.multiple_of(i * size, size), size)

    def w_copy(i):
        return pltpu.make_async_copy(w_ref.at[at(i, nc)], w_v.at[at(i, nc)], w_sem.at[i])

    def h_copy(i):
        return pltpu.make_async_copy(aall_ref.at[:, 0:h_v.shape[2], at(i, wb)], h_v.at[i % 2], h_sem.at[i % 2])

    def dw_copy(i):
        return pltpu.make_async_copy(dw_v.at[i % 2], dw_ref.at[at(i, wb)], dw_sem.at[i % 2])

    def x_copy(i):
        return pltpu.make_async_copy(xall_ref.at[at(i, xr)], x_v.at[at(i, xr)], x_sem.at[i])

    def dz_copy(c):
        return pltpu.make_async_copy(dzt_ref.at[at(KEEP + c, re)], dz_v.at[c % 2], dz_sem.at[c % 2])

    def de_copy(u):
        return pltpu.make_async_copy(de_v.at[u % 2], de_ref.at[at(KEEP + u // 4, re), at(u % 4, nc)], de_sem.at[u % 2])

    def pin(t):
        return pltpu.make_async_copy(part_ref.at[at(t, pr)], st_v.at[t % 4], in_sem.at[t % 4])

    def pout(t):
        return pltpu.make_async_copy(st_v.at[t % 4], de_ref.at[at(t, pr)], out_sem.at[t % 4])

    def carry(t):
        pin(t).wait()
        pout(t).start()

        @pl.when(t >= 2)
        def _():
            pout(t - 2).wait()

        @pl.when(t + 2 < pieces)
        def _():
            pin(t + 2).start()

    g_load = pltpu.make_async_copy(gall_ref, g_v, g_sem)
    for i in range(4):
        w_copy(i).start()
    g_load.start()
    h_copy(0).start()
    h_copy(1).start()
    pin(0).start()
    pin(1).start()

    def hidden_part(i, _):
        w_copy(i).wait()
        sl = at(i, nc)
        back = lax.dot_general(go_ref[...], w_v[sl, :], (((1,), (1,)), ((), ())), preferred_element_type=F32)
        dh_ref[:, sl] = (da_ref[:, sl] + back).astype(BF16)
        return 0
    lax.fori_loop(0, 4, hidden_part, 0)
    g_load.wait()

    def dw_part(i, _):
        h_copy(i).wait()
        x_copy(i).start()

        @pl.when(i == BLOCKS - 2)
        def _():
            dz_copy(0).start()
            dz_copy(1).start()
        carry(i)

        @pl.when(i >= 2)
        def _():
            dw_copy(i - 2).wait()
        h = h_v[i % 2].reshape(g_v.shape[0], wb)
        dw_v[i % 2] = lax.dot_general(h, g_v[...], (((0,), (0,)), ((), ())), preferred_element_type=F32)
        dw_copy(i).start()

        @pl.when(i + 2 < BLOCKS)
        def _():
            h_copy(i + 2).start()
        return 0
    lax.fori_loop(0, BLOCKS, dw_part, 0)
    for i in range(BLOCKS):
        x_copy(i).wait()

    def de_part(u, _):
        c = u // 4

        @pl.when(u % 4 == 0)
        def _():
            dz_copy(c).wait()
        carry(BLOCKS + u)

        @pl.when(u >= 2)
        def _():
            de_copy(u - 2).wait()
        de_v[u % 2] = jnp.dot(dz_v[c % 2], x_v[:, at(u % 4, nc)], preferred_element_type=F32)
        de_copy(u).start()

        @pl.when(jnp.logical_and(u % 4 == 3, c + 2 < todo))
        def _():
            dz_copy(c + 2).start()
        return 0
    lax.fori_loop(0, 4 * todo, de_part, 0)
    for i in (BLOCKS - 2, BLOCKS - 1):
        dw_copy(i).wait()
    for i in (4 * todo - 2, 4 * todo - 1):
        de_copy(i).wait()
    for t in (pieces - 2, pieces - 1):
        pout(t).wait()


def dense(part, dzt, xall, aall, gall, da1, dgown, w_two):
    rows, kk = dzt.shape
    depth = xall.shape[1]
    total, tokens = gall.shape[0], da1.shape[0]
    re, wb, nc = rows // BLOCKS, depth // BLOCKS, depth // 4
    pieces = BLOCKS + 4 * (BLOCKS - KEEP)
    sds = jax.ShapeDtypeStruct
    dma = pltpu.SemaphoreType.DMA
    any_spec = pl.BlockSpec(memory_space=pl.ANY)
    vmem = pl.BlockSpec(memory_space=pltpu.VMEM)
    return pl.pallas_call(
        dense_kernel,
        out_shape=(sds((rows, depth), F32), sds((depth, depth), F32), sds((tokens, depth), BF16)),
        in_specs=[any_spec] * 5 + [vmem, vmem, any_spec],
        out_specs=(any_spec, any_spec, vmem),
        scratch_shapes=[pltpu.VMEM((depth, depth), BF16), pltpu.VMEM((total, depth), BF16), pltpu.VMEM((kk, depth), BF16),
                        pltpu.VMEM((2, BLOCKS, total // BLOCKS, wb), BF16), pltpu.VMEM((2, wb, depth), F32),
                        pltpu.VMEM((2, re, kk), BF16), pltpu.VMEM((2, re, nc), F32),
                        pltpu.VMEM((4, KEEP * re // pieces, depth), F32),
                        dma((4,)), dma, dma((BLOCKS,)), dma((2,)), dma((2,)), dma((2,)), dma((2,)), dma((4,)), dma((4,))],
        compiler_params=pltpu.CompilerParams(vmem_limit_bytes=67043328),
        name='dense',
    )(part, dzt, xall, aall, gall, da1, dgown, w_two)


def solution(mesh):
    n = mesh.shape['tp']
    tok_spec = P(('dp', 'tp'), None)
    row_spec = P(None, ('dp', 'tp'))

    def device_step(hidden, w_two, ln_scale, ln_shift, embed, targets, loss_mask):
        tokens, depth = hidden.shape
        q = tokens // BLOCKS
        me = lax.axis_index('tp')
        code = (targets + 65536 * loss_mask).reshape(2, BLOCKS, q).transpose(1, 0, 2)
        place = (me % 2) * CHIPS + me // 2
        seat = lax.broadcasted_iota(jnp.int32, (1, 1, 2 * CHIPS, 1), 2) == place
        code = jnp.where(seat, code[:, :, None, :], 0).reshape(BLOCKS, 2 * 2 * CHIPS * q)
        aall, xall, dzt, dgall, da1, dgown, loss, total, dgb, part = stream(
            n, hidden, w_two, ln_scale, ln_shift, embed, code)
        d_embed, d_w, d_hidden = dense(part, dzt, xall, aall.reshape(BLOCKS, 2 * n * q, depth), dgall.reshape(n * tokens, depth),
                                       da1.reshape(tokens, depth), dgown.reshape(tokens, depth), w_two)
        loss = loss.reshape(BLOCKS, 2, 2 * CHIPS, q)
        mine = lax.dynamic_index_in_dim(loss, place, axis=2, keepdims=False)
        token_loss = mine.transpose(1, 0, 2).reshape(2, tokens)
        return token_loss, total[0, :1], d_hidden, d_embed, d_w, dgb[0:2], dgb[2:4]

    return jax.shard_map(device_step, mesh=mesh,
                         in_specs=(tok_spec, P(), P(), P(), P('tp', None), row_spec, row_spec),
                         out_specs=(row_spec, P('dp'), tok_spec, tok_spec, P('dp', None), P('dp', None), P('dp', None)),
                         check_vma=False)
```

```python
import functools

import jax
import jax.numpy as jnp
from jax import lax
from jax.experimental import pallas as pl
from jax.experimental.pallas import tpu as pltpu
from jax.sharding import PartitionSpec as P

LN_EPS = 1e-5
CHIPS = 4
BLOCKS = 8
KEEP = 6
WAYS = 4
LANES = 2
F32 = jnp.float32
BF16 = jnp.bfloat16


def to(idx):
    return dict(device_id={'tp': idx}, device_id_type=pl.DeviceIdType.MESH)


def remote(src, dst, send, recv, idx):
    return pltpu.make_async_remote_copy(src_ref=src, dst_ref=dst, send_sem=send, recv_sem=recv, **to(idx))


def stream_kernel(dims, h_ref, w_ref, gain_ref, bias_ref, e_ref, code_ref,
                  aall_ref, xall_ref, dzt_ref, dgall_ref, da1_ref, dgown_ref, loss_ref, total_ref, dgb_ref, de_ref,
                  e_v, a_v, x_v, z_v, dz_v, dx_v, pr_v, mg_v, ow_v, hown_v, a2own_v, dg_v, da_v,
                  stsrc_v, strcv_v, crcv_v, tgt_v, msk_v, wgt_v, ms_v, row_v, tot_v, gsrc_v, grcv_v,
                  ld_sem, h_send, h_recv, h_loc, g_send, g_recv, g_loc,
                  st_send, st_recv, pr_send, pr_recv, r2_send, r3_send, mg_recv, ow_recv, pair_free,
                  cd_send, cd_recv, x_sem, dz_sem, a_sem, out_sem, gb_send, gb_recv, xin_sem, dzin_sem, de_sem):
    n, q, depth, rows, rc, nc, sub = dims
    re = rows // BLOCKS
    half = CHIPS * q
    tok = 2 * half
    cols = 2 * tok
    me = lax.axis_index('tp')
    chip = me // 2
    core = me % 2
    peer = me + 1 - 2 * core
    right_chip = (chip + 1) % CHIPS
    left_chip = (chip + CHIPS - 1) % CHIPS
    far_chip = (chip + 2) % CHIPS
    right = right_chip * 2 + core
    left = left_chip * 2 + core

    top, bottom = pl.ds(0, depth), pl.ds(depth, rows - depth)
    ld_e = [pltpu.make_async_copy(e_ref.at[d], e_v.at[d], ld_sem.at[i]) for i, d in ((0, top), (3, bottom))]
    ld_w = pltpu.make_async_copy(w_ref, e_v.at[top], ld_sem.at[1])
    ld_h = pltpu.make_async_copy(h_ref, hown_v, ld_sem.at[2])
    ld_h.start()
    ld_w.start()
    ld_e[1].start()

    barrier = pltpu.get_barrier_semaphore()
    for r in range(1, n):
        pl.semaphore_signal(barrier, inc=1, **to((me + r) % n))
    pl.semaphore_wait(barrier, n - 1)

    def code_copy(r):
        return remote(code_ref, crcv_v.at[r], cd_send.at[r], cd_recv.at[r], (me + r) % n)

    for r in range(1, n):
        code_copy(r).start()

    lo, hi = pl.ds(0, q // 2), pl.ds(q // 2, q // 2)

    def g1_copies(src, dst, send, recv):
        piece = dst.at[core, chip]
        return (remote(src, piece, send.at[0], recv.at[0], right),
                remote(src, piece, send.at[1], recv.at[1], left),
                remote(src, piece, send.at[2], recv.at[4], peer))

    def g2_copies(dst, send, recv):
        fl, fr = dst.at[core, left_chip], dst.at[core, right_chip]
        return (remote(fl.at[lo], fl.at[lo], send.at[3], recv.at[2], right),
                remote(fr.at[hi], fr.at[hi], send.at[4], recv.at[3], left),
                remote(fl, fl, send.at[5], recv.at[5], peer),
                remote(fr, fr, send.at[6], recv.at[6], peer))

    def g3_copies(dst, send, recv):
        far = dst.at[core, far_chip]
        return (remote(far, far, send.at[7], recv.at[7], peer),)

    def gather1(src, dst, send, recv, loc):
        for c in g1_copies(src, dst, send, recv):
            c.start()
        pltpu.make_async_copy(src, dst.at[core, chip], loc).start()

    def gather2(src, dst, send, recv, loc):
        remote(src, dst.at[core, left_chip], send.at[0], recv.at[0], right).wait_recv()
        remote(src, dst.at[core, right_chip], send.at[1], recv.at[1], left).wait_recv()
        for c in g2_copies(dst, send, recv):
            c.start()
        for c in g1_copies(src, dst, send, recv):
            c.wait_send()
        pltpu.make_async_copy(src, dst.at[core, chip], loc).wait()

    def gather3(dst, send, recv):
        far = dst.at[core, far_chip]
        remote(far.at[lo], far.at[lo], send.at[3], recv.at[2], right).wait_recv()
        remote(far.at[hi], far.at[hi], send.at[4], recv.at[3], left).wait_recv()
        for c in g3_copies(dst, send, recv):
            c.start()
        for c in g2_copies(dst, send, recv):
            c.wait_send()

    def gather4(dst, send, recv):
        for i, c in enumerate((chip, left_chip, right_chip, far_chip)):
            piece = dst.at[1 - core, c]
            remote(piece, piece, send.at[7], recv.at[4 + i], peer).wait_recv()
        for c in g3_copies(dst, send, recv):
            c.wait_send()

    def own(b, h):
        return (hown_v if h == 0 else a2own_v).at[pl.ds(pl.multiple_of(b * q, q), q)]

    def in1(b, h):
        gather1(own(b, h), aall_ref.at[b, h], h_send.at[b, h], h_recv.at[b, h], h_loc.at[b, h])

    def in2(b, h):
        gather2(own(b, h), aall_ref.at[b, h], h_send.at[b, h], h_recv.at[b, h], h_loc.at[b, h])

    def in3(b, h):
        gather3(aall_ref.at[b, h], h_send.at[b, h], h_recv.at[b, h])

    def dg1(b):
        gather1(dg_v.at[b % 4], dgall_ref.at[b], g_send.at[b], g_recv.at[b], g_loc.at[b])

    def dg2(b):
        gather2(dg_v.at[b % 4], dgall_ref.at[b], g_send.at[b], g_recv.at[b], g_loc.at[b])

    def dg3(b):
        gather3(dgall_ref.at[b], g_send.at[b], g_recv.at[b])

    def a_copy(b, h, kk, c):
        at = pl.ds(((h * 2 + kk) * CHIPS + c) * q, q)
        return pltpu.make_async_copy(aall_ref.at[b, h, kk, c], a_v.at[at], a_sem.at[(h * 2 + kk) * CHIPS + c])

    def block_copies(b):
        return [a_copy(b, h, kk, c) for h in range(2) for kk in range(2) for c in range(CHIPS)]

    def fetch_block(b):
        for h in range(2):
            gather4(aall_ref.at[b, h], h_send.at[b, h], h_recv.at[b, h])
        for c in block_copies(b):
            c.start()

    def project_own():
        def proj(i, _):
            sl = pl.ds(pl.multiple_of(i * nc, nc), nc)
            a2own_v[:, sl] = jnp.dot(hown_v[...], e_v[top, sl], preferred_element_type=F32).astype(BF16)
            return 0
        lax.fori_loop(0, depth // nc, proj, 0)

    def norm_rows(start, head):
        a = a_v[pl.ds(start, 16), :].astype(F32)
        mean = jnp.mean(a, axis=-1, keepdims=True)
        cent = a - mean
        var = jnp.mean(cent * cent, axis=-1, keepdims=True)
        y = cent * lax.rsqrt(var + LN_EPS) * gain_ref[pl.ds(head, 1), :] + bias_ref[pl.ds(head, 1), :]
        x_v[pl.ds(start, 16), :] = y.astype(BF16)

    npart = depth // nc
    lrows = cols // npart

    def norm_part(i):
        head = (i * lrows) // tok
        for s in range(lrows // 16):
            norm_rows(pl.multiple_of(i * lrows + s * 16, 16), head)

    def dx_part(i, slot):
        sl = pl.ds(pl.multiple_of(i * nc, nc), nc)
        val = lax.dot_general(dz_v[...], e_v[:, sl], (((0,), (0,)), ((), ())), preferred_element_type=F32)
        for h in range(2):
            for kk in range(2):
                base = h * tok + kk * half
                dx_v[slot, kk, h, :, sl] = val[base:base + half, :]

    nr = rows // rc

    def tree(parts, op):
        while len(parts) > 1:
            parts = [op(a, b) for a, b in zip(parts[::2], parts[1::2])]
        return parts[0]

    def part_view(ref, i):
        return ref.at[pl.ds(pl.multiple_of(i * rc, rc), rc)]

    def back_part(i, p, lanes, td):
        shift, w = row_v[0:1, lanes], row_v[1:2, lanes]
        zc, dc = part_view(z_v, i), part_view(dz_v, i)
        for s in range(p * sub, p * sub + sub, 16):
            both = []
            for t in (s, s + 8):
                pw = jnp.exp(zc[t:t + 8, lanes] - shift)
                both.append(jnp.where(td == t, pw - w, pw))
            dc[s:s + 16, lanes] = jnp.concatenate(both, axis=0).astype(BF16)

    def z_part(i, p):
        ec = part_view(e_v, i)
        part_view(z_v, i)[p * sub:p * sub + sub, :] = lax.dot_general(
            ec[p * sub:p * sub + sub, :], x_v[...], (((1,), (1,)), ((), ())), preferred_element_type=F32)

    def stat_part(i, p, lanes, td, state):
        zc = part_view(z_v, i)
        m_old, acc, tl = state
        at = range(p * sub, p * sub + sub, 8)
        tops = [zc[s:s + 8, lanes] for s in at[:WAYS]]
        for k, s in enumerate(at[WAYS:]):
            tops[k % WAYS] = jnp.maximum(tops[k % WAYS], zc[s:s + 8, lanes])
        m = jnp.maximum(m_old, tree(tops, jnp.maximum))
        accs = [None] * WAYS
        for k, s in enumerate(at):
            z = zc[s:s + 8, lanes]
            e = jnp.exp(z - m)
            accs[k % WAYS] = e if accs[k % WAYS] is None else accs[k % WAYS] + e
            tl = jnp.where(td == s, z, tl)
        return m, acc * jnp.exp(m_old - m) + tree(accs, jnp.add), tl

    def d_body(i, back, new):
        span = cols // LANES
        iota = lax.broadcasted_iota(jnp.int32, (8, span), 0)
        cut = [slice(k * span, k * span + span) for k in range(LANES)]
        td_old = [tgt_v[pl.ds(8, 1), c] - i * rc - iota for c in cut]
        td_new = [tgt_v[pl.ds(9, 1), c] - i * rc - iota for c in cut]
        state = [tuple(ms_v[k, :, c] for k in range(3)) for c in cut]
        for p in range(rc // sub):
            if back:
                for k in range(LANES):
                    back_part(i, p, cut[k], td_old[k])
            if new:
                z_part(i, p)
                for k in range(LANES):
                    state[k] = stat_part(i, p, cut[k], td_new[k], state[k])
        if new:
            for k in range(LANES):
                for q_ in range(3):
                    ms_v[q_, :, cut[k]] = state[k][q_]

    def stat_copy(slot, r):
        return remote(stsrc_v.at[slot], strcv_v.at[slot, r], st_send.at[slot, r], st_recv.at[slot, r], (me + r) % n)

    def send_stats(b):
        slot = b % 2
        m = ms_v[0]
        top = jnp.max(m, axis=0, keepdims=True)
        stsrc_v[slot, 0:1, :] = top
        stsrc_v[slot, 1:2, :] = jnp.sum(ms_v[1] * jnp.exp(m - top), axis=0, keepdims=True)
        stsrc_v[slot, 2:3, :] = jnp.sum(ms_v[2], axis=0, keepdims=True)
        for r in range(1, n):
            stat_copy(slot, r).start()

    def join_stats(b):
        slot = b % 2
        for r in range(1, n):
            stat_copy(slot, r).wait()
        parts = [stsrc_v[slot]] + [strcv_v[slot, r] for r in range(1, n)]
        top = parts[0][0:1]
        for p in parts[1:]:
            top = jnp.maximum(top, p[0:1])
        total = jnp.zeros_like(top)
        hit = jnp.zeros_like(top)
        for p in parts:
            total = total + p[1:2] * jnp.exp(p[0:1] - top)
            hit = hit + p[2:3]
        lse = top + jnp.log(total)
        w = wgt_v[pl.ds(b, 1), :]
        row_v[0:1, :] = jnp.where(w > 0.0, lse - jnp.log(jnp.where(w > 0.0, w, 1.0)), 3.0e38)
        row_v[1:2, :] = w
        tgt_v[pl.ds(8, 1), :] = tgt_v[pl.ds(b, 1), :]
        loss = (lse - hit) * msk_v[pl.ds(b, 1), :]
        loss_ref[pl.ds(b, 1), :] = loss
        tot_v[0:1, :] = tot_v[0:1, :] + loss / tot_v[1:2, :]

    def pair_copy(b):
        slot = b % 2
        return remote(dx_v.at[b % 3, 1 - core], pr_v.at[slot], pr_send.at[slot], pr_recv.at[slot], peer)

    def rs1(b):
        @pl.when(b >= 2)
        def _():
            pl.semaphore_wait(pair_free, 1)
        pair_copy(b).start()

    def crow(c):
        return pl.ds(pl.multiple_of(c * q, q), q)

    def r2_copies(b):
        mine, s3, mg, ow = dx_v.at[b % 3, core], b % 3, b % 4, b % 5
        return (remote(mine.at[0, crow(far_chip)], mg_v.at[mg, 0], r2_send.at[s3, 0], mg_recv.at[mg, 0], right),
                remote(mine.at[1, crow(far_chip)], mg_v.at[mg, 1], r2_send.at[s3, 1], mg_recv.at[mg, 1], left),
                remote(mine.at[1, crow(right_chip)], ow_v.at[ow, 0, 1], r2_send.at[s3, 2], ow_recv.at[ow, 0, 1], right),
                remote(mine.at[0, crow(left_chip)], ow_v.at[ow, 1, 0], r2_send.at[s3, 3], ow_recv.at[ow, 1, 0], left))

    def rs2(b):
        slot, s3 = b % 2, b % 3
        pair_copy(b).wait()

        def add(i, _):
            h = i // CHIPS
            c = i % CHIPS
            dx_v[s3, core, h, crow(c), :] += pr_v[slot, h, crow(c), :]
            return 0
        lax.fori_loop(0, 2 * CHIPS, add, 0)

        @pl.when(b < BLOCKS - 2)
        def _():
            pl.semaphore_signal(pair_free, inc=1, **to(peer))
        for c in r2_copies(b):
            c.start()

    def r3_copies(b):
        mine, s3, ow = dx_v.at[b % 3, core], b % 3, b % 5
        return (remote(mine.at[0, crow(right_chip)], ow_v.at[ow, 0, 0], r3_send.at[s3, 0], ow_recv.at[ow, 0, 0], right),
                remote(mine.at[1, crow(left_chip)], ow_v.at[ow, 1, 1], r3_send.at[s3, 1], ow_recv.at[ow, 1, 1], left))

    def rs3(b):
        s3, mg = b % 3, b % 4
        c2 = r2_copies(b)
        c2[0].wait_recv()
        c2[1].wait_recv()
        dx_v[s3, core, 0, crow(right_chip), :] += mg_v[mg, 0]
        dx_v[s3, core, 1, crow(left_chip), :] += mg_v[mg, 1]
        for c in r3_copies(b):
            c.start()

    def rs4(b):
        ow = b % 5
        c2, c3 = r2_copies(b), r3_copies(b)
        c2[2].wait_recv()
        c2[3].wait_recv()
        c3[0].wait_recv()
        c3[1].wait_recv()

        @pl.when(b >= 1)
        def _():
            out_copies(b - 1)[0].wait()
            out_copies(b - 1)[1].wait()
        for h in range(2):
            dy = dx_v[b % 3, core, h, crow(chip), :] + ow_v[ow, 0, h] + ow_v[ow, 1, h]
            a = own(b, h)[...].astype(F32)
            mean = jnp.mean(a, axis=-1, keepdims=True)
            cent = a - mean
            rstd = lax.rsqrt(jnp.mean(cent * cent, axis=-1, keepdims=True) + LN_EPS)
            xhat = cent * rstd
            gsrc_v[h:h + 1, :] += jnp.sum(dy * xhat, axis=0, keepdims=True)
            gsrc_v[2 + h:3 + h, :] += jnp.sum(dy, axis=0, keepdims=True)
            dxh = dy * gain_ref[h:h + 1, :]
            c1 = jnp.mean(dxh, axis=-1, keepdims=True)
            c2_ = jnp.mean(dxh * xhat, axis=-1, keepdims=True)
            da = rstd * (dxh - c1 - xhat * c2_)
            if h == 0:
                da_v[...] = da
            else:
                dg_v[b % 4] = da.astype(BF16)
        for c in out_copies(b):
            c.start()
        for c in c2 + c3:
            c.wait_send()

    def out_copies(b):
        return (pltpu.make_async_copy(da_v, da1_ref.at[b], out_sem.at[0]),
                pltpu.make_async_copy(dg_v.at[b % 4], dgown_ref.at[b], out_sem.at[1]))

    def xin_copy(i):
        sl = pl.ds(pl.multiple_of(i * nc, nc), nc)
        return pltpu.make_async_copy(xall_ref.at[:, sl], e_v.at[:, sl], xin_sem.at[i])

    def dzin_copies(c, odd):
        at = pl.ds(pl.multiple_of(c * re, re), re)
        if odd:
            return [pltpu.make_async_copy(dzt_ref.at[at, pl.ds(k * cols, cols)], dz_v.at[pl.ds(k * re, re)], dzin_sem.at[k])
                    for k in range(BLOCKS)]
        return [pltpu.make_async_copy(dzt_ref.at[at, pl.ds(k * depth, depth)], (a_v, x_v)[k], dzin_sem.at[BLOCKS + k])
                for k in range(2)]

    def de_copy(c, i):
        return pltpu.make_async_copy(
            z_v.at[pl.ds(pl.multiple_of(i * re, re), re)],
            de_ref.at[pl.ds(pl.multiple_of(c * re, re), re), pl.ds(pl.multiple_of(i * nc, nc), nc)], de_sem.at[i])

    def de_chunk(c, odd):
        for d in dzin_copies(c, odd):
            d.wait()

        def part(i, _):
            sl = pl.ds(pl.multiple_of(i * nc, nc), nc)

            @pl.when(c == 0)
            def _():
                xin_copy(i).wait()

            @pl.when(c >= 1)
            def _():
                de_copy(c - 1, i).wait()
            if odd:
                val = jnp.dot(dz_v[:re, :], e_v[:cols, sl], preferred_element_type=F32)
                for k in range(1, BLOCKS):
                    val = val + jnp.dot(dz_v[k * re:k * re + re, :], e_v[k * cols:k * cols + cols, sl], preferred_element_type=F32)
            else:
                val = jnp.dot(a_v[...], e_v[:depth, sl], preferred_element_type=F32)
                val = val + jnp.dot(x_v[...], e_v[depth:, sl], preferred_element_type=F32)
            z_v[pl.ds(pl.multiple_of(i * re, re), re), :] = val
            de_copy(c, i).start()
            return 0
        lax.fori_loop(0, npart, part, 0)

        @pl.when(c + 2 < KEEP)
        def _():
            for d in dzin_copies(c + 2, odd):
                d.start()

    def inside(b, fn, name='svc'):
        @pl.when(jnp.logical_and(b >= 0, b < BLOCKS))
        def _():
            with jax.named_scope(name):
                fn(b)

    def between(j, lo, hi, fn, name='svc'):
        @pl.when(jnp.logical_and(j >= lo, j <= hi))
        def _():
            with jax.named_scope(name):
                fn()

    def x_copy(b):
        return pltpu.make_async_copy(x_v, xall_ref.at[pl.ds(pl.multiple_of(b * cols, cols), cols)], x_sem)

    def dz_copy(b):
        return pltpu.make_async_copy(dz_v, dzt_ref.at[:, pl.ds(pl.multiple_of(b * cols, cols), cols)], dz_sem)

    def loop(k, fn):
        def body(i, _):
            fn(i)
            return 0
        lax.fori_loop(0, k, body, 0)

    ld_h.wait()
    in1(0, 0)
    in1(1, 0)
    ld_w.wait()
    project_own()
    ld_e[0].start()
    in1(0, 1)
    in1(1, 1)
    in2(0, 0)
    in2(1, 0)
    for r in range(1, n):
        code_copy(r).wait()
    code = code_ref[...]
    for r in range(1, n):
        code = code + crcv_v[r]
    mask = (code >= 65536).astype(jnp.int32)
    local = code - mask * 65536 - me * rows
    tgt_v[0:BLOCKS, :] = jnp.where(jnp.logical_and(local >= 0, local < rows), local, -(1 << 24))
    maskf = mask.astype(F32)
    msk_v[...] = maskf
    per_col = jnp.sum(maskf, axis=0, keepdims=True)
    n0 = jnp.sum(per_col[:, :tok], axis=1, keepdims=True)
    n1 = jnp.sum(per_col[:, tok:], axis=1, keepdims=True)
    counts = jnp.concatenate([jnp.broadcast_to(n0, (1, tok)), jnp.broadcast_to(n1, (1, tok))], axis=1)
    wgt_v[...] = maskf / counts
    tot_v[0:1, :] = jnp.zeros((1, cols), F32)
    tot_v[1:2, :] = counts
    gsrc_v[...] = jnp.zeros_like(gsrc_v)
    in3(0, 0)
    in2(0, 1)
    in3(0, 1)
    in2(1, 1)
    fetch_block(0)
    for c in ld_e:
        c.wait()

    def both(fn):
        def run(b):
            fn(b, 0)
            fn(b, 1)
        return run

    def last_stage(b):
        rs4(b)
        dg1(b)

    def gather_in(h):
        between(h, -2, BLOCKS - 5, lambda: both(in1)(h + 4), 'in1')
        between(h, -1, BLOCKS - 4, lambda: both(in2)(h + 3), 'in2')
        between(h, 0, BLOCKS - 3, lambda: both(in3)(h + 2), 'in3')

    def step(t, _):
        j = t - 1
        def block_wait():
            for c in block_copies(j + 1):
                c.wait()
        between(j, -1, BLOCKS - 2, block_wait, 'bwait')
        between(j, 1, BLOCKS, lambda: x_wait(j), 'xwait')

        def full_a():
            def body(i):
                dx_part(i, (j - 1) % 3)
                norm_part(i)
            loop(npart, body)
        between(j, -1, 0, lambda: loop(npart, norm_part), 'norm')
        between(j, 1, BLOCKS - 2, full_a, 'full_a')
        between(j, BLOCKS, BLOCKS, start_tail, 'start_tail')

        def last_a(i):
            dx_part(i, (j - 1) % 3)

            @pl.when(j == BLOCKS)
            def _():
                xin_copy(i).start()
        between(j, BLOCKS - 1, BLOCKS, lambda: loop(npart, last_a), 'last_a')
        between(j, BLOCKS + 1, BLOCKS + 3, lambda: de_chunk(2 * (j - BLOCKS) - 1, True), 'de_a')
        between(j, -1, BLOCKS - 2, lambda: x_copy(j + 1).start(), 'xstart')
        between(j, BLOCKS, BLOCKS, start_odd, 'start_odd')
        inside(j - 1, rs1, 'rs1')
        between(j, BLOCKS + 2, BLOCKS + 2, lambda: last_stage(BLOCKS - 1), 'rs4last')
        between(j, -1, -1, lambda: both(in3)(1), 'in3p')
        gather_in(2 * j)
        between(j, 5, BLOCKS + 3, lambda: dg3(j - 5), 'dg3')
        between(j, BLOCKS + 3, BLOCKS + 3, lambda: dg3(BLOCKS - 1), 'dg3last')
        inside(j, join_stats, 'join')
        between(j, 1, BLOCKS - 1, lambda: dz_copy(j - 1).wait(), 'dzwait')
        between(j, BLOCKS, BLOCKS + 2, lambda: de_chunk(2 * (j - BLOCKS), False), 'de_d')

        def start_stats():
            ms_v[0] = jnp.full((8, cols), -3.0e38, F32)
            ms_v[1] = jnp.zeros((8, cols), F32)
            ms_v[2] = jnp.zeros((8, cols), F32)
            tgt_v[pl.ds(9, 1), :] = tgt_v[pl.ds(j + 1, 1), :]
        between(j, -1, BLOCKS - 2, start_stats)

        between(j, -1, -1, lambda: loop(nr, lambda i: d_body(i, False, True)), 'only_z')
        between(j, 0, BLOCKS - 2, lambda: loop(nr, lambda i: d_body(i, True, True)), 'full_d')
        between(j, BLOCKS - 1, BLOCKS - 1, lambda: loop(nr, lambda i: d_body(i, True, False)), 'back')
        between(j, -1, BLOCKS - 3, lambda: fetch_block(j + 2), 'fetch')
        between(j, -1, BLOCKS - 2, lambda: send_stats(j + 1), 'stats')
        inside(j, lambda b: dz_copy(b).start(), 'dzstart')
        inside(j - 2, rs3, 'rs3')
        between(j, 3, BLOCKS + 1, lambda: last_stage(j - 3), 'rs4g1')
        between(j, 4, BLOCKS + 2, lambda: dg2(j - 4), 'dg2')
        gather_in(2 * j + 1)
        inside(j - 1, rs2, 'rs2')
        between(j, BLOCKS + 2, BLOCKS + 2, lambda: dg2(BLOCKS - 1), 'dg2last')
        between(j, BLOCKS + 2, BLOCKS + 2, gb_start, 'gbstart')
        return 0

    def gb_copy(r):
        return remote(gsrc_v, grcv_v.at[r], gb_send.at[r], gb_recv.at[r], (me + r) % n)

    def gb_start():
        for r in range(1, n):
            gb_copy(r).start()

    def start_tail():
        dz_copy(BLOCKS - 1).wait()
        for d in dzin_copies(0, False):
            d.start()

    def start_odd():
        for d in dzin_copies(1, True):
            d.start()

    def x_wait(j):
        @pl.when(j <= BLOCKS - 1)
        def _():
            x_copy(j).wait()

    def first_x(j):
        x_copy(j).wait()

    def step_outer(t, c):
        @pl.when(t == 1)
        def _():
            first_x(0)
        return step(t, c)

    lax.fori_loop(0, BLOCKS + 5, step_outer, 0)

    for b in range(BLOCKS):
        gather4(dgall_ref.at[b], g_send.at[b], g_recv.at[b])
    for c in out_copies(BLOCKS - 1):
        c.wait()
    total_ref[...] = jnp.broadcast_to(jnp.sum(tot_v[0:1, :], axis=1, keepdims=True), total_ref.shape)

    for i in range(npart):
        de_copy(KEEP - 1, i).wait()
    for r in range(1, n):
        gb_copy(r).wait()
    acc = gsrc_v[...]
    for r in range(1, n):
        acc = acc + grcv_v[r]
    dgb_ref[...] = acc


def stream(n, hidden, w_two, gain, bias, embed, code):
    tokens, depth = hidden.shape
    rows = embed.shape[0]
    q = tokens // BLOCKS
    half = CHIPS * q
    tok = 2 * half
    cols = 2 * tok
    nc = depth // 4
    rc, sub = rows // 2, rows // 8
    assert BLOCKS * cols == rows == 2 * depth and nc == cols
    dims = (n, q, depth, rows, rc, nc, sub)
    any_spec = pl.BlockSpec(memory_space=pl.ANY)
    vmem = pl.BlockSpec(memory_space=pltpu.VMEM)
    dma = pltpu.SemaphoreType.DMA
    sds = jax.ShapeDtypeStruct
    return pl.pallas_call(
        functools.partial(stream_kernel, dims),
        out_shape=(sds((BLOCKS, 2, 2, CHIPS, q, depth), BF16), sds((BLOCKS * cols, depth), BF16),
                   sds((rows, BLOCKS * cols), BF16), sds((BLOCKS, 2, CHIPS, q, depth), BF16),
                   sds((BLOCKS, q, depth), F32), sds((BLOCKS, q, depth), BF16),
                   sds((BLOCKS, cols), F32), sds((8, 128), F32), sds((8, depth), F32),
                   sds((KEEP * (rows // BLOCKS), depth), F32)),
        in_specs=[any_spec, any_spec, vmem, vmem, any_spec, vmem],
        out_specs=(any_spec,) * 6 + (vmem,) * 3 + (any_spec,),
        scratch_shapes=[
            pltpu.VMEM((rows, depth), BF16),
            pltpu.VMEM((cols, depth), BF16), pltpu.VMEM((cols, depth), BF16),
            pltpu.VMEM((rows, cols), F32), pltpu.VMEM((rows, cols), BF16),
            pltpu.VMEM((3, 2, 2, half, depth), F32), pltpu.VMEM((2, 2, half, depth), F32),
            pltpu.VMEM((4, 2, q, depth), F32), pltpu.VMEM((5, 2, 2, q, depth), F32),
            pltpu.VMEM((tokens, depth), BF16), pltpu.VMEM((tokens, depth), BF16),
            pltpu.VMEM((4, q, depth), BF16), pltpu.VMEM((q, depth), F32),
            pltpu.VMEM((2, 8, cols), F32), pltpu.VMEM((2, n, 8, cols), F32),
            pltpu.VMEM((n, BLOCKS, cols), jnp.int32), pltpu.VMEM((16, cols), jnp.int32),
            pltpu.VMEM((BLOCKS, cols), F32), pltpu.VMEM((BLOCKS, cols), F32),
            pltpu.VMEM((3, 8, cols), F32), pltpu.VMEM((8, cols), F32), pltpu.VMEM((8, cols), F32),
            pltpu.VMEM((8, depth), F32), pltpu.VMEM((n, 8, depth), F32),
            dma((4,)), dma((BLOCKS, 2, 8)), dma((BLOCKS, 2, 8)), dma((BLOCKS, 2)), dma((BLOCKS, 8)), dma((BLOCKS, 8)),
            dma((BLOCKS,)), dma((2, n)), dma((2, n)), dma((2,)), dma((2,)), dma((3, 4)), dma((3, 2)),
            dma((4, 2)), dma((5, 2, 2)), pltpu.SemaphoreType.REGULAR,
            dma((n,)), dma((n,)), dma, dma, dma((4 * CHIPS,)), dma((2,)), dma((n,)), dma((n,)),
            dma((depth // nc,)), dma((BLOCKS + 2,)), dma((depth // nc,)),
        ],
        compiler_params=pltpu.CompilerParams(collective_id=0, has_side_effects=True, vmem_limit_bytes=67043328),
        name='stream',
    )(hidden, w_two, gain, bias, embed, code)


def dense_kernel(part_ref, dzt_ref, xall_ref, aall_ref, gall_ref, da_ref, go_ref, w_ref, loss_ref, sum_ref, dgb_ref,
                 de_ref, dw_ref, dh_ref, tl_ref, total_ref, gs_ref, gb_ref,
                 da_v, go_v, w_v, g_v, x_v, h_v, dw_v, dz_v, de_v, st_v, w_sem, g_sem, x_sem, h_sem, dw_sem, dz_sem, de_sem, in_sem, out_sem, a_sem):
    depth = x_v.shape[1]
    nc, wb = depth // 4, depth // BLOCKS
    re = dzt_ref.shape[0] // BLOCKS
    xr = x_v.shape[0] // BLOCKS
    todo = BLOCKS - KEEP
    pieces = BLOCKS + 4 * todo
    pr = KEEP * re // pieces

    def at(i, size):
        return pl.ds(pl.multiple_of(i * size, size), size)

    def w_copy(i):
        return pltpu.make_async_copy(w_ref.at[at(i, nc)], w_v.at[at(i, nc)], w_sem.at[i])

    def h_copy(i):
        return pltpu.make_async_copy(aall_ref.at[:, 0:h_v.shape[2], at(i, wb)], h_v.at[i % 2], h_sem.at[i % 2])

    def dw_copy(i):
        return pltpu.make_async_copy(dw_v.at[i % 2], dw_ref.at[at(i, wb)], dw_sem.at[i % 2])

    def x_copy(i):
        return pltpu.make_async_copy(xall_ref.at[at(i, xr)], x_v.at[at(i, xr)], x_sem.at[i])

    def dz_copy(c):
        return pltpu.make_async_copy(dzt_ref.at[at(KEEP + c, re)], dz_v.at[c % 2], dz_sem.at[c % 2])

    def de_copy(u):
        return pltpu.make_async_copy(de_v.at[u % 2], de_ref.at[at(KEEP + u // 4, re), at(u % 4, nc)], de_sem.at[u % 2])

    def pin(t):
        return pltpu.make_async_copy(part_ref.at[at(t, pr)], st_v.at[t % 4], in_sem.at[t % 4])

    def pout(t):
        return pltpu.make_async_copy(st_v.at[t % 4], de_ref.at[at(t, pr)], out_sem.at[t % 4])

    def carry(t):
        pin(t).wait()
        pout(t).start()

        @pl.when(t >= 2)
        def _():
            pout(t - 2).wait()

        @pl.when(t + 2 < pieces)
        def _():
            pin(t + 2).start()

    g_load = pltpu.make_async_copy(gall_ref, g_v, g_sem)
    da_load = pltpu.make_async_copy(da_ref, da_v, a_sem.at[0])
    go_load = pltpu.make_async_copy(go_ref, go_v, a_sem.at[1])
    go_load.start()
    w_copy(0).start()
    da_load.start()
    for i in range(1, 4):
        w_copy(i).start()
    g_load.start()
    h_copy(0).start()
    h_copy(1).start()
    pin(0).start()
    pin(1).start()

    gs_ref[...] = dgb_ref[0:2, :]
    gb_ref[...] = dgb_ref[2:4, :]
    total_ref[0] = sum_ref[0, 0]
    me = lax.axis_index('tp')
    lanes = loss_ref.shape[1]
    q = lanes // 2 // (2 * CHIPS)
    place = (me % 2) * CHIPS + me // 2
    for h in range(2):
        turned = pltpu.roll(loss_ref[...], (lanes - h * (lanes // 2) - place * q) % lanes, 1)
        tl_ref[h:h + 1, :] = jnp.concatenate([turned[b:b + 1, :q] for b in range(BLOCKS)], axis=1)
    go_load.wait()
    da_load.wait()

    def hidden_part(i, _):
        w_copy(i).wait()
        sl = at(i, nc)
        back = lax.dot_general(go_v[...], w_v[sl, :], (((1,), (1,)), ((), ())), preferred_element_type=F32)
        dh_ref[:, sl] = (da_v[:, sl] + back).astype(BF16)
        return 0
    with jax.named_scope('k2_dh'):
        lax.fori_loop(0, 4, hidden_part, 0)
    with jax.named_scope('k2_g'):
        g_load.wait()

    def dw_part(i, _):
        h_copy(i).wait()
        x_copy(i).start()

        @pl.when(i == BLOCKS - 2)
        def _():
            dz_copy(0).start()
            dz_copy(1).start()
        carry(i)

        @pl.when(i >= 2)
        def _():
            dw_copy(i - 2).wait()
        h = h_v[i % 2].reshape(g_v.shape[0], wb)
        dw_v[i % 2] = lax.dot_general(h, g_v[...], (((0,), (0,)), ((), ())), preferred_element_type=F32)
        dw_copy(i).start()

        @pl.when(i + 2 < BLOCKS)
        def _():
            h_copy(i + 2).start()
        return 0
    with jax.named_scope('k2_dw'):
        lax.fori_loop(0, BLOCKS, dw_part, 0)
    with jax.named_scope('k2_x'):
        for i in range(BLOCKS):
            x_copy(i).wait()

    def de_part(u, _):
        c = u // 4

        @pl.when(u % 4 == 0)
        def _():
            dz_copy(c).wait()
        carry(BLOCKS + u)

        @pl.when(u >= 2)
        def _():
            de_copy(u - 2).wait()
        de_v[u % 2] = jnp.dot(dz_v[c % 2], x_v[:, at(u % 4, nc)], preferred_element_type=F32)
        de_copy(u).start()

        @pl.when(jnp.logical_and(u % 4 == 3, c + 2 < todo))
        def _():
            dz_copy(c + 2).start()
        return 0
    with jax.named_scope('k2_de'):
        lax.fori_loop(0, 4 * todo, de_part, 0)
    for i in (BLOCKS - 2, BLOCKS - 1):
        dw_copy(i).wait()
    for i in (4 * todo - 2, 4 * todo - 1):
        de_copy(i).wait()
    for t in (pieces - 2, pieces - 1):
        pout(t).wait()


def dense(part, dzt, xall, aall, gall, da1, dgown, w_two, loss, total_loss, dgb):
    rows, kk = dzt.shape
    depth = xall.shape[1]
    total, tokens = gall.shape[0], da1.shape[0]
    re, wb, nc = rows // BLOCKS, depth // BLOCKS, depth // 4
    pieces = BLOCKS + 4 * (BLOCKS - KEEP)
    sds = jax.ShapeDtypeStruct
    dma = pltpu.SemaphoreType.DMA
    any_spec = pl.BlockSpec(memory_space=pl.ANY)
    vmem = pl.BlockSpec(memory_space=pltpu.VMEM)
    return pl.pallas_call(
        dense_kernel,
        out_shape=(sds((rows, depth), F32), sds((depth, depth), F32), sds((tokens, depth), BF16), sds((2, tokens), F32),
                   sds((1,), F32), sds((2, depth), F32), sds((2, depth), F32)),
        in_specs=[any_spec] * 8 + [vmem] * 3,
        out_specs=(any_spec, any_spec, vmem, vmem, pl.BlockSpec(memory_space=pltpu.SMEM), vmem, vmem),
        scratch_shapes=[pltpu.VMEM((tokens, depth), F32), pltpu.VMEM((tokens, depth), BF16), pltpu.VMEM((depth, depth), BF16), pltpu.VMEM((total, depth), BF16), pltpu.VMEM((kk, depth), BF16),
                        pltpu.VMEM((2, BLOCKS, total // BLOCKS, wb), BF16), pltpu.VMEM((2, wb, depth), F32),
                        pltpu.VMEM((2, re, kk), BF16), pltpu.VMEM((2, re, nc), F32),
                        pltpu.VMEM((4, KEEP * re // pieces, depth), F32),
                        dma((4,)), dma, dma((BLOCKS,)), dma((2,)), dma((2,)), dma((2,)), dma((2,)), dma((4,)), dma((4,)), dma((2,))],
        compiler_params=pltpu.CompilerParams(vmem_limit_bytes=67043328),
        name='dense',
    )(part, dzt, xall, aall, gall, da1, dgown, w_two, loss, total_loss, dgb)


def solution(mesh):
    n = mesh.shape['tp']
    tok_spec = P(('dp', 'tp'), None)
    row_spec = P(None, ('dp', 'tp'))

    def device_step(hidden, w_two, ln_scale, ln_shift, embed, targets, loss_mask):
        tokens, depth = hidden.shape
        q = tokens // BLOCKS
        me = lax.axis_index('tp')
        code = (targets + 65536 * loss_mask).reshape(2, BLOCKS, q).transpose(1, 0, 2)
        place = (me % 2) * CHIPS + me // 2
        seat = lax.broadcasted_iota(jnp.int32, (1, 1, 2 * CHIPS, 1), 2) == place
        code = jnp.where(seat, code[:, :, None, :], 0).reshape(BLOCKS, 2 * 2 * CHIPS * q)
        aall, xall, dzt, dgall, da1, dgown, loss, total, dgb, part = stream(
            n, hidden, w_two, ln_scale, ln_shift, embed, code)
        d_embed, d_w, d_hidden, token_loss, total_loss, d_scale, d_shift = dense(
            part, dzt, xall, aall.reshape(BLOCKS, 2 * n * q, depth), dgall.reshape(n * tokens, depth),
            da1.reshape(tokens, depth), dgown.reshape(tokens, depth), w_two, loss, total, dgb)
        return token_loss, total_loss, d_hidden, d_embed, d_w, d_scale, d_shift

    return jax.shard_map(device_step, mesh=mesh,
                         in_specs=(tok_spec, P(), P(), P(), P('tp', None), row_spec, row_spec),
                         out_specs=(row_spec, P('dp'), tok_spec, tok_spec, P('dp', None), P('dp', None), P('dp', None)),
                         check_vma=False)
```

```python
import functools

import jax
import jax.numpy as jnp
from jax import lax
from jax.experimental import pallas as pl
from jax.experimental.pallas import tpu as pltpu
from jax.sharding import PartitionSpec as P

LN_EPS = 1e-5
CHIPS = 4
BLOCKS = 8
KEEP = 6
WAYS = 4
LANES = 2
F32 = jnp.float32
BF16 = jnp.bfloat16


def to(idx):
    return dict(device_id={'tp': idx}, device_id_type=pl.DeviceIdType.MESH)


def remote(src, dst, send, recv, idx):
    return pltpu.make_async_remote_copy(src_ref=src, dst_ref=dst, send_sem=send, recv_sem=recv, **to(idx))


def stream_kernel(dims, h_ref, w_ref, gain_ref, bias_ref, e_ref, code_ref,
                  aall_ref, xall_ref, dzt_ref, dgall_ref, da1_ref, dgown_ref, loss_ref, total_ref, dgb_ref, de_ref,
                  e_v, a_v, x_v, z_v, dz_v, dx_v, pr_v, mg_v, ow_v, own_v, dg_v, da_v,
                  stsrc_v, strcv_v, crcv_v, tgt_v, msk_v, wgt_v, ms_v, row_v, tot_v, gsrc_v, grcv_v,
                  ld_sem, h_send, h_recv, h_loc, g_send, g_recv, g_loc,
                  st_send, st_recv, pr_send, pr_recv, r2_send, r3_send, mg_recv, ow_recv, pair_free,
                  cd_send, cd_recv, x_sem, dz_sem, a_sem, out_sem, gb_send, gb_recv, xin_sem, dzin_sem, de_sem):
    n, q, depth, rows, rc, nc, sub = dims
    re = rows // BLOCKS
    half = CHIPS * q
    tok = 2 * half
    cols = 2 * tok
    me = lax.axis_index('tp')
    chip = me // 2
    core = me % 2
    peer = me + 1 - 2 * core
    right_chip = (chip + 1) % CHIPS
    left_chip = (chip + CHIPS - 1) % CHIPS
    far_chip = (chip + 2) % CHIPS
    right = right_chip * 2 + core
    left = left_chip * 2 + core

    top, bottom = pl.ds(0, depth), pl.ds(depth, rows - depth)
    ld_e = [pltpu.make_async_copy(e_ref.at[d], e_v.at[d], ld_sem.at[i]) for i, d in ((0, top), (3, bottom))]
    ld_w = pltpu.make_async_copy(w_ref, e_v.at[top], ld_sem.at[1])
    ld_h = pltpu.make_async_copy(h_ref, own_v.at[0], ld_sem.at[2])
    ld_h.start()
    ld_w.start()

    barrier = pltpu.get_barrier_semaphore()
    for r in range(1, n):
        pl.semaphore_signal(barrier, inc=1, **to((me + r) % n))
    pl.semaphore_wait(barrier, n - 1)

    def code_copy(r):
        return remote(code_ref, crcv_v.at[r], cd_send.at[r], cd_recv.at[r], (me + r) % n)

    for r in range(1, n):
        code_copy(r).start()

    lo, hi = pl.ds(0, q // 2), pl.ds(q // 2, q // 2)

    def g1_copies(src, dst, send, recv):
        piece = dst.at[core, chip]
        return (remote(src, piece, send.at[0], recv.at[0], right),
                remote(src, piece, send.at[1], recv.at[1], left),
                remote(src, piece, send.at[2], recv.at[4], peer))

    def g2_copies(dst, send, recv):
        fl, fr = dst.at[core, left_chip], dst.at[core, right_chip]
        return (remote(fl.at[lo], fl.at[lo], send.at[3], recv.at[2], right),
                remote(fr.at[hi], fr.at[hi], send.at[4], recv.at[3], left),
                remote(fl, fl, send.at[5], recv.at[5], peer),
                remote(fr, fr, send.at[6], recv.at[6], peer))

    def g3_copies(dst, send, recv):
        far = dst.at[core, far_chip]
        return (remote(far, far, send.at[7], recv.at[7], peer),)

    def gather1(src, dst, send, recv, loc):
        for c in g1_copies(src, dst, send, recv):
            c.start()
        pltpu.make_async_copy(src, dst.at[core, chip], loc).start()

    def gather2(src, dst, send, recv, loc):
        remote(src, dst.at[core, left_chip], send.at[0], recv.at[0], right).wait_recv()
        remote(src, dst.at[core, right_chip], send.at[1], recv.at[1], left).wait_recv()
        for c in g2_copies(dst, send, recv):
            c.start()
        for c in g1_copies(src, dst, send, recv):
            c.wait_send()
        pltpu.make_async_copy(src, dst.at[core, chip], loc).wait()

    def gather3(dst, send, recv):
        far = dst.at[core, far_chip]
        remote(far.at[lo], far.at[lo], send.at[3], recv.at[2], right).wait_recv()
        remote(far.at[hi], far.at[hi], send.at[4], recv.at[3], left).wait_recv()
        for c in g3_copies(dst, send, recv):
            c.start()
        for c in g2_copies(dst, send, recv):
            c.wait_send()

    def gather4(dst, send, recv):
        for i, c in enumerate((chip, left_chip, right_chip, far_chip)):
            piece = dst.at[1 - core, c]
            remote(piece, piece, send.at[7], recv.at[4 + i], peer).wait_recv()
        for c in g3_copies(dst, send, recv):
            c.wait_send()

    def own(b, h):
        return own_v.at[h, pl.ds(pl.multiple_of(b * q, q), q)]

    def in1(b, h):
        gather1(own(b, h), aall_ref.at[b, h], h_send.at[b, h], h_recv.at[b, h], h_loc.at[b, h])

    def in2(b, h):
        gather2(own(b, h), aall_ref.at[b, h], h_send.at[b, h], h_recv.at[b, h], h_loc.at[b, h])

    def in3(b, h):
        gather3(aall_ref.at[b, h], h_send.at[b, h], h_recv.at[b, h])

    def dg1(b):
        gather1(dg_v.at[b % 4], dgall_ref.at[b], g_send.at[b], g_recv.at[b], g_loc.at[b])

    def dg2(b):
        gather2(dg_v.at[b % 4], dgall_ref.at[b], g_send.at[b], g_recv.at[b], g_loc.at[b])

    def dg3(b):
        gather3(dgall_ref.at[b], g_send.at[b], g_recv.at[b])

    def both(fn):
        def run(b):
            def body(h, _):
                fn(b, h)
                return 0
            lax.fori_loop(0, 2, body, 0)
        return run

    def a_copy(b, h, kk, c):
        at = pl.ds(((h * 2 + kk) * CHIPS + c) * q, q)
        return pltpu.make_async_copy(aall_ref.at[b, h, kk, c], a_v.at[at], a_sem.at[(h * 2 + kk) * CHIPS + c])

    def block_copies(b):
        return [a_copy(b, h, kk, c) for h in range(2) for kk in range(2) for c in range(CHIPS)]

    def fetch_block(b):
        for h in range(2):
            gather4(aall_ref.at[b, h], h_send.at[b, h], h_recv.at[b, h])
        for c in block_copies(b):
            c.start()

    def project_own():
        def proj(i, _):
            sl = pl.ds(pl.multiple_of(i * nc, nc), nc)
            own_v[1, :, sl] = jnp.dot(own_v[0], e_v[top, sl], preferred_element_type=F32).astype(BF16)
            return 0
        lax.fori_loop(0, depth // nc, proj, 0)

    def norm_rows(start, head):
        a = a_v[pl.ds(start, 16), :].astype(F32)
        mean = jnp.mean(a, axis=-1, keepdims=True)
        cent = a - mean
        var = jnp.mean(cent * cent, axis=-1, keepdims=True)
        y = cent * lax.rsqrt(var + LN_EPS) * gain_ref[pl.ds(head, 1), :] + bias_ref[pl.ds(head, 1), :]
        x_v[pl.ds(start, 16), :] = y.astype(BF16)

    npart = depth // nc
    lrows = cols // npart

    def norm_part(i):
        head = (i * lrows) // tok
        for s in range(lrows // 16):
            norm_rows(pl.multiple_of(i * lrows + s * 16, 16), head)

    def dx_part(i, slot):
        sl = pl.ds(pl.multiple_of(i * nc, nc), nc)
        val = lax.dot_general(dz_v[...], e_v[:, sl], (((0,), (0,)), ((), ())), preferred_element_type=F32)
        for h in range(2):
            for kk in range(2):
                base = h * tok + kk * half
                dx_v[slot, kk, h, :, sl] = val[base:base + half, :]

    nr = rows // rc

    def tree(parts, op):
        while len(parts) > 1:
            parts = [op(a, b) for a, b in zip(parts[::2], parts[1::2])]
        return parts[0]

    def part_view(ref, i):
        return ref.at[pl.ds(pl.multiple_of(i * rc, rc), rc)]

    def back_part(i, p, lanes, td):
        shift, w = row_v[0:1, lanes], row_v[1:2, lanes]
        zc, dc = part_view(z_v, i), part_view(dz_v, i)
        for s in range(p * sub, p * sub + sub, 16):
            both = []
            for t in (s, s + 8):
                pw = jnp.exp(zc[t:t + 8, lanes] - shift)
                both.append(jnp.where(td == t, pw - w, pw))
            dc[s:s + 16, lanes] = jnp.concatenate(both, axis=0).astype(BF16)

    def z_part(i, p):
        ec = part_view(e_v, i)
        part_view(z_v, i)[p * sub:p * sub + sub, :] = lax.dot_general(
            ec[p * sub:p * sub + sub, :], x_v[...], (((1,), (1,)), ((), ())), preferred_element_type=F32)

    def stat_part(i, p, lanes, td, state):
        zc = part_view(z_v, i)
        m_old, acc, tl = state
        at = range(p * sub, p * sub + sub, 8)
        tops = [zc[s:s + 8, lanes] for s in at[:WAYS]]
        for k, s in enumerate(at[WAYS:]):
            tops[k % WAYS] = jnp.maximum(tops[k % WAYS], zc[s:s + 8, lanes])
        m = jnp.maximum(m_old, tree(tops, jnp.maximum))
        accs = [None] * WAYS
        for k, s in enumerate(at):
            z = zc[s:s + 8, lanes]
            e = jnp.exp(z - m)
            accs[k % WAYS] = e if accs[k % WAYS] is None else accs[k % WAYS] + e
            tl = jnp.where(td == s, z, tl)
        return m, acc * jnp.exp(m_old - m) + tree(accs, jnp.add), tl

    def d_body(i, back, new):
        span = cols // LANES
        iota = lax.broadcasted_iota(jnp.int32, (8, span), 0)
        cut = [slice(k * span, k * span + span) for k in range(LANES)]
        td_old = [tgt_v[pl.ds(8, 1), c] - i * rc - iota for c in cut]
        td_new = [tgt_v[pl.ds(9, 1), c] - i * rc - iota for c in cut]
        state = [tuple(ms_v[k, :, c] for k in range(3)) for c in cut]
        for p in range(rc // sub):
            if back:
                for k in range(LANES):
                    back_part(i, p, cut[k], td_old[k])
            if new:
                z_part(i, p)
                for k in range(LANES):
                    state[k] = stat_part(i, p, cut[k], td_new[k], state[k])
        if new:
            for k in range(LANES):
                for q_ in range(3):
                    ms_v[q_, :, cut[k]] = state[k][q_]

    def stat_copy(slot, r):
        return remote(stsrc_v.at[slot], strcv_v.at[slot, r], st_send.at[slot, r], st_recv.at[slot, r], (me + r) % n)

    def send_stats(b):
        slot = b % 2
        m = ms_v[0]
        top = jnp.max(m, axis=0, keepdims=True)
        stsrc_v[slot, 0:1, :] = top
        stsrc_v[slot, 1:2, :] = jnp.sum(ms_v[1] * jnp.exp(m - top), axis=0, keepdims=True)
        stsrc_v[slot, 2:3, :] = jnp.sum(ms_v[2], axis=0, keepdims=True)
        for r in range(1, n):
            stat_copy(slot, r).start()

    def join_stats(b):
        slot = b % 2
        for r in range(1, n):
            stat_copy(slot, r).wait()
        parts = [stsrc_v[slot]] + [strcv_v[slot, r] for r in range(1, n)]
        top = parts[0][0:1]
        for p in parts[1:]:
            top = jnp.maximum(top, p[0:1])
        total = jnp.zeros_like(top)
        hit = jnp.zeros_like(top)
        for p in parts:
            total = total + p[1:2] * jnp.exp(p[0:1] - top)
            hit = hit + p[2:3]
        lse = top + jnp.log(total)
        w = wgt_v[pl.ds(b, 1), :]
        row_v[0:1, :] = jnp.where(w > 0.0, lse - jnp.log(jnp.where(w > 0.0, w, 1.0)), 3.0e38)
        row_v[1:2, :] = w
        tgt_v[pl.ds(8, 1), :] = tgt_v[pl.ds(b, 1), :]
        loss = (lse - hit) * msk_v[pl.ds(b, 1), :]
        loss_ref[pl.ds(b, 1), :] = loss
        tot_v[0:1, :] = tot_v[0:1, :] + loss / tot_v[1:2, :]

    def pair_copy(b):
        slot = b % 2
        return remote(dx_v.at[b % 3, 1 - core], pr_v.at[slot], pr_send.at[slot], pr_recv.at[slot], peer)

    def rs1(b):
        @pl.when(b >= 2)
        def _():
            pl.semaphore_wait(pair_free, 1)
        pair_copy(b).start()

    def crow(c):
        return pl.ds(pl.multiple_of(c * q, q), q)

    def r2_copies(b):
        mine, s3, mg, ow = dx_v.at[b % 3, core], b % 3, b % 4, b % 5
        return (remote(mine.at[0, crow(far_chip)], mg_v.at[mg, 0], r2_send.at[s3, 0], mg_recv.at[mg, 0], right),
                remote(mine.at[1, crow(far_chip)], mg_v.at[mg, 1], r2_send.at[s3, 1], mg_recv.at[mg, 1], left),
                remote(mine.at[1, crow(right_chip)], ow_v.at[ow, 0, 1], r2_send.at[s3, 2], ow_recv.at[ow, 0, 1], right),
                remote(mine.at[0, crow(left_chip)], ow_v.at[ow, 1, 0], r2_send.at[s3, 3], ow_recv.at[ow, 1, 0], left))

    def rs2(b):
        slot, s3 = b % 2, b % 3
        pair_copy(b).wait()

        def add(i, _):
            h = i // CHIPS
            c = i % CHIPS
            dx_v[s3, core, h, crow(c), :] += pr_v[slot, h, crow(c), :]
            return 0
        lax.fori_loop(0, 2 * CHIPS, add, 0)

        @pl.when(b < BLOCKS - 2)
        def _():
            pl.semaphore_signal(pair_free, inc=1, **to(peer))
        for c in r2_copies(b):
            c.start()

    def r3_copies(b):
        mine, s3, ow = dx_v.at[b % 3, core], b % 3, b % 5
        return (remote(mine.at[0, crow(right_chip)], ow_v.at[ow, 0, 0], r3_send.at[s3, 0], ow_recv.at[ow, 0, 0], right),
                remote(mine.at[1, crow(left_chip)], ow_v.at[ow, 1, 1], r3_send.at[s3, 1], ow_recv.at[ow, 1, 1], left))

    def rs3(b):
        s3, mg = b % 3, b % 4
        c2 = r2_copies(b)
        c2[0].wait_recv()
        c2[1].wait_recv()
        dx_v[s3, core, 0, crow(right_chip), :] += mg_v[mg, 0]
        dx_v[s3, core, 1, crow(left_chip), :] += mg_v[mg, 1]
        for c in r3_copies(b):
            c.start()

    def rs4(b):
        ow = b % 5
        c2, c3 = r2_copies(b), r3_copies(b)
        c2[2].wait_recv()
        c2[3].wait_recv()
        c3[0].wait_recv()
        c3[1].wait_recv()

        @pl.when(b >= 1)
        def _():
            out_copies(b - 1)[0].wait()
            out_copies(b - 1)[1].wait()
        for h in range(2):
            dy = dx_v[b % 3, core, h, crow(chip), :] + ow_v[ow, 0, h] + ow_v[ow, 1, h]
            a = own(b, h)[...].astype(F32)
            mean = jnp.mean(a, axis=-1, keepdims=True)
            cent = a - mean
            rstd = lax.rsqrt(jnp.mean(cent * cent, axis=-1, keepdims=True) + LN_EPS)
            xhat = cent * rstd
            gsrc_v[h:h + 1, :] += jnp.sum(dy * xhat, axis=0, keepdims=True)
            gsrc_v[2 + h:3 + h, :] += jnp.sum(dy, axis=0, keepdims=True)
            dxh = dy * gain_ref[h:h + 1, :]
            c1 = jnp.mean(dxh, axis=-1, keepdims=True)
            c2_ = jnp.mean(dxh * xhat, axis=-1, keepdims=True)
            da = rstd * (dxh - c1 - xhat * c2_)
            if h == 0:
                da_v[...] = da
            else:
                dg_v[b % 4] = da.astype(BF16)
        for c in out_copies(b):
            c.start()
        for c in c2 + c3:
            c.wait_send()

    def out_copies(b):
        return (pltpu.make_async_copy(da_v, da1_ref.at[b], out_sem.at[0]),
                pltpu.make_async_copy(dg_v.at[b % 4], dgown_ref.at[b], out_sem.at[1]))

    def xin_copy(i):
        sl = pl.ds(pl.multiple_of(i * nc, nc), nc)
        return pltpu.make_async_copy(xall_ref.at[:, sl], e_v.at[:, sl], xin_sem.at[i])

    def dzin_copies(c, odd):
        at = pl.ds(pl.multiple_of(c * re, re), re)
        if odd:
            return [pltpu.make_async_copy(dzt_ref.at[at, pl.ds(k * cols, cols)], dz_v.at[pl.ds(k * re, re)], dzin_sem.at[k])
                    for k in range(BLOCKS)]
        return [pltpu.make_async_copy(dzt_ref.at[at, pl.ds(k * depth, depth)], (a_v, x_v)[k], dzin_sem.at[BLOCKS + k])
                for k in range(2)]

    def de_copy(c, i):
        return pltpu.make_async_copy(
            z_v.at[pl.ds(pl.multiple_of(i * re, re), re)],
            de_ref.at[pl.ds(pl.multiple_of(c * re, re), re), pl.ds(pl.multiple_of(i * nc, nc), nc)], de_sem.at[i])

    def de_chunk(c, odd):
        for d in dzin_copies(c, odd):
            d.wait()

        def part(i, _):
            sl = pl.ds(pl.multiple_of(i * nc, nc), nc)

            @pl.when(c == 0)
            def _():
                xin_copy(i).wait()

            @pl.when(c >= 1)
            def _():
                de_copy(c - 1, i).wait()
            if odd:
                val = jnp.dot(dz_v[:re, :], e_v[:cols, sl], preferred_element_type=F32)
                for k in range(1, BLOCKS):
                    val = val + jnp.dot(dz_v[k * re:k * re + re, :], e_v[k * cols:k * cols + cols, sl], preferred_element_type=F32)
            else:
                val = jnp.dot(a_v[...], e_v[:depth, sl], preferred_element_type=F32)
                val = val + jnp.dot(x_v[...], e_v[depth:, sl], preferred_element_type=F32)
            z_v[pl.ds(pl.multiple_of(i * re, re), re), :] = val
            de_copy(c, i).start()
            return 0
        lax.fori_loop(0, npart, part, 0)

        @pl.when(c + 2 < KEEP)
        def _():
            for d in dzin_copies(c + 2, odd):
                d.start()

    def inside(b, fn, name='svc'):
        @pl.when(jnp.logical_and(b >= 0, b < BLOCKS))
        def _():
            with jax.named_scope(name):
                fn(b)

    def between(j, lo, hi, fn, name='svc'):
        @pl.when(jnp.logical_and(j >= lo, j <= hi))
        def _():
            with jax.named_scope(name):
                fn()

    def x_copy(b):
        return pltpu.make_async_copy(x_v, xall_ref.at[pl.ds(pl.multiple_of(b * cols, cols), cols)], x_sem)

    def dz_copy(b):
        return pltpu.make_async_copy(dz_v, dzt_ref.at[:, pl.ds(pl.multiple_of(b * cols, cols), cols)], dz_sem)

    def loop(k, fn):
        def body(i, _):
            fn(i)
            return 0
        lax.fori_loop(0, k, body, 0)

    with jax.named_scope('p_h'):
        ld_h.wait()
    in1(0, 0)
    with jax.named_scope('p_w'):
        ld_w.wait()
    ld_e[1].start()
    with jax.named_scope('p_proj'):
        project_own()
    ld_e[0].start()
    in1(0, 1)
    with jax.named_scope('p_in2'):
        in2(0, 0)
    with jax.named_scope('p_code'):
        for r in range(1, n):
            code_copy(r).wait()
    code = code_ref[...]
    for r in range(1, n):
        code = code + crcv_v[r]
    mask = (code >= 65536).astype(jnp.int32)
    local = code - mask * 65536 - me * rows
    tgt_v[0:BLOCKS, :] = jnp.where(jnp.logical_and(local >= 0, local < rows), local, -(1 << 24))
    maskf = mask.astype(F32)
    msk_v[...] = maskf
    per_col = jnp.sum(maskf, axis=0, keepdims=True)
    n0 = jnp.sum(per_col[:, :tok], axis=1, keepdims=True)
    n1 = jnp.sum(per_col[:, tok:], axis=1, keepdims=True)
    counts = jnp.concatenate([jnp.broadcast_to(n0, (1, tok)), jnp.broadcast_to(n1, (1, tok))], axis=1)
    wgt_v[...] = maskf / counts
    tot_v[0:1, :] = jnp.zeros((1, cols), F32)
    tot_v[1:2, :] = counts
    gsrc_v[...] = jnp.zeros_like(gsrc_v)
    with jax.named_scope('p_in2b'):
        in2(0, 1)
    for b in (1, 2):
        both(in1)(b)
    with jax.named_scope('p_in3'):
        both(in3)(0)
    with jax.named_scope('p_fetch'):
        fetch_block(0)
    for c in ld_e:
        c.wait()

    def last_stage(b):
        rs4(b)
        dg1(b)

    def gather_in(p):
        inside(p + 3, both(in1), 'in1')
        inside(p + 2, both(in2), 'in2')
        inside(p + 1, both(in3), 'in3')

    def gather_first():
        both(in2)(1)
        both(in1)(3)

    def gather_second():
        both(in3)(1)
        both(in2)(2)

    def gather_third():
        both(in3)(2)
        both(in2)(3)
        both(in1)(4)

    def step(t, _):
        j = t - 1
        def block_wait():
            for c in block_copies(j + 1):
                c.wait()
        between(j, -1, BLOCKS - 2, block_wait, 'bwait')
        between(j, 1, BLOCKS, lambda: x_wait(j), 'xwait')

        def full_a():
            def body(i):
                dx_part(i, (j - 1) % 3)
                norm_part(i)
            loop(npart, body)
        between(j, -1, 0, lambda: loop(npart, norm_part), 'norm')
        between(j, 1, BLOCKS - 2, full_a, 'full_a')
        between(j, BLOCKS, BLOCKS, start_tail, 'start_tail')

        def last_a(i):
            dx_part(i, (j - 1) % 3)

            @pl.when(j == BLOCKS)
            def _():
                xin_copy(i).start()
        between(j, BLOCKS - 1, BLOCKS, lambda: loop(npart, last_a), 'last_a')
        between(j, BLOCKS + 1, BLOCKS + 3, lambda: de_chunk(2 * (j - BLOCKS) - 1, True), 'de_a')
        between(j, -1, BLOCKS - 2, lambda: x_copy(j + 1).start(), 'xstart')
        between(j, BLOCKS, BLOCKS, start_odd, 'start_odd')
        inside(j - 1, rs1, 'rs1')
        between(j, -1, -1, gather_first, 'gfirst')
        between(j, 1, 2, lambda: gather_in(2 * j + 1))
        between(j, 1, BLOCKS - 3, lambda: fetch_block(j + 2), 'fetch')
        def last_dg3():
            dg3(BLOCKS - 2)
            dg3(BLOCKS - 1)
        between(j, BLOCKS + 3, BLOCKS + 3, last_dg3, 'dg3last')
        between(j, BLOCKS, BLOCKS, lambda: rs3(BLOCKS - 3), 'rs3')
        def late_stages():
            def body(b, _):
                last_stage(b)
                return 0
            lax.fori_loop(j - 4, 2 * j - BLOCKS - 4, body, 0)
        between(j, BLOCKS + 1, BLOCKS + 2, late_stages, 'rs4late')
        inside(j, join_stats, 'join')
        between(j, 1, BLOCKS - 1, lambda: dz_copy(j - 1).wait(), 'dzwait')
        between(j, BLOCKS, BLOCKS + 2, lambda: de_chunk(2 * (j - BLOCKS), False), 'de_d')

        def start_stats():
            ms_v[0] = jnp.full((8, cols), -3.0e38, F32)
            ms_v[1] = jnp.zeros((8, cols), F32)
            ms_v[2] = jnp.zeros((8, cols), F32)
            tgt_v[pl.ds(9, 1), :] = tgt_v[pl.ds(j + 1, 1), :]
        between(j, -1, BLOCKS - 2, start_stats)

        def first_d(i):
            d_body(i, False, True)

            @pl.when(i == 0)
            def _():
                gather_second()
        between(j, -1, -1, lambda: loop(nr, first_d), 'only_z')
        between(j, 0, BLOCKS - 2, lambda: loop(nr, lambda i: d_body(i, True, True)), 'full_d')
        between(j, BLOCKS - 1, BLOCKS - 1, lambda: loop(nr, lambda i: d_body(i, True, False)), 'back')
        between(j, -1, 0, lambda: fetch_block(j + 2), 'fetch')
        between(j, -1, BLOCKS - 2, lambda: send_stats(j + 1), 'stats')
        inside(j, lambda b: dz_copy(b).start(), 'dzstart')
        between(j, 2, BLOCKS - 2, lambda: rs3(j - 2), 'rs3')
        between(j, BLOCKS, BLOCKS + 1, lambda: rs3(j - 2), 'rs3')
        between(j, 3, BLOCKS - 1, lambda: last_stage(j - 3), 'rs4g1')
        between(j, 4, BLOCKS + 2, lambda: dg2(j - 4), 'dg2')
        between(j, -1, -1, gather_third, 'gthird')
        between(j, 0, 2, lambda: gather_in(2 * j + 2))
        between(j, 5, BLOCKS + 2, lambda: dg3(j - 5), 'dg3')
        inside(j - 1, rs2, 'rs2')
        between(j, BLOCKS + 2, BLOCKS + 2, lambda: dg2(BLOCKS - 1), 'dg2last')
        between(j, BLOCKS + 2, BLOCKS + 2, gb_start, 'gbstart')
        return 0

    def gb_copy(r):
        return remote(gsrc_v, grcv_v.at[r], gb_send.at[r], gb_recv.at[r], (me + r) % n)

    def gb_start():
        for r in range(1, n):
            gb_copy(r).start()

    def start_tail():
        dz_copy(BLOCKS - 1).wait()
        for d in dzin_copies(0, False):
            d.start()

    def start_odd():
        for d in dzin_copies(1, True):
            d.start()

    def x_wait(j):
        @pl.when(j <= BLOCKS - 1)
        def _():
            x_copy(j).wait()

    def first_x(j):
        x_copy(j).wait()

    def step_outer(t, c):
        @pl.when(t == 1)
        def _():
            first_x(0)
        return step(t, c)

    lax.fori_loop(0, BLOCKS + 5, step_outer, 0)

    for b in range(BLOCKS):
        gather4(dgall_ref.at[b], g_send.at[b], g_recv.at[b])
    for c in out_copies(BLOCKS - 1):
        c.wait()
    total_ref[...] = jnp.broadcast_to(jnp.sum(tot_v[0:1, :], axis=1, keepdims=True), total_ref.shape)

    for i in range(npart):
        de_copy(KEEP - 1, i).wait()
    for r in range(1, n):
        gb_copy(r).wait()
    acc = gsrc_v[...]
    for r in range(1, n):
        acc = acc + grcv_v[r]
    dgb_ref[...] = acc


def stream(n, hidden, w_two, gain, bias, embed, code):
    tokens, depth = hidden.shape
    rows = embed.shape[0]
    q = tokens // BLOCKS
    half = CHIPS * q
    tok = 2 * half
    cols = 2 * tok
    nc = depth // 4
    rc, sub = rows // 2, rows // 8
    assert BLOCKS * cols == rows == 2 * depth and nc == cols
    dims = (n, q, depth, rows, rc, nc, sub)
    any_spec = pl.BlockSpec(memory_space=pl.ANY)
    vmem = pl.BlockSpec(memory_space=pltpu.VMEM)
    dma = pltpu.SemaphoreType.DMA
    sds = jax.ShapeDtypeStruct
    return pl.pallas_call(
        functools.partial(stream_kernel, dims),
        out_shape=(sds((BLOCKS, 2, 2, CHIPS, q, depth), BF16), sds((BLOCKS * cols, depth), BF16),
                   sds((rows, BLOCKS * cols), BF16), sds((BLOCKS, 2, CHIPS, q, depth), BF16),
                   sds((BLOCKS, q, depth), F32), sds((BLOCKS, q, depth), BF16),
                   sds((BLOCKS, cols), F32), sds((8, 128), F32), sds((8, depth), F32),
                   sds((KEEP * (rows // BLOCKS), depth), F32)),
        in_specs=[any_spec, any_spec, vmem, vmem, any_spec, vmem],
        out_specs=(any_spec,) * 6 + (vmem,) * 3 + (any_spec,),
        scratch_shapes=[
            pltpu.VMEM((rows, depth), BF16),
            pltpu.VMEM((cols, depth), BF16), pltpu.VMEM((cols, depth), BF16),
            pltpu.VMEM((rows, cols), F32), pltpu.VMEM((rows, cols), BF16),
            pltpu.VMEM((3, 2, 2, half, depth), F32), pltpu.VMEM((2, 2, half, depth), F32),
            pltpu.VMEM((4, 2, q, depth), F32), pltpu.VMEM((5, 2, 2, q, depth), F32),
            pltpu.VMEM((2, tokens, depth), BF16),
            pltpu.VMEM((4, q, depth), BF16), pltpu.VMEM((q, depth), F32),
            pltpu.VMEM((2, 8, cols), F32), pltpu.VMEM((2, n, 8, cols), F32),
            pltpu.VMEM((n, BLOCKS, cols), jnp.int32), pltpu.VMEM((16, cols), jnp.int32),
            pltpu.VMEM((BLOCKS, cols), F32), pltpu.VMEM((BLOCKS, cols), F32),
            pltpu.VMEM((3, 8, cols), F32), pltpu.VMEM((8, cols), F32), pltpu.VMEM((8, cols), F32),
            pltpu.VMEM((8, depth), F32), pltpu.VMEM((n, 8, depth), F32),
            dma((4,)), dma((BLOCKS, 2, 8)), dma((BLOCKS, 2, 8)), dma((BLOCKS, 2)), dma((BLOCKS, 8)), dma((BLOCKS, 8)),
            dma((BLOCKS,)), dma((2, n)), dma((2, n)), dma((2,)), dma((2,)), dma((3, 4)), dma((3, 2)),
            dma((4, 2)), dma((5, 2, 2)), pltpu.SemaphoreType.REGULAR,
            dma((n,)), dma((n,)), dma, dma, dma((4 * CHIPS,)), dma((2,)), dma((n,)), dma((n,)),
            dma((depth // nc,)), dma((BLOCKS + 2,)), dma((depth // nc,)),
        ],
        compiler_params=pltpu.CompilerParams(collective_id=0, has_side_effects=True, vmem_limit_bytes=67043328),
        name='stream',
    )(hidden, w_two, gain, bias, embed, code)


def dense_kernel(part_ref, dzt_ref, xall_ref, aall_ref, gall_ref, da_ref, go_ref, w_ref, loss_ref, sum_ref, dgb_ref,
                 de_ref, dw_ref, dh_ref, tl_ref, total_ref, gs_ref, gb_ref,
                 da_v, go_v, w_v, g_v, x_v, h_v, dw_v, dz_v, de_v, st_v, w_sem, g_sem, x_sem, h_sem, dw_sem, dz_sem, de_sem, in_sem, out_sem, a_sem):
    depth = x_v.shape[1]
    nc, wb = depth // 4, depth // BLOCKS
    re = dzt_ref.shape[0] // BLOCKS
    xr = x_v.shape[0] // BLOCKS
    todo = BLOCKS - KEEP
    pieces = 8 * todo
    pr = KEEP * re // pieces

    def at(i, size):
        return pl.ds(pl.multiple_of(i * size, size), size)

    def w_copy(i):
        return pltpu.make_async_copy(w_ref.at[at(i, nc)], w_v.at[at(i, nc)], w_sem.at[i])

    def h_copy(i):
        return pltpu.make_async_copy(aall_ref.at[:, 0:h_v.shape[2], at(i, wb)], h_v.at[i % 2], h_sem.at[i % 2])

    def dw_copy(i):
        return pltpu.make_async_copy(dw_v.at[i % 2], dw_ref.at[at(i, wb)], dw_sem.at[i % 2])

    def x_copy(i):
        return pltpu.make_async_copy(xall_ref.at[at(i, xr)], x_v.at[at(i, xr)], x_sem.at[i])

    def dz_copy(c):
        return pltpu.make_async_copy(dzt_ref.at[at(KEEP + c, re)], dz_v.at[c % 2], dz_sem.at[c % 2])

    def de_copy(u):
        return pltpu.make_async_copy(de_v.at[u % 2], de_ref.at[at(KEEP + u // 4, re), at(u % 4, nc)], de_sem.at[u % 2])

    def pin(t):
        return pltpu.make_async_copy(part_ref.at[at(t, pr)], st_v.at[t % 4], in_sem.at[t % 4])

    def pout(t):
        return pltpu.make_async_copy(st_v.at[t % 4], de_ref.at[at(t, pr)], out_sem.at[t % 4])

    def carry(t):
        pin(t).wait()
        pout(t).start()

        @pl.when(t >= 2)
        def _():
            pout(t - 2).wait()

        @pl.when(t + 2 < pieces)
        def _():
            pin(t + 2).start()

    g_load = pltpu.make_async_copy(gall_ref, g_v, g_sem)
    da_load = pltpu.make_async_copy(da_ref, da_v, a_sem.at[0])
    go_load = pltpu.make_async_copy(go_ref, go_v, a_sem.at[1])
    go_load.start()
    w_copy(0).start()
    da_load.start()
    for i in range(1, 4):
        w_copy(i).start()
    g_load.start()
    h_copy(0).start()
    h_copy(1).start()

    go_load.wait()
    da_load.wait()

    def hidden_part(i, _):
        w_copy(i).wait()
        sl = at(i, nc)
        back = lax.dot_general(go_v[...], w_v[sl, :], (((1,), (1,)), ((), ())), preferred_element_type=F32)
        dh_ref[:, sl] = (da_v[:, sl] + back).astype(BF16)
        return 0
    with jax.named_scope('k2_dh'):
        lax.fori_loop(0, 4, hidden_part, 0)
    gs_ref[...] = dgb_ref[0:2, :]
    gb_ref[...] = dgb_ref[2:4, :]
    total_ref[0] = sum_ref[0, 0]
    me = lax.axis_index('tp')
    lanes = loss_ref.shape[1]
    q = lanes // 2 // (2 * CHIPS)
    place = (me % 2) * CHIPS + me // 2
    for h in range(2):
        turned = pltpu.roll(loss_ref[...], (lanes - h * (lanes // 2) - place * q) % lanes, 1)
        tl_ref[h:h + 1, :] = jnp.concatenate([turned[b:b + 1, :q] for b in range(BLOCKS)], axis=1)
    with jax.named_scope('k2_g'):
        g_load.wait()

    def dw_part(i, _):
        h_copy(i).wait()
        x_copy(i).start()

        @pl.when(i == BLOCKS - 2)
        def _():
            dz_copy(0).start()
            dz_copy(1).start()
            pin(0).start()
            pin(1).start()
        @pl.when(i >= 2)
        def _():
            dw_copy(i - 2).wait()
        h = h_v[i % 2].reshape(g_v.shape[0], wb)
        dw_v[i % 2] = lax.dot_general(h, g_v[...], (((0,), (0,)), ((), ())), preferred_element_type=F32)
        dw_copy(i).start()

        @pl.when(i + 2 < BLOCKS)
        def _():
            h_copy(i + 2).start()
        return 0
    with jax.named_scope('k2_dw'):
        lax.fori_loop(0, BLOCKS, dw_part, 0)
    with jax.named_scope('k2_x'):
        for i in range(BLOCKS):
            x_copy(i).wait()

    def de_part(u, _):
        c = u // 4

        @pl.when(u % 4 == 0)
        def _():
            dz_copy(c).wait()
        carry(2 * u)

        @pl.when(u >= 2)
        def _():
            de_copy(u - 2).wait()
        de_v[u % 2] = jnp.dot(dz_v[c % 2], x_v[:, at(u % 4, nc)], preferred_element_type=F32)
        de_copy(u).start()
        carry(2 * u + 1)

        @pl.when(jnp.logical_and(u % 4 == 3, c + 2 < todo))
        def _():
            dz_copy(c + 2).start()
        return 0
    with jax.named_scope('k2_de'):
        lax.fori_loop(0, 4 * todo, de_part, 0)
    for i in (BLOCKS - 2, BLOCKS - 1):
        dw_copy(i).wait()
    for i in (4 * todo - 2, 4 * todo - 1):
        de_copy(i).wait()
    for t in (pieces - 2, pieces - 1):
        pout(t).wait()


def dense(part, dzt, xall, aall, gall, da1, dgown, w_two, loss, total_loss, dgb):
    rows, kk = dzt.shape
    depth = xall.shape[1]
    total, tokens = gall.shape[0], da1.shape[0]
    re, wb, nc = rows // BLOCKS, depth // BLOCKS, depth // 4
    pieces = 8 * (BLOCKS - KEEP)
    sds = jax.ShapeDtypeStruct
    dma = pltpu.SemaphoreType.DMA
    any_spec = pl.BlockSpec(memory_space=pl.ANY)
    vmem = pl.BlockSpec(memory_space=pltpu.VMEM)
    return pl.pallas_call(
        dense_kernel,
        out_shape=(sds((rows, depth), F32), sds((depth, depth), F32), sds((tokens, depth), BF16), sds((2, tokens), F32),
                   sds((1,), F32), sds((2, depth), F32), sds((2, depth), F32)),
        in_specs=[any_spec] * 8 + [vmem] * 3,
        out_specs=(any_spec, any_spec, vmem, vmem, pl.BlockSpec(memory_space=pltpu.SMEM), vmem, vmem),
        scratch_shapes=[pltpu.VMEM((tokens, depth), F32), pltpu.VMEM((tokens, depth), BF16), pltpu.VMEM((depth, depth), BF16), pltpu.VMEM((total, depth), BF16), pltpu.VMEM((kk, depth), BF16),
                        pltpu.VMEM((2, BLOCKS, total // BLOCKS, wb), BF16), pltpu.VMEM((2, wb, depth), F32),
                        pltpu.VMEM((2, re, kk), BF16), pltpu.VMEM((2, re, nc), F32),
                        pltpu.VMEM((4, KEEP * re // pieces, depth), F32),
                        dma((4,)), dma, dma((BLOCKS,)), dma((2,)), dma((2,)), dma((2,)), dma((2,)), dma((4,)), dma((4,)), dma((2,))],
        compiler_params=pltpu.CompilerParams(vmem_limit_bytes=67043328),
        name='dense',
    )(part, dzt, xall, aall, gall, da1, dgown, w_two, loss, total_loss, dgb)


def solution(mesh):
    n = mesh.shape['tp']
    tok_spec = P(('dp', 'tp'), None)
    row_spec = P(None, ('dp', 'tp'))

    def device_step(hidden, w_two, ln_scale, ln_shift, embed, targets, loss_mask):
        tokens, depth = hidden.shape
        q = tokens // BLOCKS
        me = lax.axis_index('tp')
        code = (targets + 65536 * loss_mask).reshape(2, BLOCKS, q).transpose(1, 0, 2)
        place = (me % 2) * CHIPS + me // 2
        seat = lax.broadcasted_iota(jnp.int32, (1, 1, 2 * CHIPS, 1), 2) == place
        code = jnp.where(seat, code[:, :, None, :], 0).reshape(BLOCKS, 2 * 2 * CHIPS * q)
        aall, xall, dzt, dgall, da1, dgown, loss, total, dgb, part = stream(
            n, hidden, w_two, ln_scale, ln_shift, embed, code)
        d_embed, d_w, d_hidden, token_loss, total_loss, d_scale, d_shift = dense(
            part, dzt, xall, aall.reshape(BLOCKS, 2 * n * q, depth), dgall.reshape(n * tokens, depth),
            da1.reshape(tokens, depth), dgown.reshape(tokens, depth), w_two, loss, total, dgb)
        return token_loss, total_loss, d_hidden, d_embed, d_w, d_scale, d_shift

    return jax.shard_map(device_step, mesh=mesh,
                         in_specs=(tok_spec, P(), P(), P(), P('tp', None), row_spec, row_spec),
                         out_specs=(row_spec, P('dp'), tok_spec, tok_spec, P('dp', None), P('dp', None), P('dp', None)),
                         check_vma=False)
```

```python
import functools

import jax
import jax.numpy as jnp
from jax import lax
from jax.experimental import pallas as pl
from jax.experimental.pallas import tpu as pltpu
from jax.sharding import PartitionSpec as P

LN_EPS = 1e-5
CHIPS = 4
BLOCKS = 8
KEEP = 6
WAYS = 4
LANES = 2
F32 = jnp.float32
BF16 = jnp.bfloat16


def to(idx):
    return dict(device_id={'tp': idx}, device_id_type=pl.DeviceIdType.MESH)


def remote(src, dst, send, recv, idx):
    return pltpu.make_async_remote_copy(src_ref=src, dst_ref=dst, send_sem=send, recv_sem=recv, **to(idx))


def stream_kernel(dims, h_ref, w_ref, gain_ref, bias_ref, e_ref, code_ref,
                  aall_ref, xall_ref, dzt_ref, dgall_ref, da1_ref, dgown_ref, loss_ref, total_ref, dgb_ref, de_ref,
                  e_v, a_v, x_v, z_v, dz_v, dx_v, pr_v, mg_v, ow_v, own_v, dg_v, da_v,
                  stsrc_v, strcv_v, crcv_v, tgt_v, msk_v, wgt_v, ms_v, row_v, tot_v, gsrc_v, grcv_v,
                  ld_sem, h_send, h_recv, h_loc, g_send, g_recv, g_loc,
                  st_send, st_recv, pr_send, pr_recv, r2_send, r3_send, mg_recv, ow_recv, pair_free,
                  cd_send, cd_recv, x_sem, dz_sem, a_sem, out_sem, gb_send, gb_recv, xin_sem, dzin_sem, de_sem):
    n, q, depth, rows, rc, nc, sub = dims
    re = rows // BLOCKS
    half = CHIPS * q
    tok = 2 * half
    cols = 2 * tok
    me = lax.axis_index('tp')
    chip = me // 2
    core = me % 2
    peer = me + 1 - 2 * core
    right_chip = (chip + 1) % CHIPS
    left_chip = (chip + CHIPS - 1) % CHIPS
    far_chip = (chip + 2) % CHIPS
    right = right_chip * 2 + core
    left = left_chip * 2 + core

    top, bottom = pl.ds(0, depth), pl.ds(depth, rows - depth)
    ld_e = [pltpu.make_async_copy(e_ref.at[d], e_v.at[d], ld_sem.at[i]) for i, d in ((0, top), (3, bottom))]
    ld_w = pltpu.make_async_copy(w_ref, e_v.at[bottom], ld_sem.at[1])
    ld_h = pltpu.make_async_copy(h_ref, own_v.at[0], ld_sem.at[2])
    ld_h.start()
    ld_w.start()

    barrier = pltpu.get_barrier_semaphore()
    for r in range(1, n):
        pl.semaphore_signal(barrier, inc=1, **to((me + r) % n))
    pl.semaphore_wait(barrier, n - 1)

    def code_copy(r):
        return remote(code_ref, crcv_v.at[r], cd_send.at[r], cd_recv.at[r], (me + r) % n)

    for r in range(1, n):
        code_copy(r).start()

    lo, hi = pl.ds(0, q // 2), pl.ds(q // 2, q // 2)

    def g1_copies(src, dst, send, recv):
        piece = dst.at[core, chip]
        return (remote(src, piece, send.at[0], recv.at[0], right),
                remote(src, piece, send.at[1], recv.at[1], left),
                remote(src, piece, send.at[2], recv.at[4], peer))

    def g2_copies(dst, send, recv):
        fl, fr = dst.at[core, left_chip], dst.at[core, right_chip]
        return (remote(fl.at[lo], fl.at[lo], send.at[3], recv.at[2], right),
                remote(fr.at[hi], fr.at[hi], send.at[4], recv.at[3], left),
                remote(fl, fl, send.at[5], recv.at[5], peer),
                remote(fr, fr, send.at[6], recv.at[6], peer))

    def g3_copies(dst, send, recv):
        far = dst.at[core, far_chip]
        return (remote(far, far, send.at[7], recv.at[7], peer),)

    def gather1(src, dst, send, recv, loc):
        for c in g1_copies(src, dst, send, recv):
            c.start()
        pltpu.make_async_copy(src, dst.at[core, chip], loc).start()

    def gather2(src, dst, send, recv, loc):
        remote(src, dst.at[core, left_chip], send.at[0], recv.at[0], right).wait_recv()
        remote(src, dst.at[core, right_chip], send.at[1], recv.at[1], left).wait_recv()
        for c in g2_copies(dst, send, recv):
            c.start()
        for c in g1_copies(src, dst, send, recv):
            c.wait_send()
        pltpu.make_async_copy(src, dst.at[core, chip], loc).wait()

    def gather3(dst, send, recv):
        far = dst.at[core, far_chip]
        remote(far.at[lo], far.at[lo], send.at[3], recv.at[2], right).wait_recv()
        remote(far.at[hi], far.at[hi], send.at[4], recv.at[3], left).wait_recv()
        for c in g3_copies(dst, send, recv):
            c.start()
        for c in g2_copies(dst, send, recv):
            c.wait_send()

    def gather4(dst, send, recv):
        for i, c in enumerate((chip, left_chip, right_chip, far_chip)):
            piece = dst.at[1 - core, c]
            remote(piece, piece, send.at[7], recv.at[4 + i], peer).wait_recv()
        for c in g3_copies(dst, send, recv):
            c.wait_send()

    def own(b, h):
        return own_v.at[h, pl.ds(pl.multiple_of(b * q, q), q)]

    def in1(b, h):
        gather1(own(b, h), aall_ref.at[b, h], h_send.at[b, h], h_recv.at[b, h], h_loc.at[b, h])

    def in2(b, h):
        gather2(own(b, h), aall_ref.at[b, h], h_send.at[b, h], h_recv.at[b, h], h_loc.at[b, h])

    def in3(b, h):
        gather3(aall_ref.at[b, h], h_send.at[b, h], h_recv.at[b, h])

    def dg1(b):
        gather1(dg_v.at[b % 4], dgall_ref.at[b], g_send.at[b], g_recv.at[b], g_loc.at[b])

    def dg2(b):
        gather2(dg_v.at[b % 4], dgall_ref.at[b], g_send.at[b], g_recv.at[b], g_loc.at[b])

    def dg3(b):
        gather3(dgall_ref.at[b], g_send.at[b], g_recv.at[b])

    def span(fn, lo, hi):
        def body(u, _):
            fn(u // 2, u % 2)
            return 0
        lax.fori_loop(2 * lo, 2 * hi, body, 0)

    def a_copy(b, h, kk, c):
        at = pl.ds(((h * 2 + kk) * CHIPS + c) * q, q)
        return pltpu.make_async_copy(aall_ref.at[b, h, kk, c], a_v.at[at], a_sem.at[(h * 2 + kk) * CHIPS + c])

    def block_copies(b):
        return [a_copy(b, h, kk, c) for h in range(2) for kk in range(2) for c in range(CHIPS)]

    def fetch_block(b):
        for h in range(2):
            gather4(aall_ref.at[b, h], h_send.at[b, h], h_recv.at[b, h])
        for c in block_copies(b):
            c.start()

    def project(src, dst):
        def proj(i, _):
            sl = pl.ds(pl.multiple_of(i * nc, nc), nc)
            dst[:, sl] = jnp.dot(src[...], e_v[bottom, sl], preferred_element_type=F32).astype(BF16)
            return 0
        lax.fori_loop(0, depth // nc, proj, 0)

    def norm_rows(start, head):
        a = a_v[pl.ds(start, 16), :].astype(F32)
        mean = jnp.mean(a, axis=-1, keepdims=True)
        cent = a - mean
        var = jnp.mean(cent * cent, axis=-1, keepdims=True)
        y = cent * lax.rsqrt(var + LN_EPS) * gain_ref[pl.ds(head, 1), :] + bias_ref[pl.ds(head, 1), :]
        x_v[pl.ds(start, 16), :] = y.astype(BF16)

    npart = depth // nc
    lrows = cols // npart

    def norm_part(i):
        head = (i * lrows) // tok
        for s in range(lrows // 16):
            norm_rows(pl.multiple_of(i * lrows + s * 16, 16), head)

    def dx_part(i, slot):
        sl = pl.ds(pl.multiple_of(i * nc, nc), nc)
        val = lax.dot_general(dz_v[...], e_v[:, sl], (((0,), (0,)), ((), ())), preferred_element_type=F32)
        for h in range(2):
            for kk in range(2):
                base = h * tok + kk * half
                dx_v[slot, kk, h, :, sl] = val[base:base + half, :]

    nr = rows // rc

    def tree(parts, op):
        while len(parts) > 1:
            parts = [op(a, b) for a, b in zip(parts[::2], parts[1::2])]
        return parts[0]

    def part_view(ref, i):
        return ref.at[pl.ds(pl.multiple_of(i * rc, rc), rc)]

    def back_part(i, p, lanes, td):
        shift, w = row_v[0:1, lanes], row_v[1:2, lanes]
        zc, dc = part_view(z_v, i), part_view(dz_v, i)
        for s in range(p * sub, p * sub + sub, 16):
            both = []
            for t in (s, s + 8):
                pw = jnp.exp(zc[t:t + 8, lanes] - shift)
                both.append(jnp.where(td == t, pw - w, pw))
            dc[s:s + 16, lanes] = jnp.concatenate(both, axis=0).astype(BF16)

    def z_part(i, p):
        ec = part_view(e_v, i)
        part_view(z_v, i)[p * sub:p * sub + sub, :] = lax.dot_general(
            ec[p * sub:p * sub + sub, :], x_v[...], (((1,), (1,)), ((), ())), preferred_element_type=F32)

    def stat_part(i, p, lanes, td, state):
        zc = part_view(z_v, i)
        m_old, acc, tl = state
        at = range(p * sub, p * sub + sub, 8)
        tops = [zc[s:s + 8, lanes] for s in at[:WAYS]]
        for k, s in enumerate(at[WAYS:]):
            tops[k % WAYS] = jnp.maximum(tops[k % WAYS], zc[s:s + 8, lanes])
        m = jnp.maximum(m_old, tree(tops, jnp.maximum))
        accs = [None] * WAYS
        for k, s in enumerate(at):
            z = zc[s:s + 8, lanes]
            e = jnp.exp(z - m)
            accs[k % WAYS] = e if accs[k % WAYS] is None else accs[k % WAYS] + e
            tl = jnp.where(td == s, z, tl)
        return m, acc * jnp.exp(m_old - m) + tree(accs, jnp.add), tl

    def d_body(i, back, new):
        span = cols // LANES
        iota = lax.broadcasted_iota(jnp.int32, (8, span), 0)
        cut = [slice(k * span, k * span + span) for k in range(LANES)]
        td_old = [tgt_v[pl.ds(8, 1), c] - i * rc - iota for c in cut]
        td_new = [tgt_v[pl.ds(9, 1), c] - i * rc - iota for c in cut]
        state = [tuple(ms_v[k, :, c] for k in range(3)) for c in cut]
        for p in range(rc // sub):
            if back:
                for k in range(LANES):
                    back_part(i, p, cut[k], td_old[k])
            if new:
                z_part(i, p)
                for k in range(LANES):
                    state[k] = stat_part(i, p, cut[k], td_new[k], state[k])
        if new:
            for k in range(LANES):
                for q_ in range(3):
                    ms_v[q_, :, cut[k]] = state[k][q_]

    def stat_copy(slot, r):
        return remote(stsrc_v.at[slot], strcv_v.at[slot, r], st_send.at[slot, r], st_recv.at[slot, r], (me + r) % n)

    def send_stats(b):
        slot = b % 2
        m = ms_v[0]
        top = jnp.max(m, axis=0, keepdims=True)
        stsrc_v[slot, 0:1, :] = top
        stsrc_v[slot, 1:2, :] = jnp.sum(ms_v[1] * jnp.exp(m - top), axis=0, keepdims=True)
        stsrc_v[slot, 2:3, :] = jnp.sum(ms_v[2], axis=0, keepdims=True)
        for r in range(1, n):
            stat_copy(slot, r).start()

    def join_stats(b):
        slot = b % 2
        for r in range(1, n):
            stat_copy(slot, r).wait()
        parts = [stsrc_v[slot]] + [strcv_v[slot, r] for r in range(1, n)]
        top = parts[0][0:1]
        for p in parts[1:]:
            top = jnp.maximum(top, p[0:1])
        total = jnp.zeros_like(top)
        hit = jnp.zeros_like(top)
        for p in parts:
            total = total + p[1:2] * jnp.exp(p[0:1] - top)
            hit = hit + p[2:3]
        lse = top + jnp.log(total)
        w = wgt_v[pl.ds(b, 1), :]
        row_v[0:1, :] = jnp.where(w > 0.0, lse - jnp.log(jnp.where(w > 0.0, w, 1.0)), 3.0e38)
        row_v[1:2, :] = w
        tgt_v[pl.ds(8, 1), :] = tgt_v[pl.ds(b, 1), :]
        loss = (lse - hit) * msk_v[pl.ds(b, 1), :]
        loss_ref[pl.ds(b, 1), :] = loss
        tot_v[0:1, :] = tot_v[0:1, :] + loss / tot_v[1:2, :]

    def pair_copy(b):
        slot = b % 2
        return remote(dx_v.at[b % 3, 1 - core], pr_v.at[slot], pr_send.at[slot], pr_recv.at[slot], peer)

    def rs1(b):
        @pl.when(b >= 2)
        def _():
            pl.semaphore_wait(pair_free, 1)
        pair_copy(b).start()

    def crow(c):
        return pl.ds(pl.multiple_of(c * q, q), q)

    def r2_copies(b):
        mine, s3, mg, ow = dx_v.at[b % 3, core], b % 3, b % 4, b % 5
        return (remote(mine.at[0, crow(far_chip)], mg_v.at[mg, 0], r2_send.at[s3, 0], mg_recv.at[mg, 0], right),
                remote(mine.at[1, crow(far_chip)], mg_v.at[mg, 1], r2_send.at[s3, 1], mg_recv.at[mg, 1], left),
                remote(mine.at[1, crow(right_chip)], ow_v.at[ow, 0, 1], r2_send.at[s3, 2], ow_recv.at[ow, 0, 1], right),
                remote(mine.at[0, crow(left_chip)], ow_v.at[ow, 1, 0], r2_send.at[s3, 3], ow_recv.at[ow, 1, 0], left))

    def rs2(b):
        slot, s3 = b % 2, b % 3
        pair_copy(b).wait()

        def add(i, _):
            h = i // CHIPS
            c = i % CHIPS
            dx_v[s3, core, h, crow(c), :] += pr_v[slot, h, crow(c), :]
            return 0
        lax.fori_loop(0, 2 * CHIPS, add, 0)

        @pl.when(b < BLOCKS - 2)
        def _():
            pl.semaphore_signal(pair_free, inc=1, **to(peer))
        for c in r2_copies(b):
            c.start()

    def r3_copies(b):
        mine, s3, ow = dx_v.at[b % 3, core], b % 3, b % 5
        return (remote(mine.at[0, crow(right_chip)], ow_v.at[ow, 0, 0], r3_send.at[s3, 0], ow_recv.at[ow, 0, 0], right),
                remote(mine.at[1, crow(left_chip)], ow_v.at[ow, 1, 1], r3_send.at[s3, 1], ow_recv.at[ow, 1, 1], left))

    def rs3(b):
        s3, mg = b % 3, b % 4
        c2 = r2_copies(b)
        c2[0].wait_recv()
        c2[1].wait_recv()
        dx_v[s3, core, 0, crow(right_chip), :] += mg_v[mg, 0]
        dx_v[s3, core, 1, crow(left_chip), :] += mg_v[mg, 1]
        for c in r3_copies(b):
            c.start()

    def rs4(b):
        ow = b % 5
        c2, c3 = r2_copies(b), r3_copies(b)
        c2[2].wait_recv()
        c2[3].wait_recv()
        c3[0].wait_recv()
        c3[1].wait_recv()

        @pl.when(b >= 1)
        def _():
            out_copies(b - 1)[0].wait()
            out_copies(b - 1)[1].wait()
        for h in range(2):
            dy = dx_v[b % 3, core, h, crow(chip), :] + ow_v[ow, 0, h] + ow_v[ow, 1, h]
            a = own(b, h)[...].astype(F32)
            mean = jnp.mean(a, axis=-1, keepdims=True)
            cent = a - mean
            rstd = lax.rsqrt(jnp.mean(cent * cent, axis=-1, keepdims=True) + LN_EPS)
            xhat = cent * rstd
            gsrc_v[h:h + 1, :] += jnp.sum(dy * xhat, axis=0, keepdims=True)
            gsrc_v[2 + h:3 + h, :] += jnp.sum(dy, axis=0, keepdims=True)
            dxh = dy * gain_ref[h:h + 1, :]
            c1 = jnp.mean(dxh, axis=-1, keepdims=True)
            c2_ = jnp.mean(dxh * xhat, axis=-1, keepdims=True)
            da = rstd * (dxh - c1 - xhat * c2_)
            if h == 0:
                da_v[...] = da
            else:
                dg_v[b % 4] = da.astype(BF16)
        for c in out_copies(b):
            c.start()
        for c in c2 + c3:
            c.wait_send()

    def out_copies(b):
        return (pltpu.make_async_copy(da_v, da1_ref.at[b], out_sem.at[0]),
                pltpu.make_async_copy(dg_v.at[b % 4], dgown_ref.at[b], out_sem.at[1]))

    def xin_copy(i):
        sl = pl.ds(pl.multiple_of(i * nc, nc), nc)
        return pltpu.make_async_copy(xall_ref.at[:, sl], e_v.at[:, sl], xin_sem.at[i])

    def dzin_copies(c, odd):
        at = pl.ds(pl.multiple_of(c * re, re), re)
        if odd:
            return [pltpu.make_async_copy(dzt_ref.at[at, pl.ds(k * cols, cols)], dz_v.at[pl.ds(k * re, re)], dzin_sem.at[k])
                    for k in range(BLOCKS)]
        return [pltpu.make_async_copy(dzt_ref.at[at, pl.ds(k * depth, depth)], (a_v, x_v)[k], dzin_sem.at[BLOCKS + k])
                for k in range(2)]

    def de_copy(c, i):
        return pltpu.make_async_copy(
            z_v.at[pl.ds(pl.multiple_of(i * re, re), re)],
            de_ref.at[pl.ds(pl.multiple_of(c * re, re), re), pl.ds(pl.multiple_of(i * nc, nc), nc)], de_sem.at[i])

    def de_chunk(c, odd, extra=None):
        for d in dzin_copies(c, odd):
            d.wait()

        def part(i, _):
            sl = pl.ds(pl.multiple_of(i * nc, nc), nc)

            @pl.when(c == 0)
            def _():
                xin_copy(i).wait()

            @pl.when(c >= 1)
            def _():
                de_copy(c - 1, i).wait()
            if odd:
                val = jnp.dot(dz_v[:re, :], e_v[:cols, sl], preferred_element_type=F32)
                for k in range(1, BLOCKS):
                    val = val + jnp.dot(dz_v[k * re:k * re + re, :], e_v[k * cols:k * cols + cols, sl], preferred_element_type=F32)
            else:
                val = jnp.dot(a_v[...], e_v[:depth, sl], preferred_element_type=F32)
                val = val + jnp.dot(x_v[...], e_v[depth:, sl], preferred_element_type=F32)
            z_v[pl.ds(pl.multiple_of(i * re, re), re), :] = val
            de_copy(c, i).start()
            if extra is not None:
                @pl.when(jnp.logical_and(c == KEEP - 1, i == npart - 2))
                def _():
                    extra()
            return 0
        lax.fori_loop(0, npart, part, 0)

        @pl.when(c + 2 < KEEP)
        def _():
            for d in dzin_copies(c + 2, odd):
                d.start()

    def inside(b, fn, name='svc'):
        @pl.when(jnp.logical_and(b >= 0, b < BLOCKS))
        def _():
            with jax.named_scope(name):
                fn(b)

    def between(j, lo, hi, fn, name='svc'):
        @pl.when(jnp.logical_and(j >= lo, j <= hi))
        def _():
            with jax.named_scope(name):
                fn()

    def x_copy(b):
        return pltpu.make_async_copy(x_v, xall_ref.at[pl.ds(pl.multiple_of(b * cols, cols), cols)], x_sem)

    def dz_copy(b):
        return pltpu.make_async_copy(dz_v, dzt_ref.at[:, pl.ds(pl.multiple_of(b * cols, cols), cols)], dz_sem)

    def loop(k, fn):
        def body(i, _):
            fn(i)
            return 0
        lax.fori_loop(0, k, body, 0)

    with jax.named_scope('p_h'):
        ld_h.wait()
    in1(0, 0)
    with jax.named_scope('p_w'):
        ld_w.wait()
    ld_e[0].start()
    with jax.named_scope('p_proj'):
        project(own_v.at[0], own_v.at[1])
    with jax.named_scope('p_in2'):
        in2(0, 0)
    span(in1, 1, 3)
    with jax.named_scope('p_code'):
        for r in range(1, n):
            code_copy(r).wait()
    code = code_ref[...]
    for r in range(1, n):
        code = code + crcv_v[r]
    mask = (code >= 65536).astype(jnp.int32)
    local = code - mask * 65536 - me * rows
    tgt_v[0:BLOCKS, :] = jnp.where(jnp.logical_and(local >= 0, local < rows), local, -(1 << 24))
    maskf = mask.astype(F32)
    msk_v[...] = maskf
    per_col = jnp.sum(maskf, axis=0, keepdims=True)
    n0 = jnp.sum(per_col[:, :tok], axis=1, keepdims=True)
    n1 = jnp.sum(per_col[:, tok:], axis=1, keepdims=True)
    counts = jnp.concatenate([jnp.broadcast_to(n0, (1, tok)), jnp.broadcast_to(n1, (1, tok))], axis=1)
    wgt_v[...] = maskf / counts
    tot_v[0:1, :] = jnp.zeros((1, cols), F32)
    tot_v[1:2, :] = counts
    gsrc_v[...] = jnp.zeros_like(gsrc_v)
    with jax.named_scope('p_in3'):
        in3(0, 0)
    with jax.named_scope('p_fetch'):
        gather4(aall_ref.at[0, 0], h_send.at[0, 0], h_recv.at[0, 0])
        first = [a_copy(0, 0, kk, c) for kk in range(2) for c in range(CHIPS)]
        for c in first:
            c.start()
        for c in first:
            c.wait()
    with jax.named_scope('p_proj0'):
        project(a_v.at[pl.ds(0, tok)], a_v.at[pl.ds(tok, tok)])
    ld_e[1].start()
    ld_e[0].wait()

    def last_stage(b):
        rs4(b)
        dg1(b)

    def gather_b0():
        span(in2, 1, 2)
        span(in1, 3, 4)

    def gather_d0():
        ld_e[1].wait()
        span(in3, 1, 2)
        span(in2, 2, 3)
        span(in1, 4, 5)

    def gather_e0():
        span(in3, 2, 3)
        span(in2, 3, 5)
        span(in1, 5, 6)

    def gather_e1():
        span(in3, 3, 5)
        span(in2, 5, 6)
        span(in1, 6, 8)

    def gather_b2():
        span(in3, 5, 6)
        span(in2, 6, 8)

    def gather_e2():
        span(in3, 6, 8)

    def step(t, _):
        j = t - 1
        def last_dg3():
            dg3(BLOCKS - 2)
            dg3(BLOCKS - 1)

        def block_wait():
            for c in block_copies(j + 1):
                c.wait()
        between(j, 0, BLOCKS - 2, block_wait, 'bwait')
        between(j, 1, BLOCKS, lambda: x_wait(j), 'xwait')

        def full_a():
            def body(i):
                dx_part(i, (j - 1) % 3)
                norm_part(i)
            loop(npart, body)
        between(j, -1, 0, lambda: loop(npart, norm_part), 'norm')
        between(j, 1, BLOCKS - 2, full_a, 'full_a')
        between(j, BLOCKS, BLOCKS, start_tail, 'start_tail')

        def last_a(i):
            dx_part(i, (j - 1) % 3)

            @pl.when(j == BLOCKS)
            def _():
                xin_copy(i).start()
        between(j, BLOCKS - 1, BLOCKS, lambda: loop(npart, last_a), 'last_a')
        between(j, BLOCKS + 1, BLOCKS + 3, lambda: de_chunk(2 * (j - BLOCKS) - 1, True, last_dg3), 'de_a')
        between(j, -1, BLOCKS - 2, lambda: x_copy(j + 1).start(), 'xstart')
        between(j, BLOCKS, BLOCKS, start_odd, 'start_odd')
        inside(j - 1, rs1, 'rs1')
        between(j, -1, -1, gather_b0, 'gb0')
        between(j, 1, 1, gather_b2, 'gb2')
        between(j, 1, BLOCKS - 3, lambda: fetch_block(j + 2), 'fetch')
        between(j, BLOCKS, BLOCKS, lambda: rs3(BLOCKS - 3), 'rs3')
        def late_stages():
            def body(b, _):
                last_stage(b)
                return 0
            lax.fori_loop(j - 4, 2 * j - BLOCKS - 4, body, 0)
        between(j, BLOCKS + 1, BLOCKS + 2, late_stages, 'rs4late')
        inside(j, join_stats, 'join')
        between(j, 1, BLOCKS - 1, lambda: dz_copy(j - 1).wait(), 'dzwait')
        between(j, BLOCKS, BLOCKS + 2, lambda: de_chunk(2 * (j - BLOCKS), False), 'de_d')

        def start_stats():
            ms_v[0] = jnp.full((8, cols), -3.0e38, F32)
            ms_v[1] = jnp.zeros((8, cols), F32)
            ms_v[2] = jnp.zeros((8, cols), F32)
            tgt_v[pl.ds(9, 1), :] = tgt_v[pl.ds(j + 1, 1), :]
        between(j, -1, BLOCKS - 2, start_stats)

        def first_d(i):
            d_body(i, False, True)

            @pl.when(i == 0)
            def _():
                gather_d0()
        between(j, -1, -1, lambda: loop(nr, first_d), 'only_z')
        def mid_d(i):
            d_body(i, True, True)

            @pl.when(i == 0)
            def _():
                between(j, 2, BLOCKS - 2, lambda: rs3(j - 2), 'rs3')
                between(j, 1, BLOCKS - 2, lambda: rs2(j - 1), 'rs2')
        between(j, 0, BLOCKS - 2, lambda: loop(nr, mid_d), 'full_d')
        between(j, BLOCKS - 1, BLOCKS - 1, lambda: loop(nr, lambda i: d_body(i, True, False)), 'back')
        between(j, -1, 0, lambda: fetch_block(j + 2), 'fetch')
        between(j, -1, BLOCKS - 2, lambda: send_stats(j + 1), 'stats')
        inside(j, lambda b: dz_copy(b).start(), 'dzstart')
        between(j, BLOCKS, BLOCKS + 1, lambda: rs3(j - 2), 'rs3')
        between(j, 3, BLOCKS - 1, lambda: last_stage(j - 3), 'rs4g1')
        between(j, 4, BLOCKS + 2, lambda: dg2(j - 4), 'dg2')
        between(j, -1, -1, gather_e0, 'ge0')
        between(j, 0, 0, gather_e1, 'ge1')
        between(j, 1, 1, gather_e2, 'ge2')
        between(j, 5, BLOCKS + 2, lambda: dg3(j - 5), 'dg3')
        between(j, BLOCKS - 1, BLOCKS, lambda: rs2(j - 1), 'rs2')
        between(j, BLOCKS + 2, BLOCKS + 2, lambda: dg2(BLOCKS - 1), 'dg2last')
        between(j, BLOCKS + 2, BLOCKS + 2, gb_start, 'gbstart')
        return 0

    def gb_copy(r):
        return remote(gsrc_v, grcv_v.at[r], gb_send.at[r], gb_recv.at[r], (me + r) % n)

    def gb_start():
        for r in range(1, n):
            gb_copy(r).start()

    def start_tail():
        dz_copy(BLOCKS - 1).wait()
        for d in dzin_copies(0, False):
            d.start()

    def start_odd():
        for d in dzin_copies(1, True):
            d.start()

    def x_wait(j):
        @pl.when(j <= BLOCKS - 1)
        def _():
            x_copy(j).wait()

    def first_x(j):
        x_copy(j).wait()

    def step_outer(t, c):
        @pl.when(t == 1)
        def _():
            first_x(0)
        return step(t, c)

    lax.fori_loop(0, BLOCKS + 5, step_outer, 0)

    for b in range(BLOCKS):
        gather4(dgall_ref.at[b], g_send.at[b], g_recv.at[b])
    for c in out_copies(BLOCKS - 1):
        c.wait()
    total_ref[...] = jnp.broadcast_to(jnp.sum(tot_v[0:1, :], axis=1, keepdims=True), total_ref.shape)

    for i in range(npart):
        de_copy(KEEP - 1, i).wait()
    for r in range(1, n):
        gb_copy(r).wait()
    acc = gsrc_v[...]
    for r in range(1, n):
        acc = acc + grcv_v[r]
    dgb_ref[...] = acc


def stream(n, hidden, w_two, gain, bias, embed, code):
    tokens, depth = hidden.shape
    rows = embed.shape[0]
    q = tokens // BLOCKS
    half = CHIPS * q
    tok = 2 * half
    cols = 2 * tok
    nc = depth // 4
    rc, sub = rows // 2, rows // 8
    assert BLOCKS * cols == rows == 2 * depth and nc == cols
    dims = (n, q, depth, rows, rc, nc, sub)
    any_spec = pl.BlockSpec(memory_space=pl.ANY)
    vmem = pl.BlockSpec(memory_space=pltpu.VMEM)
    dma = pltpu.SemaphoreType.DMA
    sds = jax.ShapeDtypeStruct
    return pl.pallas_call(
        functools.partial(stream_kernel, dims),
        out_shape=(sds((BLOCKS, 2, 2, CHIPS, q, depth), BF16), sds((BLOCKS * cols, depth), BF16),
                   sds((rows, BLOCKS * cols), BF16), sds((BLOCKS, 2, CHIPS, q, depth), BF16),
                   sds((BLOCKS, q, depth), F32), sds((BLOCKS, q, depth), BF16),
                   sds((BLOCKS, cols), F32), sds((8, 128), F32), sds((8, depth), F32),
                   sds((KEEP * (rows // BLOCKS), depth), F32)),
        in_specs=[any_spec, any_spec, vmem, vmem, any_spec, vmem],
        out_specs=(any_spec,) * 6 + (vmem,) * 3 + (any_spec,),
        scratch_shapes=[
            pltpu.VMEM((rows, depth), BF16),
            pltpu.VMEM((cols, depth), BF16), pltpu.VMEM((cols, depth), BF16),
            pltpu.VMEM((rows, cols), F32), pltpu.VMEM((rows, cols), BF16),
            pltpu.VMEM((3, 2, 2, half, depth), F32), pltpu.VMEM((2, 2, half, depth), F32),
            pltpu.VMEM((4, 2, q, depth), F32), pltpu.VMEM((5, 2, 2, q, depth), F32),
            pltpu.VMEM((2, tokens, depth), BF16),
            pltpu.VMEM((4, q, depth), BF16), pltpu.VMEM((q, depth), F32),
            pltpu.VMEM((2, 8, cols), F32), pltpu.VMEM((2, n, 8, cols), F32),
            pltpu.VMEM((n, BLOCKS, cols), jnp.int32), pltpu.VMEM((16, cols), jnp.int32),
            pltpu.VMEM((BLOCKS, cols), F32), pltpu.VMEM((BLOCKS, cols), F32),
            pltpu.VMEM((3, 8, cols), F32), pltpu.VMEM((8, cols), F32), pltpu.VMEM((8, cols), F32),
            pltpu.VMEM((8, depth), F32), pltpu.VMEM((n, 8, depth), F32),
            dma((4,)), dma((BLOCKS, 2, 8)), dma((BLOCKS, 2, 8)), dma((BLOCKS, 2)), dma((BLOCKS, 8)), dma((BLOCKS, 8)),
            dma((BLOCKS,)), dma((2, n)), dma((2, n)), dma((2,)), dma((2,)), dma((3, 4)), dma((3, 2)),
            dma((4, 2)), dma((5, 2, 2)), pltpu.SemaphoreType.REGULAR,
            dma((n,)), dma((n,)), dma, dma, dma((4 * CHIPS,)), dma((2,)), dma((n,)), dma((n,)),
            dma((depth // nc,)), dma((BLOCKS + 2,)), dma((depth // nc,)),
        ],
        compiler_params=pltpu.CompilerParams(collective_id=0, has_side_effects=True, vmem_limit_bytes=67043328),
        name='stream',
    )(hidden, w_two, gain, bias, embed, code)


def dense_kernel(part_ref, dzt_ref, xall_ref, aall_ref, gall_ref, da_ref, go_ref, w_ref, loss_ref, sum_ref, dgb_ref,
                 de_ref, dw_ref, dh_ref, tl_ref, total_ref, gs_ref, gb_ref,
                 da_v, go_v, w_v, g_v, x_v, h_v, dw_v, dz_v, de_v, st_v, w_sem, g_sem, x_sem, h_sem, dw_sem, dz_sem, de_sem, in_sem, out_sem, a_sem):
    depth = x_v.shape[1]
    nc, wb = depth // 4, depth // BLOCKS
    re = dzt_ref.shape[0] // BLOCKS
    xr = x_v.shape[0] // BLOCKS
    todo = BLOCKS - KEEP
    pieces = BLOCKS + 8 * todo
    pr = KEEP * re // pieces

    def at(i, size):
        return pl.ds(pl.multiple_of(i * size, size), size)

    def w_copy(i):
        return pltpu.make_async_copy(w_ref.at[at(i, nc)], w_v.at[at(i, nc)], w_sem.at[i])

    def h_copy(i):
        return pltpu.make_async_copy(aall_ref.at[:, 0:h_v.shape[2], at(i, wb)], h_v.at[i % 2], h_sem.at[i % 2])

    def dw_copy(i):
        return pltpu.make_async_copy(dw_v.at[i % 2], dw_ref.at[at(i, wb)], dw_sem.at[i % 2])

    def x_copy(i):
        return pltpu.make_async_copy(xall_ref.at[at(i, xr)], x_v.at[at(i, xr)], x_sem.at[i])

    def dz_copy(c):
        return pltpu.make_async_copy(dzt_ref.at[at(KEEP + c, re)], dz_v.at[c % 2], dz_sem.at[c % 2])

    def de_copy(u):
        return pltpu.make_async_copy(de_v.at[u % 2], de_ref.at[at(KEEP + u // 4, re), at(u % 4, nc)], de_sem.at[u % 2])

    def pin(t):
        return pltpu.make_async_copy(part_ref.at[at(t, pr)], st_v.at[t % 4], in_sem.at[t % 4])

    def pout(t):
        return pltpu.make_async_copy(st_v.at[t % 4], de_ref.at[at(t, pr)], out_sem.at[t % 4])

    def carry(t):
        pin(t).wait()
        pout(t).start()

        @pl.when(t >= 2)
        def _():
            pout(t - 2).wait()

        @pl.when(t + 2 < pieces)
        def _():
            pin(t + 2).start()

    g_load = pltpu.make_async_copy(gall_ref, g_v, g_sem)
    da_load = pltpu.make_async_copy(da_ref, da_v, a_sem.at[0])
    go_load = pltpu.make_async_copy(go_ref, go_v, a_sem.at[1])
    go_load.start()
    w_copy(0).start()
    da_load.start()
    for i in range(1, 4):
        w_copy(i).start()
    g_load.start()
    h_copy(0).start()
    h_copy(1).start()
    pin(0).start()
    pin(1).start()

    go_load.wait()
    da_load.wait()

    def hidden_part(i, _):
        w_copy(i).wait()
        sl = at(i, nc)
        back = lax.dot_general(go_v[...], w_v[sl, :], (((1,), (1,)), ((), ())), preferred_element_type=F32)
        dh_ref[:, sl] = (da_v[:, sl] + back).astype(BF16)
        return 0
    with jax.named_scope('k2_dh'):
        lax.fori_loop(0, 4, hidden_part, 0)
    gs_ref[...] = dgb_ref[0:2, :]
    gb_ref[...] = dgb_ref[2:4, :]
    total_ref[0] = sum_ref[0, 0]
    me = lax.axis_index('tp')
    lanes = loss_ref.shape[1]
    q = lanes // 2 // (2 * CHIPS)
    place = (me % 2) * CHIPS + me // 2
    for h in range(2):
        turned = pltpu.roll(loss_ref[...], (lanes - h * (lanes // 2) - place * q) % lanes, 1)
        tl_ref[h:h + 1, :] = jnp.concatenate([turned[b:b + 1, :q] for b in range(BLOCKS)], axis=1)
    with jax.named_scope('k2_g'):
        g_load.wait()

    def dw_part(i, _):
        h_copy(i).wait()
        carry(i)

        @pl.when(i < BLOCKS // 2)
        def _():
            x_copy(2 * i).start()
            x_copy(2 * i + 1).start()

        @pl.when(i == BLOCKS // 2)
        def _():
            dz_copy(0).start()

        @pl.when(i == BLOCKS // 2 + 2)
        def _():
            dz_copy(1).start()
        @pl.when(i >= 2)
        def _():
            dw_copy(i - 2).wait()
        h = h_v[i % 2].reshape(g_v.shape[0], wb)
        dw_v[i % 2] = lax.dot_general(h, g_v[...], (((0,), (0,)), ((), ())), preferred_element_type=F32)
        dw_copy(i).start()

        @pl.when(i + 2 < BLOCKS)
        def _():
            h_copy(i + 2).start()
        return 0
    with jax.named_scope('k2_dw'):
        lax.fori_loop(0, BLOCKS, dw_part, 0)
    with jax.named_scope('k2_x'):
        for i in range(BLOCKS):
            x_copy(i).wait()

    def de_part(u, _):
        c = u // 4

        @pl.when(u % 4 == 0)
        def _():
            dz_copy(c).wait()
        carry(BLOCKS + 2 * u)

        @pl.when(u >= 2)
        def _():
            de_copy(u - 2).wait()
        de_v[u % 2] = jnp.dot(dz_v[c % 2], x_v[:, at(u % 4, nc)], preferred_element_type=F32)
        de_copy(u).start()
        carry(BLOCKS + 2 * u + 1)

        @pl.when(jnp.logical_and(u % 4 == 3, c + 2 < todo))
        def _():
            dz_copy(c + 2).start()
        return 0
    with jax.named_scope('k2_de'):
        lax.fori_loop(0, 4 * todo, de_part, 0)
    for i in (BLOCKS - 2, BLOCKS - 1):
        dw_copy(i).wait()
    for i in (4 * todo - 2, 4 * todo - 1):
        de_copy(i).wait()
    for t in (pieces - 2, pieces - 1):
        pout(t).wait()


def dense(part, dzt, xall, aall, gall, da1, dgown, w_two, loss, total_loss, dgb):
    rows, kk = dzt.shape
    depth = xall.shape[1]
    total, tokens = gall.shape[0], da1.shape[0]
    re, wb, nc = rows // BLOCKS, depth // BLOCKS, depth // 4
    pieces = BLOCKS + 8 * (BLOCKS - KEEP)
    sds = jax.ShapeDtypeStruct
    dma = pltpu.SemaphoreType.DMA
    any_spec = pl.BlockSpec(memory_space=pl.ANY)
    vmem = pl.BlockSpec(memory_space=pltpu.VMEM)
    return pl.pallas_call(
        dense_kernel,
        out_shape=(sds((rows, depth), F32), sds((depth, depth), F32), sds((tokens, depth), BF16), sds((2, tokens), F32),
                   sds((1,), F32), sds((2, depth), F32), sds((2, depth), F32)),
        in_specs=[any_spec] * 8 + [vmem] * 3,
        out_specs=(any_spec, any_spec, vmem, vmem, pl.BlockSpec(memory_space=pltpu.SMEM), vmem, vmem),
        scratch_shapes=[pltpu.VMEM((tokens, depth), F32), pltpu.VMEM((tokens, depth), BF16), pltpu.VMEM((depth, depth), BF16), pltpu.VMEM((total, depth), BF16), pltpu.VMEM((kk, depth), BF16),
                        pltpu.VMEM((2, BLOCKS, total // BLOCKS, wb), BF16), pltpu.VMEM((2, wb, depth), F32),
                        pltpu.VMEM((2, re, kk), BF16), pltpu.VMEM((2, re, nc), F32),
                        pltpu.VMEM((4, KEEP * re // pieces, depth), F32),
                        dma((4,)), dma, dma((BLOCKS,)), dma((2,)), dma((2,)), dma((2,)), dma((2,)), dma((4,)), dma((4,)), dma((2,))],
        compiler_params=pltpu.CompilerParams(vmem_limit_bytes=67043328),
        name='dense',
    )(part, dzt, xall, aall, gall, da1, dgown, w_two, loss, total_loss, dgb)


def solution(mesh):
    n = mesh.shape['tp']
    tok_spec = P(('dp', 'tp'), None)
    row_spec = P(None, ('dp', 'tp'))

    def device_step(hidden, w_two, ln_scale, ln_shift, embed, targets, loss_mask):
        tokens, depth = hidden.shape
        q = tokens // BLOCKS
        me = lax.axis_index('tp')
        code = (targets + 65536 * loss_mask).reshape(2, BLOCKS, q).transpose(1, 0, 2)
        place = (me % 2) * CHIPS + me // 2
        seat = lax.broadcasted_iota(jnp.int32, (1, 1, 2 * CHIPS, 1), 2) == place
        code = jnp.where(seat, code[:, :, None, :], 0).reshape(BLOCKS, 2 * 2 * CHIPS * q)
        aall, xall, dzt, dgall, da1, dgown, loss, total, dgb, part = stream(
            n, hidden, w_two, ln_scale, ln_shift, embed, code)
        d_embed, d_w, d_hidden, token_loss, total_loss, d_scale, d_shift = dense(
            part, dzt, xall, aall.reshape(BLOCKS, 2 * n * q, depth), dgall.reshape(n * tokens, depth),
            da1.reshape(tokens, depth), dgown.reshape(tokens, depth), w_two, loss, total, dgb)
        return token_loss, total_loss, d_hidden, d_embed, d_w, d_scale, d_shift

    return jax.shard_map(device_step, mesh=mesh,
                         in_specs=(tok_spec, P(), P(), P(), P('tp', None), row_spec, row_spec),
                         out_specs=(row_spec, P('dp'), tok_spec, tok_spec, P('dp', None), P('dp', None), P('dp', None)),
                         check_vma=False)
```

```python
import functools

import jax
import jax.numpy as jnp
from jax import lax
from jax.experimental import pallas as pl
from jax.experimental.pallas import tpu as pltpu
from jax.sharding import PartitionSpec as P

LN_EPS = 1e-5
CHIPS = 4
BLOCKS = 8
KEEP = 6
WAYS = 4
LANES = 2
F32 = jnp.float32
BF16 = jnp.bfloat16


def to(idx):
    return dict(device_id={'tp': idx}, device_id_type=pl.DeviceIdType.MESH)


def remote(src, dst, send, recv, idx):
    return pltpu.make_async_remote_copy(src_ref=src, dst_ref=dst, send_sem=send, recv_sem=recv, **to(idx))


def stream_kernel(dims, h_ref, w_ref, gain_ref, bias_ref, e_ref, code_ref,
                  aall_ref, xall_ref, dzt_ref, dgall_ref, da1_ref, dgown_ref, loss_ref, total_ref, dgb_ref, de_ref,
                  e_v, a_v, x_v, z_v, dz_v, dx_v, pr_v, mg_v, ow_v, own_v, dg_v, da_v,
                  stsrc_v, strcv_v, crcv_v, tgt_v, msk_v, wgt_v, ms_v, row_v, tot_v, gsrc_v, grcv_v,
                  ld_sem, h_send, h_recv, h_loc, g_send, g_recv, g_loc,
                  st_send, st_recv, pr_send, pr_recv, r2_send, r3_send, mg_recv, ow_recv, pair_free,
                  cd_send, cd_recv, x_sem, dz_sem, a_sem, out_sem, gb_send, gb_recv, xin_sem, dzin_sem, de_sem):
    n, q, depth, rows, rc, nc, sub = dims
    re = rows // BLOCKS
    half = CHIPS * q
    tok = 2 * half
    cols = 2 * tok
    me = lax.axis_index('tp')
    chip = me // 2
    core = me % 2
    peer = me + 1 - 2 * core
    right_chip = (chip + 1) % CHIPS
    left_chip = (chip + CHIPS - 1) % CHIPS
    far_chip = (chip + 2) % CHIPS
    right = right_chip * 2 + core
    left = left_chip * 2 + core

    top, bottom = pl.ds(0, depth), pl.ds(depth, rows - depth)
    ld_e = [pltpu.make_async_copy(e_ref.at[d], e_v.at[d], ld_sem.at[i]) for i, d in ((0, top), (3, bottom))]
    ld_w = pltpu.make_async_copy(w_ref, e_v.at[bottom], ld_sem.at[1])
    ld_h = pltpu.make_async_copy(h_ref, own_v.at[0], ld_sem.at[2])
    ld_h.start()
    ld_w.start()

    barrier = pltpu.get_barrier_semaphore()
    for r in range(1, n):
        pl.semaphore_signal(barrier, inc=1, **to((me + r) % n))
    pl.semaphore_wait(barrier, n - 1)

    def code_copy(r):
        return remote(code_ref, crcv_v.at[r], cd_send.at[r], cd_recv.at[r], (me + r) % n)

    for r in range(1, n):
        code_copy(r).start()

    lo, hi = pl.ds(0, q // 2), pl.ds(q // 2, q // 2)

    def g1_copies(src, dst, send, recv):
        piece = dst.at[core, chip]
        return (remote(src, piece, send.at[0], recv.at[0], right),
                remote(src, piece, send.at[1], recv.at[1], left),
                remote(src, piece, send.at[2], recv.at[4], peer))

    def g2_copies(dst, send, recv):
        fl, fr = dst.at[core, left_chip], dst.at[core, right_chip]
        return (remote(fl.at[lo], fl.at[lo], send.at[3], recv.at[2], right),
                remote(fr.at[hi], fr.at[hi], send.at[4], recv.at[3], left),
                remote(fl, fl, send.at[5], recv.at[5], peer),
                remote(fr, fr, send.at[6], recv.at[6], peer))

    def g3_copies(dst, send, recv):
        far = dst.at[core, far_chip]
        return (remote(far, far, send.at[7], recv.at[7], peer),)

    def gather1(src, dst, send, recv, loc):
        for c in g1_copies(src, dst, send, recv):
            c.start()
        pltpu.make_async_copy(src, dst.at[core, chip], loc).start()

    def gather2(src, dst, send, recv, loc):
        remote(src, dst.at[core, left_chip], send.at[0], recv.at[0], right).wait_recv()
        remote(src, dst.at[core, right_chip], send.at[1], recv.at[1], left).wait_recv()
        for c in g2_copies(dst, send, recv):
            c.start()
        for c in g1_copies(src, dst, send, recv):
            c.wait_send()
        pltpu.make_async_copy(src, dst.at[core, chip], loc).wait()

    def gather3(dst, send, recv):
        far = dst.at[core, far_chip]
        remote(far.at[lo], far.at[lo], send.at[3], recv.at[2], right).wait_recv()
        remote(far.at[hi], far.at[hi], send.at[4], recv.at[3], left).wait_recv()
        for c in g3_copies(dst, send, recv):
            c.start()
        for c in g2_copies(dst, send, recv):
            c.wait_send()

    def gather4(dst, send, recv):
        for i, c in enumerate((chip, left_chip, right_chip, far_chip)):
            piece = dst.at[1 - core, c]
            remote(piece, piece, send.at[7], recv.at[4 + i], peer).wait_recv()
        for c in g3_copies(dst, send, recv):
            c.wait_send()

    def own(b, h):
        return own_v.at[h, pl.ds(pl.multiple_of(b * q, q), q)]

    def in1(b, h):
        gather1(own(b, h), aall_ref.at[b, h], h_send.at[b, h], h_recv.at[b, h], h_loc.at[b, h])

    def in2(b, h):
        gather2(own(b, h), aall_ref.at[b, h], h_send.at[b, h], h_recv.at[b, h], h_loc.at[b, h])

    def in3(b, h):
        gather3(aall_ref.at[b, h], h_send.at[b, h], h_recv.at[b, h])

    def dg1(b):
        gather1(dg_v.at[b % 4], dgall_ref.at[b], g_send.at[b], g_recv.at[b], g_loc.at[b])

    def dg2(b):
        gather2(dg_v.at[b % 4], dgall_ref.at[b], g_send.at[b], g_recv.at[b], g_loc.at[b])

    def dg3(b):
        gather3(dgall_ref.at[b], g_send.at[b], g_recv.at[b])

    def span(fn, lo, hi):
        def body(u, _):
            fn(u // 2, u % 2)
            return 0
        lax.fori_loop(2 * lo, 2 * hi, body, 0)

    def a_copy(b, h, kk, c):
        at = pl.ds(((h * 2 + kk) * CHIPS + c) * q, q)
        return pltpu.make_async_copy(aall_ref.at[b, h, kk, c], a_v.at[at], a_sem.at[(h * 2 + kk) * CHIPS + c])

    def block_copies(b):
        return [a_copy(b, h, kk, c) for h in range(2) for kk in range(2) for c in range(CHIPS)]

    def fetch_block(b):
        for h in range(2):
            gather4(aall_ref.at[b, h], h_send.at[b, h], h_recv.at[b, h])
        for c in block_copies(b):
            c.start()

    def project(src, dst):
        def proj(i, _):
            sl = pl.ds(pl.multiple_of(i * nc, nc), nc)
            dst[:, sl] = jnp.dot(src[...], e_v[bottom, sl], preferred_element_type=F32).astype(BF16)
            return 0
        lax.fori_loop(0, depth // nc, proj, 0)

    def norm_rows(start, head):
        a = a_v[pl.ds(start, 16), :].astype(F32)
        mean = jnp.mean(a, axis=-1, keepdims=True)
        cent = a - mean
        var = jnp.mean(cent * cent, axis=-1, keepdims=True)
        y = cent * lax.rsqrt(var + LN_EPS) * gain_ref[pl.ds(head, 1), :] + bias_ref[pl.ds(head, 1), :]
        x_v[pl.ds(start, 16), :] = y.astype(BF16)

    npart = depth // nc
    lrows = cols // npart

    def norm_part(i):
        head = (i * lrows) // tok
        for s in range(lrows // 16):
            norm_rows(pl.multiple_of(i * lrows + s * 16, 16), head)

    def dx_part(i, slot):
        sl = pl.ds(pl.multiple_of(i * nc, nc), nc)
        val = lax.dot_general(dz_v[...], e_v[:, sl], (((0,), (0,)), ((), ())), preferred_element_type=F32)
        for h in range(2):
            for kk in range(2):
                base = h * tok + kk * half
                dx_v[slot, kk, h, :, sl] = val[base:base + half, :]

    nr = rows // rc

    def tree(parts, op):
        while len(parts) > 1:
            parts = [op(a, b) for a, b in zip(parts[::2], parts[1::2])]
        return parts[0]

    def part_view(ref, i):
        return ref.at[pl.ds(pl.multiple_of(i * rc, rc), rc)]

    def back_part(i, p, lanes, td):
        shift, w = row_v[0:1, lanes], row_v[1:2, lanes]
        zc, dc = part_view(z_v, i), part_view(dz_v, i)
        for s in range(p * sub, p * sub + sub, 16):
            both = []
            for t in (s, s + 8):
                pw = jnp.exp(zc[t:t + 8, lanes] - shift)
                both.append(jnp.where(td == t, pw - w, pw))
            dc[s:s + 16, lanes] = jnp.concatenate(both, axis=0).astype(BF16)

    def z_part(i, p):
        ec = part_view(e_v, i)
        part_view(z_v, i)[p * sub:p * sub + sub, :] = lax.dot_general(
            ec[p * sub:p * sub + sub, :], x_v[...], (((1,), (1,)), ((), ())), preferred_element_type=F32)

    def stat_part(i, p, lanes, td, state):
        zc = part_view(z_v, i)
        m_old, acc, tl = state
        at = range(p * sub, p * sub + sub, 8)
        tops = [zc[s:s + 8, lanes] for s in at[:WAYS]]
        for k, s in enumerate(at[WAYS:]):
            tops[k % WAYS] = jnp.maximum(tops[k % WAYS], zc[s:s + 8, lanes])
        m = jnp.maximum(m_old, tree(tops, jnp.maximum))
        accs = [None] * WAYS
        for k, s in enumerate(at):
            z = zc[s:s + 8, lanes]
            e = jnp.exp(z - m)
            accs[k % WAYS] = e if accs[k % WAYS] is None else accs[k % WAYS] + e
            tl = jnp.where(td == s, z, tl)
        return m, acc * jnp.exp(m_old - m) + tree(accs, jnp.add), tl

    def d_body(i, back, new):
        span = cols // LANES
        iota = lax.broadcasted_iota(jnp.int32, (8, span), 0)
        cut = [slice(k * span, k * span + span) for k in range(LANES)]
        td_old = [tgt_v[pl.ds(8, 1), c] - i * rc - iota for c in cut]
        td_new = [tgt_v[pl.ds(9, 1), c] - i * rc - iota for c in cut]
        state = [tuple(ms_v[k, :, c] for k in range(3)) for c in cut]
        for p in range(rc // sub):
            if back:
                for k in range(LANES):
                    back_part(i, p, cut[k], td_old[k])
            if new:
                z_part(i, p)
                for k in range(LANES):
                    state[k] = stat_part(i, p, cut[k], td_new[k], state[k])
        if new:
            for k in range(LANES):
                for q_ in range(3):
                    ms_v[q_, :, cut[k]] = state[k][q_]

    def stat_copy(slot, r):
        return remote(stsrc_v.at[slot], strcv_v.at[slot, r], st_send.at[slot, r], st_recv.at[slot, r], (me + r) % n)

    def send_stats(b):
        slot = b % 2
        m = ms_v[0]
        top = jnp.max(m, axis=0, keepdims=True)
        stsrc_v[slot, 0:1, :] = top
        stsrc_v[slot, 1:2, :] = jnp.sum(ms_v[1] * jnp.exp(m - top), axis=0, keepdims=True)
        stsrc_v[slot, 2:3, :] = jnp.sum(ms_v[2], axis=0, keepdims=True)
        for r in range(1, n):
            stat_copy(slot, r).start()

    def join_stats(b):
        slot = b % 2
        for r in range(1, n):
            stat_copy(slot, r).wait()
        parts = [stsrc_v[slot]] + [strcv_v[slot, r] for r in range(1, n)]
        top = parts[0][0:1]
        for p in parts[1:]:
            top = jnp.maximum(top, p[0:1])
        total = jnp.zeros_like(top)
        hit = jnp.zeros_like(top)
        for p in parts:
            total = total + p[1:2] * jnp.exp(p[0:1] - top)
            hit = hit + p[2:3]
        lse = top + jnp.log(total)
        w = wgt_v[pl.ds(b, 1), :]
        row_v[0:1, :] = jnp.where(w > 0.0, lse - jnp.log(jnp.where(w > 0.0, w, 1.0)), 3.0e38)
        row_v[1:2, :] = w
        tgt_v[pl.ds(8, 1), :] = tgt_v[pl.ds(b, 1), :]
        loss = (lse - hit) * msk_v[pl.ds(b, 1), :]
        loss_ref[pl.ds(b, 1), :] = loss
        tot_v[0:1, :] = tot_v[0:1, :] + loss / tot_v[1:2, :]

    def pair_copy(b):
        slot = b % 2
        return remote(dx_v.at[b % 3, 1 - core], pr_v.at[slot], pr_send.at[slot], pr_recv.at[slot], peer)

    def rs1(b):
        @pl.when(b >= 2)
        def _():
            pl.semaphore_wait(pair_free, 1)
        pair_copy(b).start()

    def crow(c):
        return pl.ds(pl.multiple_of(c * q, q), q)

    def r2_copies(b):
        mine, s3, mg, ow = dx_v.at[b % 3, core], b % 3, b % 4, b % 5
        return (remote(mine.at[0, crow(far_chip)], mg_v.at[mg, 0], r2_send.at[s3, 0], mg_recv.at[mg, 0], right),
                remote(mine.at[1, crow(far_chip)], mg_v.at[mg, 1], r2_send.at[s3, 1], mg_recv.at[mg, 1], left),
                remote(mine.at[1, crow(right_chip)], ow_v.at[ow, 0, 1], r2_send.at[s3, 2], ow_recv.at[ow, 0, 1], right),
                remote(mine.at[0, crow(left_chip)], ow_v.at[ow, 1, 0], r2_send.at[s3, 3], ow_recv.at[ow, 1, 0], left))

    def rs2(b):
        slot, s3 = b % 2, b % 3
        pair_copy(b).wait()

        def add(i, _):
            h = i // CHIPS
            c = i % CHIPS
            dx_v[s3, core, h, crow(c), :] += pr_v[slot, h, crow(c), :]
            return 0
        lax.fori_loop(0, 2 * CHIPS, add, 0)

        @pl.when(b < BLOCKS - 2)
        def _():
            pl.semaphore_signal(pair_free, inc=1, **to(peer))
        for c in r2_copies(b):
            c.start()

    def r3_copies(b):
        mine, s3, ow = dx_v.at[b % 3, core], b % 3, b % 5
        return (remote(mine.at[0, crow(right_chip)], ow_v.at[ow, 0, 0], r3_send.at[s3, 0], ow_recv.at[ow, 0, 0], right),
                remote(mine.at[1, crow(left_chip)], ow_v.at[ow, 1, 1], r3_send.at[s3, 1], ow_recv.at[ow, 1, 1], left))

    def rs3(b):
        s3, mg = b % 3, b % 4
        c2 = r2_copies(b)
        c2[0].wait_recv()
        c2[1].wait_recv()
        dx_v[s3, core, 0, crow(right_chip), :] += mg_v[mg, 0]
        dx_v[s3, core, 1, crow(left_chip), :] += mg_v[mg, 1]
        for c in r3_copies(b):
            c.start()

    def rs4(b):
        ow = b % 5
        c2, c3 = r2_copies(b), r3_copies(b)
        c2[2].wait_recv()
        c2[3].wait_recv()
        c3[0].wait_recv()
        c3[1].wait_recv()

        @pl.when(b >= 1)
        def _():
            out_copies(b - 1)[0].wait()
            out_copies(b - 1)[1].wait()
        for h in range(2):
            dy = dx_v[b % 3, core, h, crow(chip), :] + ow_v[ow, 0, h] + ow_v[ow, 1, h]
            a = own(b, h)[...].astype(F32)
            mean = jnp.mean(a, axis=-1, keepdims=True)
            cent = a - mean
            rstd = lax.rsqrt(jnp.mean(cent * cent, axis=-1, keepdims=True) + LN_EPS)
            xhat = cent * rstd
            gsrc_v[h:h + 1, :] += jnp.sum(dy * xhat, axis=0, keepdims=True)
            gsrc_v[2 + h:3 + h, :] += jnp.sum(dy, axis=0, keepdims=True)
            dxh = dy * gain_ref[h:h + 1, :]
            c1 = jnp.mean(dxh, axis=-1, keepdims=True)
            c2_ = jnp.mean(dxh * xhat, axis=-1, keepdims=True)
            da = rstd * (dxh - c1 - xhat * c2_)
            if h == 0:
                da_v[...] = da
            else:
                dg_v[b % 4] = da.astype(BF16)
        for c in out_copies(b):
            c.start()
        for c in c2 + c3:
            c.wait_send()

    def out_copies(b):
        return (pltpu.make_async_copy(da_v, da1_ref.at[b], out_sem.at[0]),
                pltpu.make_async_copy(dg_v.at[b % 4], dgown_ref.at[b], out_sem.at[1]))

    def xin_copy(i):
        sl = pl.ds(pl.multiple_of(i * nc, nc), nc)
        return pltpu.make_async_copy(xall_ref.at[:, sl], e_v.at[:, sl], xin_sem.at[i])

    def dzin_copies(c, odd):
        at = pl.ds(pl.multiple_of(c * re, re), re)
        if odd:
            return [pltpu.make_async_copy(dzt_ref.at[at, pl.ds(k * cols, cols)], dz_v.at[pl.ds(k * re, re)], dzin_sem.at[k])
                    for k in range(BLOCKS)]
        return [pltpu.make_async_copy(dzt_ref.at[at, pl.ds(k * depth, depth)], (a_v, x_v)[k], dzin_sem.at[BLOCKS + k])
                for k in range(2)]

    def de_copy(c, i):
        return pltpu.make_async_copy(
            z_v.at[pl.ds(pl.multiple_of(i * re, re), re)],
            de_ref.at[pl.ds(pl.multiple_of(c * re, re), re), pl.ds(pl.multiple_of(i * nc, nc), nc)], de_sem.at[i])

    def de_chunk(c, odd, extra=None):
        for d in dzin_copies(c, odd):
            d.wait()

        def part(i, _):
            sl = pl.ds(pl.multiple_of(i * nc, nc), nc)

            @pl.when(c == 0)
            def _():
                xin_copy(i).wait()

            @pl.when(c >= 1)
            def _():
                de_copy(c - 1, i).wait()
            if odd:
                val = jnp.dot(dz_v[:re, :], e_v[:cols, sl], preferred_element_type=F32)
                for k in range(1, BLOCKS):
                    val = val + jnp.dot(dz_v[k * re:k * re + re, :], e_v[k * cols:k * cols + cols, sl], preferred_element_type=F32)
            else:
                val = jnp.dot(a_v[...], e_v[:depth, sl], preferred_element_type=F32)
                val = val + jnp.dot(x_v[...], e_v[depth:, sl], preferred_element_type=F32)
            z_v[pl.ds(pl.multiple_of(i * re, re), re), :] = val
            de_copy(c, i).start()
            if extra is not None:
                @pl.when(jnp.logical_and(c == KEEP - 1, i == npart - 2))
                def _():
                    extra()
            return 0
        lax.fori_loop(0, npart, part, 0)

        @pl.when(c + 2 < KEEP)
        def _():
            for d in dzin_copies(c + 2, odd):
                d.start()

    def inside(b, fn, name='svc'):
        @pl.when(jnp.logical_and(b >= 0, b < BLOCKS))
        def _():
            with jax.named_scope(name):
                fn(b)

    def between(j, lo, hi, fn, name='svc'):
        @pl.when(jnp.logical_and(j >= lo, j <= hi))
        def _():
            with jax.named_scope(name):
                fn()

    def x_copy(b):
        return pltpu.make_async_copy(x_v, xall_ref.at[pl.ds(pl.multiple_of(b * cols, cols), cols)], x_sem)

    def dz_copy(b):
        return pltpu.make_async_copy(dz_v, dzt_ref.at[:, pl.ds(pl.multiple_of(b * cols, cols), cols)], dz_sem)

    def loop(k, fn):
        def body(i, _):
            fn(i)
            return 0
        lax.fori_loop(0, k, body, 0)

    with jax.named_scope('p_h'):
        ld_h.wait()
    in1(0, 0)
    with jax.named_scope('p_w'):
        ld_w.wait()
    ld_e[0].start()
    with jax.named_scope('p_proj'):
        project(own_v.at[0], own_v.at[1])
    with jax.named_scope('p_in2'):
        in2(0, 0)
    span(in1, 1, 3)
    with jax.named_scope('p_code'):
        for r in range(1, n):
            code_copy(r).wait()
    code = code_ref[...]
    for r in range(1, n):
        code = code + crcv_v[r]
    mask = (code >= 65536).astype(jnp.int32)
    local = code - mask * 65536 - me * rows
    tgt_v[0:BLOCKS, :] = jnp.where(jnp.logical_and(local >= 0, local < rows), local, -(1 << 24))
    maskf = mask.astype(F32)
    msk_v[...] = maskf
    per_col = jnp.sum(maskf, axis=0, keepdims=True)
    n0 = jnp.sum(per_col[:, :tok], axis=1, keepdims=True)
    n1 = jnp.sum(per_col[:, tok:], axis=1, keepdims=True)
    counts = jnp.concatenate([jnp.broadcast_to(n0, (1, tok)), jnp.broadcast_to(n1, (1, tok))], axis=1)
    wgt_v[...] = maskf / counts
    tot_v[0:1, :] = jnp.zeros((1, cols), F32)
    tot_v[1:2, :] = counts
    gsrc_v[...] = jnp.zeros_like(gsrc_v)
    with jax.named_scope('p_in3'):
        in3(0, 0)
    with jax.named_scope('p_fetch'):
        gather4(aall_ref.at[0, 0], h_send.at[0, 0], h_recv.at[0, 0])
        first = [a_copy(0, 0, kk, c) for kk in range(2) for c in range(CHIPS)]
        for c in first:
            c.start()
        for c in first:
            c.wait()
    with jax.named_scope('p_proj0'):
        project(a_v.at[pl.ds(0, tok)], a_v.at[pl.ds(tok, tok)])
    ld_e[1].start()
    ld_e[0].wait()

    def last_stage(b):
        rs4(b)
        dg1(b)

    def gather_b0():
        span(in2, 1, 2)
        span(in1, 3, 4)

    def gather_d0():
        ld_e[1].wait()
        span(in3, 1, 2)
        span(in2, 2, 3)
        span(in1, 4, 5)

    def gather_e0():
        span(in3, 2, 3)
        span(in2, 3, 4)
        span(in1, 5, 6)

    def gather_e1():
        span(in3, 3, 4)
        span(in2, 4, 6)
        span(in1, 6, 8)

    def gather_b2():
        span(in3, 4, 6)

    def gather_e2():
        span(in2, 6, 8)

    def gather_b3():
        span(in3, 6, 8)

    def step(t, _):
        j = t - 1
        def last_dg3():
            dg3(BLOCKS - 2)
            dg3(BLOCKS - 1)

        def block_wait():
            for c in block_copies(j + 1):
                c.wait()
        between(j, 0, BLOCKS - 2, block_wait, 'bwait')
        between(j, 1, BLOCKS, lambda: x_wait(j), 'xwait')

        def full_a():
            def body(i):
                dx_part(i, (j - 1) % 3)
                norm_part(i)
            loop(npart, body)
        between(j, -1, 0, lambda: loop(npart, norm_part), 'norm')
        between(j, 1, BLOCKS - 2, full_a, 'full_a')
        between(j, BLOCKS, BLOCKS, start_tail, 'start_tail')

        def last_a(i):
            dx_part(i, (j - 1) % 3)

            @pl.when(j == BLOCKS)
            def _():
                xin_copy(i).start()
        between(j, BLOCKS - 1, BLOCKS, lambda: loop(npart, last_a), 'last_a')
        between(j, BLOCKS + 1, BLOCKS + 3, lambda: de_chunk(2 * (j - BLOCKS) - 1, True, last_dg3), 'de_a')
        between(j, -1, BLOCKS - 2, lambda: x_copy(j + 1).start(), 'xstart')
        between(j, BLOCKS, BLOCKS, start_odd, 'start_odd')
        inside(j - 1, rs1, 'rs1')
        between(j, -1, -1, gather_b0, 'gb0')
        between(j, 1, 1, gather_b2, 'gb2')
        between(j, 2, 2, gather_b3, 'gb3')
        between(j, 1, BLOCKS - 3, lambda: fetch_block(j + 2), 'fetch')
        between(j, BLOCKS, BLOCKS, lambda: rs3(BLOCKS - 3), 'rs3')
        def late_stages():
            def body(b, _):
                last_stage(b)
                return 0
            lax.fori_loop(j - 4, 2 * j - BLOCKS - 4, body, 0)
        between(j, BLOCKS + 1, BLOCKS + 2, late_stages, 'rs4late')
        inside(j, join_stats, 'join')
        between(j, 1, BLOCKS - 1, lambda: dz_copy(j - 1).wait(), 'dzwait')
        between(j, BLOCKS, BLOCKS + 2, lambda: de_chunk(2 * (j - BLOCKS), False), 'de_d')

        def start_stats():
            ms_v[0] = jnp.full((8, cols), -3.0e38, F32)
            ms_v[1] = jnp.zeros((8, cols), F32)
            ms_v[2] = jnp.zeros((8, cols), F32)
            tgt_v[pl.ds(9, 1), :] = tgt_v[pl.ds(j + 1, 1), :]
        between(j, -1, BLOCKS - 2, start_stats)

        def first_d(i):
            d_body(i, False, True)

            @pl.when(i == 0)
            def _():
                gather_d0()
        between(j, -1, -1, lambda: loop(nr, first_d), 'only_z')
        def mid_d(i):
            d_body(i, True, True)

            @pl.when(i == 0)
            def _():
                between(j, 0, 0, lambda: fetch_block(2), 'fetch')
        between(j, 0, BLOCKS - 2, lambda: loop(nr, mid_d), 'full_d')
        between(j, BLOCKS - 1, BLOCKS - 1, lambda: loop(nr, lambda i: d_body(i, True, False)), 'back')
        between(j, -1, -1, lambda: fetch_block(1), 'fetch')
        between(j, -1, BLOCKS - 2, lambda: send_stats(j + 1), 'stats')
        inside(j, lambda b: dz_copy(b).start(), 'dzstart')
        between(j, 2, BLOCKS - 2, lambda: rs3(j - 2), 'rs3')
        between(j, BLOCKS, BLOCKS + 1, lambda: rs3(j - 2), 'rs3')
        between(j, 3, BLOCKS - 1, lambda: last_stage(j - 3), 'rs4g1')
        between(j, 4, BLOCKS + 2, lambda: dg2(j - 4), 'dg2')
        between(j, -1, -1, gather_e0, 'ge0')
        between(j, 0, 0, gather_e1, 'ge1')
        between(j, 1, 1, gather_e2, 'ge2')
        between(j, 5, BLOCKS + 2, lambda: dg3(j - 5), 'dg3')
        inside(j - 1, rs2, 'rs2')
        between(j, BLOCKS + 2, BLOCKS + 2, lambda: dg2(BLOCKS - 1), 'dg2last')
        between(j, BLOCKS + 2, BLOCKS + 2, gb_start, 'gbstart')
        return 0

    def gb_copy(r):
        return remote(gsrc_v, grcv_v.at[r], gb_send.at[r], gb_recv.at[r], (me + r) % n)

    def gb_start():
        for r in range(1, n):
            gb_copy(r).start()

    def start_tail():
        dz_copy(BLOCKS - 1).wait()
        for d in dzin_copies(0, False):
            d.start()

    def start_odd():
        for d in dzin_copies(1, True):
            d.start()

    def x_wait(j):
        @pl.when(j <= BLOCKS - 1)
        def _():
            x_copy(j).wait()

    def first_x(j):
        x_copy(j).wait()

    def step_outer(t, c):
        @pl.when(t == 1)
        def _():
            first_x(0)
        return step(t, c)

    lax.fori_loop(0, BLOCKS + 5, step_outer, 0)

    with jax.named_scope('e_g4'):
        for b in range(BLOCKS):
            gather4(dgall_ref.at[b], g_send.at[b], g_recv.at[b])
    with jax.named_scope('e_out'):
        for c in out_copies(BLOCKS - 1):
            c.wait()
    with jax.named_scope('e_de'):
        for i in range(npart):
            de_copy(KEEP - 1, i).wait()
    with jax.named_scope('e_gb'):
        for r in range(1, n):
            gb_copy(r).wait()
    with jax.named_scope('e_sum'):
        acc = gsrc_v[...]
        for r in range(1, n):
            acc = acc + grcv_v[r]
        dgb_ref[...] = acc
        total_ref[...] = jnp.broadcast_to(jnp.sum(tot_v[0:1, :], axis=1, keepdims=True), total_ref.shape)


def stream(n, hidden, w_two, gain, bias, embed, code):
    tokens, depth = hidden.shape
    rows = embed.shape[0]
    q = tokens // BLOCKS
    half = CHIPS * q
    tok = 2 * half
    cols = 2 * tok
    nc = depth // 4
    rc, sub = rows // 2, rows // 8
    assert BLOCKS * cols == rows == 2 * depth and nc == cols
    dims = (n, q, depth, rows, rc, nc, sub)
    any_spec = pl.BlockSpec(memory_space=pl.ANY)
    vmem = pl.BlockSpec(memory_space=pltpu.VMEM)
    dma = pltpu.SemaphoreType.DMA
    sds = jax.ShapeDtypeStruct
    return pl.pallas_call(
        functools.partial(stream_kernel, dims),
        out_shape=(sds((BLOCKS, 2, 2, CHIPS, q, depth), BF16), sds((BLOCKS * cols, depth), BF16),
                   sds((rows, BLOCKS * cols), BF16), sds((BLOCKS, 2, CHIPS, q, depth), BF16),
                   sds((BLOCKS, q, depth), F32), sds((BLOCKS, q, depth), BF16),
                   sds((BLOCKS, cols), F32), sds((8, 128), F32), sds((8, depth), F32),
                   sds((KEEP * (rows // BLOCKS), depth), F32)),
        in_specs=[any_spec, any_spec, vmem, vmem, any_spec, vmem],
        out_specs=(any_spec,) * 6 + (vmem,) * 3 + (any_spec,),
        scratch_shapes=[
            pltpu.VMEM((rows, depth), BF16),
            pltpu.VMEM((cols, depth), BF16), pltpu.VMEM((cols, depth), BF16),
            pltpu.VMEM((rows, cols), F32), pltpu.VMEM((rows, cols), BF16),
            pltpu.VMEM((3, 2, 2, half, depth), F32), pltpu.VMEM((2, 2, half, depth), F32),
            pltpu.VMEM((4, 2, q, depth), F32), pltpu.VMEM((5, 2, 2, q, depth), F32),
            pltpu.VMEM((2, tokens, depth), BF16),
            pltpu.VMEM((4, q, depth), BF16), pltpu.VMEM((q, depth), F32),
            pltpu.VMEM((2, 8, cols), F32), pltpu.VMEM((2, n, 8, cols), F32),
            pltpu.VMEM((n, BLOCKS, cols), jnp.int32), pltpu.VMEM((16, cols), jnp.int32),
            pltpu.VMEM((BLOCKS, cols), F32), pltpu.VMEM((BLOCKS, cols), F32),
            pltpu.VMEM((3, 8, cols), F32), pltpu.VMEM((8, cols), F32), pltpu.VMEM((8, cols), F32),
            pltpu.VMEM((8, depth), F32), pltpu.VMEM((n, 8, depth), F32),
            dma((4,)), dma((BLOCKS, 2, 8)), dma((BLOCKS, 2, 8)), dma((BLOCKS, 2)), dma((BLOCKS, 8)), dma((BLOCKS, 8)),
            dma((BLOCKS,)), dma((2, n)), dma((2, n)), dma((2,)), dma((2,)), dma((3, 4)), dma((3, 2)),
            dma((4, 2)), dma((5, 2, 2)), pltpu.SemaphoreType.REGULAR,
            dma((n,)), dma((n,)), dma, dma, dma((4 * CHIPS,)), dma((2,)), dma((n,)), dma((n,)),
            dma((depth // nc,)), dma((BLOCKS + 2,)), dma((depth // nc,)),
        ],
        compiler_params=pltpu.CompilerParams(collective_id=0, has_side_effects=True, vmem_limit_bytes=67043328),
        name='stream',
    )(hidden, w_two, gain, bias, embed, code)


def dense_kernel(part_ref, dzt_ref, xall_ref, aall_ref, gall_ref, da_ref, go_ref, w_ref, loss_ref, sum_ref, dgb_ref,
                 de_ref, dw_ref, dh_ref, tl_ref, total_ref, gs_ref, gb_ref,
                 da_v, go_v, w_v, g_v, x_v, h_v, dw_v, dz_v, de_v, st_v, w_sem, g_sem, x_sem, h_sem, dw_sem, dz_sem, de_sem, in_sem, out_sem, a_sem):
    depth = x_v.shape[1]
    nc, wb = depth // 4, depth // BLOCKS
    re = dzt_ref.shape[0] // BLOCKS
    xr = x_v.shape[0] // BLOCKS
    todo = BLOCKS - KEEP
    pieces = BLOCKS + 8 * todo
    pr = KEEP * re // pieces

    def at(i, size):
        return pl.ds(pl.multiple_of(i * size, size), size)

    def w_copy(i):
        return pltpu.make_async_copy(w_ref.at[at(i, nc)], w_v.at[at(i, nc)], w_sem.at[i])

    def h_copy(i):
        return pltpu.make_async_copy(aall_ref.at[:, 0:h_v.shape[2], at(i, wb)], h_v.at[i % 2], h_sem.at[i % 2])

    def dw_copy(i):
        return pltpu.make_async_copy(dw_v.at[i % 2], dw_ref.at[at(i, wb)], dw_sem.at[i % 2])

    def x_copy(i):
        return pltpu.make_async_copy(xall_ref.at[at(i, xr)], x_v.at[at(i, xr)], x_sem.at[i])

    def dz_copy(c):
        return pltpu.make_async_copy(dzt_ref.at[at(KEEP + c, re)], dz_v.at[c % 2], dz_sem.at[c % 2])

    def de_copy(u):
        return pltpu.make_async_copy(de_v.at[u % 2], de_ref.at[at(KEEP + u // 4, re), at(u % 4, nc)], de_sem.at[u % 2])

    def pin(t):
        return pltpu.make_async_copy(part_ref.at[at(t, pr)], st_v.at[t % 4], in_sem.at[t % 4])

    def pout(t):
        return pltpu.make_async_copy(st_v.at[t % 4], de_ref.at[at(t, pr)], out_sem.at[t % 4])

    def carry(t):
        pin(t).wait()
        pout(t).start()

        @pl.when(t >= 2)
        def _():
            pout(t - 2).wait()

        @pl.when(t + 2 < pieces)
        def _():
            pin(t + 2).start()

    g_load = pltpu.make_async_copy(gall_ref, g_v, g_sem)
    da_load = pltpu.make_async_copy(da_ref, da_v, a_sem.at[0])
    go_load = pltpu.make_async_copy(go_ref, go_v, a_sem.at[1])
    go_load.start()
    w_copy(0).start()
    da_load.start()
    for i in range(1, 4):
        w_copy(i).start()
    g_load.start()
    h_copy(0).start()
    h_copy(1).start()
    pin(0).start()
    pin(1).start()

    go_load.wait()
    da_load.wait()

    def hidden_part(i, _):
        w_copy(i).wait()
        sl = at(i, nc)
        back = lax.dot_general(go_v[...], w_v[sl, :], (((1,), (1,)), ((), ())), preferred_element_type=F32)
        dh_ref[:, sl] = (da_v[:, sl] + back).astype(BF16)
        return 0
    with jax.named_scope('k2_dh'):
        lax.fori_loop(0, 4, hidden_part, 0)
    gs_ref[...] = dgb_ref[0:2, :]
    gb_ref[...] = dgb_ref[2:4, :]
    total_ref[0] = sum_ref[0, 0]
    me = lax.axis_index('tp')
    lanes = loss_ref.shape[1]
    q = lanes // 2 // (2 * CHIPS)
    place = (me % 2) * CHIPS + me // 2
    for h in range(2):
        turned = pltpu.roll(loss_ref[...], (lanes - h * (lanes // 2) - place * q) % lanes, 1)
        tl_ref[h:h + 1, :] = jnp.concatenate([turned[b:b + 1, :q] for b in range(BLOCKS)], axis=1)
    with jax.named_scope('k2_g'):
        g_load.wait()

    def dw_part(i, _):
        h_copy(i).wait()
        carry(i)

        @pl.when(i < BLOCKS // 2)
        def _():
            x_copy(2 * i).start()
            x_copy(2 * i + 1).start()

        @pl.when(i == BLOCKS // 2)
        def _():
            dz_copy(0).start()

        @pl.when(i == BLOCKS // 2 + 2)
        def _():
            dz_copy(1).start()
        @pl.when(i >= 2)
        def _():
            dw_copy(i - 2).wait()
        h = h_v[i % 2].reshape(g_v.shape[0], wb)
        dw_v[i % 2] = lax.dot_general(h, g_v[...], (((0,), (0,)), ((), ())), preferred_element_type=F32)
        dw_copy(i).start()

        @pl.when(i + 2 < BLOCKS)
        def _():
            h_copy(i + 2).start()
        return 0
    with jax.named_scope('k2_dw'):
        lax.fori_loop(0, BLOCKS, dw_part, 0)
    with jax.named_scope('k2_x'):
        for i in range(BLOCKS):
            x_copy(i).wait()

    def de_part(u, _):
        c = u // 4

        @pl.when(u % 4 == 0)
        def _():
            dz_copy(c).wait()
        carry(BLOCKS + 2 * u)

        @pl.when(u >= 2)
        def _():
            de_copy(u - 2).wait()
        de_v[u % 2] = jnp.dot(dz_v[c % 2], x_v[:, at(u % 4, nc)], preferred_element_type=F32)
        de_copy(u).start()
        carry(BLOCKS + 2 * u + 1)

        @pl.when(jnp.logical_and(u % 4 == 3, c + 2 < todo))
        def _():
            dz_copy(c + 2).start()
        return 0
    with jax.named_scope('k2_de'):
        lax.fori_loop(0, 4 * todo, de_part, 0)
    for i in (BLOCKS - 2, BLOCKS - 1):
        dw_copy(i).wait()
    for i in (4 * todo - 2, 4 * todo - 1):
        de_copy(i).wait()
    for t in (pieces - 2, pieces - 1):
        pout(t).wait()


def dense(part, dzt, xall, aall, gall, da1, dgown, w_two, loss, total_loss, dgb):
    rows, kk = dzt.shape
    depth = xall.shape[1]
    total, tokens = gall.shape[0], da1.shape[0]
    re, wb, nc = rows // BLOCKS, depth // BLOCKS, depth // 4
    pieces = BLOCKS + 8 * (BLOCKS - KEEP)
    sds = jax.ShapeDtypeStruct
    dma = pltpu.SemaphoreType.DMA
    any_spec = pl.BlockSpec(memory_space=pl.ANY)
    vmem = pl.BlockSpec(memory_space=pltpu.VMEM)
    return pl.pallas_call(
        dense_kernel,
        out_shape=(sds((rows, depth), F32), sds((depth, depth), F32), sds((tokens, depth), BF16), sds((2, tokens), F32),
                   sds((1,), F32), sds((2, depth), F32), sds((2, depth), F32)),
        in_specs=[any_spec] * 8 + [vmem] * 3,
        out_specs=(any_spec, any_spec, vmem, vmem, pl.BlockSpec(memory_space=pltpu.SMEM), vmem, vmem),
        scratch_shapes=[pltpu.VMEM((tokens, depth), F32), pltpu.VMEM((tokens, depth), BF16), pltpu.VMEM((depth, depth), BF16), pltpu.VMEM((total, depth), BF16), pltpu.VMEM((kk, depth), BF16),
                        pltpu.VMEM((2, BLOCKS, total // BLOCKS, wb), BF16), pltpu.VMEM((2, wb, depth), F32),
                        pltpu.VMEM((2, re, kk), BF16), pltpu.VMEM((2, re, nc), F32),
                        pltpu.VMEM((4, KEEP * re // pieces, depth), F32),
                        dma((4,)), dma, dma((BLOCKS,)), dma((2,)), dma((2,)), dma((2,)), dma((2,)), dma((4,)), dma((4,)), dma((2,))],
        compiler_params=pltpu.CompilerParams(vmem_limit_bytes=67043328),
        name='dense',
    )(part, dzt, xall, aall, gall, da1, dgown, w_two, loss, total_loss, dgb)


def solution(mesh):
    n = mesh.shape['tp']
    tok_spec = P(('dp', 'tp'), None)
    row_spec = P(None, ('dp', 'tp'))

    def device_step(hidden, w_two, ln_scale, ln_shift, embed, targets, loss_mask):
        tokens, depth = hidden.shape
        q = tokens // BLOCKS
        me = lax.axis_index('tp')
        code = (targets + 65536 * loss_mask).reshape(2, BLOCKS, q).transpose(1, 0, 2)
        place = (me % 2) * CHIPS + me // 2
        seat = lax.broadcasted_iota(jnp.int32, (1, 1, 2 * CHIPS, 1), 2) == place
        code = jnp.where(seat, code[:, :, None, :], 0).reshape(BLOCKS, 2 * 2 * CHIPS * q)
        aall, xall, dzt, dgall, da1, dgown, loss, total, dgb, part = stream(
            n, hidden, w_two, ln_scale, ln_shift, embed, code)
        d_embed, d_w, d_hidden, token_loss, total_loss, d_scale, d_shift = dense(
            part, dzt, xall, aall.reshape(BLOCKS, 2 * n * q, depth), dgall.reshape(n * tokens, depth),
            da1.reshape(tokens, depth), dgown.reshape(tokens, depth), w_two, loss, total, dgb)
        return token_loss, total_loss, d_hidden, d_embed, d_w, d_scale, d_shift

    return jax.shard_map(device_step, mesh=mesh,
                         in_specs=(tok_spec, P(), P(), P(), P('tp', None), row_spec, row_spec),
                         out_specs=(row_spec, P('dp'), tok_spec, tok_spec, P('dp', None), P('dp', None), P('dp', None)),
                         check_vma=False)
```

```python
import functools

import jax
import jax.numpy as jnp
from jax import lax
from jax.experimental import pallas as pl
from jax.experimental.pallas import tpu as pltpu
from jax.sharding import PartitionSpec as P

LN_EPS = 1e-5
CHIPS = 4
BLOCKS = 8
KEEP = 6
WAYS = 4
LANES = 2
F32 = jnp.float32
BF16 = jnp.bfloat16


def to(idx):
    return dict(device_id={'tp': idx}, device_id_type=pl.DeviceIdType.MESH)


def remote(src, dst, send, recv, idx):
    return pltpu.make_async_remote_copy(src_ref=src, dst_ref=dst, send_sem=send, recv_sem=recv, **to(idx))


def stream_kernel(dims, h_ref, w_ref, gain_ref, bias_ref, e_ref, code_ref,
                  aall_ref, xall_ref, dzt_ref, dgall_ref, da1_ref, dgown_ref, loss_ref, total_ref, dgb_ref, de_ref,
                  e_v, a_v, x_v, z_v, dz_v, dx_v, pr_v, mg_v, ow_v, own_v, dg_v, da_v,
                  stsrc_v, strcv_v, crcv_v, tgt_v, msk_v, wgt_v, ms_v, row_v, tot_v, gsrc_v, grcv_v,
                  ld_sem, h_send, h_recv, h_loc, g_send, g_recv, g_loc,
                  st_send, st_recv, pr_send, pr_recv, r2_send, r3_send, mg_recv, ow_recv, pair_free,
                  cd_send, cd_recv, x_sem, dz_sem, a_sem, out_sem, gb_send, gb_recv, xin_sem, dzin_sem, de_sem):
    n, q, depth, rows, rc, nc, sub = dims
    re = rows // BLOCKS
    half = CHIPS * q
    tok = 2 * half
    cols = 2 * tok
    me = lax.axis_index('tp')
    chip = me // 2
    core = me % 2
    peer = me + 1 - 2 * core
    right_chip = (chip + 1) % CHIPS
    left_chip = (chip + CHIPS - 1) % CHIPS
    far_chip = (chip + 2) % CHIPS
    right = right_chip * 2 + core
    left = left_chip * 2 + core

    top, bottom = pl.ds(0, depth), pl.ds(depth, rows - depth)
    ld_e = [pltpu.make_async_copy(e_ref.at[d], e_v.at[d], ld_sem.at[i]) for i, d in ((0, top), (3, bottom))]
    ld_w = pltpu.make_async_copy(w_ref, e_v.at[bottom], ld_sem.at[1])
    ld_h = pltpu.make_async_copy(h_ref, own_v.at[0], ld_sem.at[2])
    ld_h.start()
    ld_w.start()

    barrier = pltpu.get_barrier_semaphore()
    for r in range(1, n):
        pl.semaphore_signal(barrier, inc=1, **to((me + r) % n))
    pl.semaphore_wait(barrier, n - 1)

    def wait_bytes(ref, sem):
        pltpu.make_async_copy(ref, ref, sem).wait()

    def code_copy(r):
        return remote(code_ref, crcv_v.at[r], cd_send, cd_recv, (me + r) % n)

    for r in range(1, n):
        code_copy(r).start()

    lo, hi = pl.ds(0, q // 2), pl.ds(q // 2, q // 2)

    def g1_copies(src, dst, send, recv):
        piece = dst.at[core, chip]
        return (remote(src, piece, send.at[0], recv.at[0], right),
                remote(src, piece, send.at[0], recv.at[1], left),
                remote(src, piece, send.at[0], recv.at[3], peer))

    def g2_copies(dst, send, recv):
        fl, fr = dst.at[core, left_chip], dst.at[core, right_chip]
        return (remote(fl.at[lo], fl.at[lo], send.at[1], recv.at[2], right),
                remote(fr.at[hi], fr.at[hi], send.at[1], recv.at[2], left),
                remote(fl, fl, send.at[1], recv.at[3], peer),
                remote(fr, fr, send.at[1], recv.at[3], peer))

    def gather1(src, dst, send, recv, loc):
        for c in g1_copies(src, dst, send, recv):
            c.start()
        pltpu.make_async_copy(src, dst.at[core, chip], loc).start()

    def gather2(src, dst, send, recv, loc):
        wait_bytes(dst.at[core, left_chip], recv.at[0])
        wait_bytes(dst.at[core, right_chip], recv.at[1])
        for c in g2_copies(dst, send, recv):
            c.start()
        wait_bytes(dst.at[core, pl.ds(0, 3)], send.at[0])
        pltpu.make_async_copy(src, dst.at[core, chip], loc).wait()

    def gather3(dst, send, recv):
        far = dst.at[core, far_chip]
        wait_bytes(far, recv.at[2])
        remote(far, far, send.at[2], recv.at[3], peer).start()
        wait_bytes(dst.at[core, pl.ds(0, 3)], send.at[1])

    def gather4(dst, send, recv):
        wait_bytes(dst.at[1 - core], recv.at[3])
        wait_bytes(dst.at[core, far_chip], send.at[2])

    def own(b, h):
        return own_v.at[h, pl.ds(pl.multiple_of(b * q, q), q)]

    def in1(b, h):
        gather1(own(b, h), aall_ref.at[b, h], h_send.at[b % 4, h], h_recv.at[b, h], h_loc.at[b % 4, h])

    def in2(b, h):
        gather2(own(b, h), aall_ref.at[b, h], h_send.at[b % 4, h], h_recv.at[b, h], h_loc.at[b % 4, h])

    def in3(b, h):
        gather3(aall_ref.at[b, h], h_send.at[b % 4, h], h_recv.at[b, h])

    def dg1(b):
        gather1(dg_v.at[b % 4], dgall_ref.at[b], g_send.at[b], g_recv.at[b], g_loc.at[b])

    def dg2(b):
        gather2(dg_v.at[b % 4], dgall_ref.at[b], g_send.at[b], g_recv.at[b], g_loc.at[b])

    def dg3(b):
        gather3(dgall_ref.at[b], g_send.at[b], g_recv.at[b])

    def span(fn, lo, hi):
        def body(u, _):
            fn(u // 2, u % 2)
            return 0
        lax.fori_loop(2 * lo, 2 * hi, body, 0)

    def a_copy(b, h, kk, c):
        at = pl.ds(((h * 2 + kk) * CHIPS + c) * q, q)
        return pltpu.make_async_copy(aall_ref.at[b, h, kk, c], a_v.at[at], a_sem)

    def block_copies(b):
        return [a_copy(b, h, kk, c) for h in range(2) for kk in range(2) for c in range(CHIPS)]

    def fetch_block(b):
        for h in range(2):
            gather4(aall_ref.at[b, h], h_send.at[b % 4, h], h_recv.at[b, h])
        for c in block_copies(b):
            c.start()

    def project(src, dst):
        def proj(i, _):
            sl = pl.ds(pl.multiple_of(i * nc, nc), nc)
            dst[:, sl] = jnp.dot(src[...], e_v[bottom, sl], preferred_element_type=F32).astype(BF16)
            return 0
        lax.fori_loop(0, depth // nc, proj, 0)

    def norm_rows(start, head):
        a = a_v[pl.ds(start, 16), :].astype(F32)
        mean = jnp.mean(a, axis=-1, keepdims=True)
        cent = a - mean
        var = jnp.mean(cent * cent, axis=-1, keepdims=True)
        y = cent * lax.rsqrt(var + LN_EPS) * gain_ref[pl.ds(head, 1), :] + bias_ref[pl.ds(head, 1), :]
        x_v[pl.ds(start, 16), :] = y.astype(BF16)

    npart = depth // nc
    lrows = cols // npart

    def norm_part(i):
        head = (i * lrows) // tok
        for s in range(lrows // 16):
            norm_rows(pl.multiple_of(i * lrows + s * 16, 16), head)

    def dx_part(i, slot):
        sl = pl.ds(pl.multiple_of(i * nc, nc), nc)
        val = lax.dot_general(dz_v[...], e_v[:, sl], (((0,), (0,)), ((), ())), preferred_element_type=F32)
        for h in range(2):
            for kk in range(2):
                base = h * tok + kk * half
                dx_v[slot, kk, h, :, sl] = val[base:base + half, :]

    nr = rows // rc

    def tree(parts, op):
        while len(parts) > 1:
            parts = [op(a, b) for a, b in zip(parts[::2], parts[1::2])]
        return parts[0]

    def part_view(ref, i):
        return ref.at[pl.ds(pl.multiple_of(i * rc, rc), rc)]

    def back_part(i, p, lanes, td):
        shift, w = row_v[0:1, lanes], row_v[1:2, lanes]
        zc, dc = part_view(z_v, i), part_view(dz_v, i)
        for s in range(p * sub, p * sub + sub, 16):
            both = []
            for t in (s, s + 8):
                pw = jnp.exp(zc[t:t + 8, lanes] - shift)
                both.append(jnp.where(td == t, pw - w, pw))
            dc[s:s + 16, lanes] = jnp.concatenate(both, axis=0).astype(BF16)

    def z_part(i, p):
        ec = part_view(e_v, i)
        part_view(z_v, i)[p * sub:p * sub + sub, :] = lax.dot_general(
            ec[p * sub:p * sub + sub, :], x_v[...], (((1,), (1,)), ((), ())), preferred_element_type=F32)

    def stat_part(i, p, lanes, td, state):
        zc = part_view(z_v, i)
        m_old, acc, tl = state
        at = range(p * sub, p * sub + sub, 8)
        tops = [zc[s:s + 8, lanes] for s in at[:WAYS]]
        for k, s in enumerate(at[WAYS:]):
            tops[k % WAYS] = jnp.maximum(tops[k % WAYS], zc[s:s + 8, lanes])
        m = jnp.maximum(m_old, tree(tops, jnp.maximum))
        accs = [None] * WAYS
        for k, s in enumerate(at):
            z = zc[s:s + 8, lanes]
            e = jnp.exp(z - m)
            accs[k % WAYS] = e if accs[k % WAYS] is None else accs[k % WAYS] + e
            tl = jnp.where(td == s, z, tl)
        return m, acc * jnp.exp(m_old - m) + tree(accs, jnp.add), tl

    def d_body(i, back, new):
        span = cols // LANES
        iota = lax.broadcasted_iota(jnp.int32, (8, span), 0)
        cut = [slice(k * span, k * span + span) for k in range(LANES)]
        td_old = [tgt_v[pl.ds(8, 1), c] - i * rc - iota for c in cut]
        td_new = [tgt_v[pl.ds(9, 1), c] - i * rc - iota for c in cut]
        state = [tuple(ms_v[k, :, c] for k in range(3)) for c in cut]
        for p in range(rc // sub):
            if back:
                for k in range(LANES):
                    back_part(i, p, cut[k], td_old[k])
            if new:
                z_part(i, p)
                for k in range(LANES):
                    state[k] = stat_part(i, p, cut[k], td_new[k], state[k])
        if new:
            for k in range(LANES):
                for q_ in range(3):
                    ms_v[q_, :, cut[k]] = state[k][q_]

    def stat_copy(slot, r):
        return remote(stsrc_v.at[slot], strcv_v.at[slot, r], st_send.at[slot], st_recv.at[slot], (me + r) % n)

    def send_stats(b):
        slot = b % 2
        m = ms_v[0]
        top = jnp.max(m, axis=0, keepdims=True)
        stsrc_v[slot, 0:1, :] = top
        stsrc_v[slot, 1:2, :] = jnp.sum(ms_v[1] * jnp.exp(m - top), axis=0, keepdims=True)
        stsrc_v[slot, 2:3, :] = jnp.sum(ms_v[2], axis=0, keepdims=True)
        for r in range(1, n):
            stat_copy(slot, r).start()

    def join_stats(b):
        slot = b % 2
        wait_bytes(strcv_v.at[slot, pl.ds(1, n - 1)], st_send.at[slot])
        wait_bytes(strcv_v.at[slot, pl.ds(1, n - 1)], st_recv.at[slot])
        parts = [stsrc_v[slot]] + [strcv_v[slot, r] for r in range(1, n)]
        top = parts[0][0:1]
        for p in parts[1:]:
            top = jnp.maximum(top, p[0:1])
        total = jnp.zeros_like(top)
        hit = jnp.zeros_like(top)
        for p in parts:
            total = total + p[1:2] * jnp.exp(p[0:1] - top)
            hit = hit + p[2:3]
        lse = top + jnp.log(total)
        w = wgt_v[pl.ds(b, 1), :]
        row_v[0:1, :] = jnp.where(w > 0.0, lse - jnp.log(jnp.where(w > 0.0, w, 1.0)), 3.0e38)
        row_v[1:2, :] = w
        tgt_v[pl.ds(8, 1), :] = tgt_v[pl.ds(b, 1), :]
        loss = (lse - hit) * msk_v[pl.ds(b, 1), :]
        loss_ref[pl.ds(b, 1), :] = loss
        tot_v[0:1, :] = tot_v[0:1, :] + loss / tot_v[1:2, :]

    def pair_copy(b):
        slot = b % 2
        return remote(dx_v.at[b % 3, 1 - core], pr_v.at[slot], pr_send.at[slot], pr_recv.at[slot], peer)

    def rs1(b):
        @pl.when(b >= 2)
        def _():
            pl.semaphore_wait(pair_free, 1)
        pair_copy(b).start()

    def crow(c):
        return pl.ds(pl.multiple_of(c * q, q), q)

    def r2_copies(b):
        mine, s3, mg, ow = dx_v.at[b % 3, core], b % 3, b % 4, b % 5
        return (remote(mine.at[0, crow(far_chip)], mg_v.at[mg, 0], r2_send.at[s3], mg_recv.at[mg], right),
                remote(mine.at[1, crow(far_chip)], mg_v.at[mg, 1], r2_send.at[s3], mg_recv.at[mg], left),
                remote(mine.at[1, crow(right_chip)], ow_v.at[ow, 0, 1], r2_send.at[s3], ow_recv.at[ow], right),
                remote(mine.at[0, crow(left_chip)], ow_v.at[ow, 1, 0], r2_send.at[s3], ow_recv.at[ow], left))

    def rs2(b):
        slot, s3 = b % 2, b % 3
        pair_copy(b).wait()

        def add(i, _):
            h = i // CHIPS
            c = i % CHIPS
            dx_v[s3, core, h, crow(c), :] += pr_v[slot, h, crow(c), :]
            return 0
        lax.fori_loop(0, 2 * CHIPS, add, 0)

        @pl.when(b < BLOCKS - 2)
        def _():
            pl.semaphore_signal(pair_free, inc=1, **to(peer))
        for c in r2_copies(b):
            c.start()

    def r3_copies(b):
        mine, s3, ow = dx_v.at[b % 3, core], b % 3, b % 5
        return (remote(mine.at[0, crow(right_chip)], ow_v.at[ow, 0, 0], r3_send.at[s3], ow_recv.at[ow], right),
                remote(mine.at[1, crow(left_chip)], ow_v.at[ow, 1, 1], r3_send.at[s3], ow_recv.at[ow], left))

    def rs3(b):
        s3, mg = b % 3, b % 4
        wait_bytes(mg_v.at[mg], mg_recv.at[mg])
        dx_v[s3, core, 0, crow(right_chip), :] += mg_v[mg, 0]
        dx_v[s3, core, 1, crow(left_chip), :] += mg_v[mg, 1]
        for c in r3_copies(b):
            c.start()

    def rs4(b):
        ow = b % 5
        wait_bytes(ow_v.at[ow], ow_recv.at[ow])

        @pl.when(b >= 1)
        def _():
            out_copies(b - 1)[0].wait()
            out_copies(b - 1)[1].wait()
        for h in range(2):
            dy = dx_v[b % 3, core, h, crow(chip), :] + ow_v[ow, 0, h] + ow_v[ow, 1, h]
            a = own(b, h)[...].astype(F32)
            mean = jnp.mean(a, axis=-1, keepdims=True)
            cent = a - mean
            rstd = lax.rsqrt(jnp.mean(cent * cent, axis=-1, keepdims=True) + LN_EPS)
            xhat = cent * rstd
            gsrc_v[h:h + 1, :] += jnp.sum(dy * xhat, axis=0, keepdims=True)
            gsrc_v[2 + h:3 + h, :] += jnp.sum(dy, axis=0, keepdims=True)
            dxh = dy * gain_ref[h:h + 1, :]
            c1 = jnp.mean(dxh, axis=-1, keepdims=True)
            c2_ = jnp.mean(dxh * xhat, axis=-1, keepdims=True)
            da = rstd * (dxh - c1 - xhat * c2_)
            if h == 0:
                da_v[...] = da
            else:
                dg_v[b % 4] = da.astype(BF16)
        for c in out_copies(b):
            c.start()
        wait_bytes(ow_v.at[ow], r2_send.at[b % 3])
        wait_bytes(mg_v.at[b % 4], r3_send.at[b % 3])

    def out_copies(b):
        return (pltpu.make_async_copy(da_v, da1_ref.at[b], out_sem.at[0]),
                pltpu.make_async_copy(dg_v.at[b % 4], dgown_ref.at[b], out_sem.at[1]))

    def xin_copy(i):
        sl = pl.ds(pl.multiple_of(i * nc, nc), nc)
        return pltpu.make_async_copy(xall_ref.at[:, sl], e_v.at[:, sl], xin_sem.at[i])

    def dzin_copies(c, odd):
        at = pl.ds(pl.multiple_of(c * re, re), re)
        if odd:
            return [pltpu.make_async_copy(dzt_ref.at[at, pl.ds(k * cols, cols)], dz_v.at[pl.ds(k * re, re)], dzin_sem.at[1])
                    for k in range(BLOCKS)]
        return [pltpu.make_async_copy(dzt_ref.at[at, pl.ds(k * depth, depth)], (a_v, x_v)[k], dzin_sem.at[0])
                for k in range(2)]

    def de_copy(c, i):
        return pltpu.make_async_copy(
            z_v.at[pl.ds(pl.multiple_of(i * re, re), re)],
            de_ref.at[pl.ds(pl.multiple_of(c * re, re), re), pl.ds(pl.multiple_of(i * nc, nc), nc)], de_sem.at[i])

    def de_chunk(c, odd, extra=None):
        if odd:
            wait_bytes(dz_v, dzin_sem.at[1])
        else:
            wait_bytes(e_v.at[pl.ds(0, 2 * re)], dzin_sem.at[0])

        def part(i, _):
            sl = pl.ds(pl.multiple_of(i * nc, nc), nc)

            @pl.when(c == 0)
            def _():
                xin_copy(i).wait()

            @pl.when(c >= 1)
            def _():
                de_copy(c - 1, i).wait()
            if odd:
                val = jnp.dot(dz_v[:re, :], e_v[:cols, sl], preferred_element_type=F32)
                for k in range(1, BLOCKS):
                    val = val + jnp.dot(dz_v[k * re:k * re + re, :], e_v[k * cols:k * cols + cols, sl], preferred_element_type=F32)
            else:
                val = jnp.dot(a_v[...], e_v[:depth, sl], preferred_element_type=F32)
                val = val + jnp.dot(x_v[...], e_v[depth:, sl], preferred_element_type=F32)
            z_v[pl.ds(pl.multiple_of(i * re, re), re), :] = val
            de_copy(c, i).start()
            if extra is not None:
                @pl.when(jnp.logical_and(c == KEEP - 1, i == npart - 2))
                def _():
                    extra()
            return 0
        lax.fori_loop(0, npart, part, 0)

        @pl.when(c + 2 < KEEP)
        def _():
            for d in dzin_copies(c + 2, odd):
                d.start()

    def inside(b, fn, name='svc'):
        @pl.when(jnp.logical_and(b >= 0, b < BLOCKS))
        def _():
            with jax.named_scope(name):
                fn(b)

    def between(j, lo, hi, fn, name='svc'):
        @pl.when(jnp.logical_and(j >= lo, j <= hi))
        def _():
            with jax.named_scope(name):
                fn()

    def x_copy(b):
        return pltpu.make_async_copy(x_v, xall_ref.at[pl.ds(pl.multiple_of(b * cols, cols), cols)], x_sem)

    def dz_copy(b):
        return pltpu.make_async_copy(dz_v, dzt_ref.at[:, pl.ds(pl.multiple_of(b * cols, cols), cols)], dz_sem)

    def loop(k, fn):
        def body(i, _):
            fn(i)
            return 0
        lax.fori_loop(0, k, body, 0)

    with jax.named_scope('p_h'):
        ld_h.wait()
    in1(0, 0)
    in1(1, 0)
    with jax.named_scope('p_w'):
        ld_w.wait()
    ld_e[0].start()
    with jax.named_scope('p_proj'):
        project(own_v.at[0], own_v.at[1])
    with jax.named_scope('p_in2'):
        in2(0, 0)
    in1(1, 1)
    span(in1, 2, 3)
    with jax.named_scope('p_code'):
        wait_bytes(crcv_v.at[pl.ds(1, n - 1)], cd_send)
        wait_bytes(crcv_v.at[pl.ds(1, n - 1)], cd_recv)
    code = code_ref[...]
    for r in range(1, n):
        code = code + crcv_v[r]
    mask = (code >= 65536).astype(jnp.int32)
    local = code - mask * 65536 - me * rows
    tgt_v[0:BLOCKS, :] = jnp.where(jnp.logical_and(local >= 0, local < rows), local, -(1 << 24))
    maskf = mask.astype(F32)
    msk_v[...] = maskf
    per_col = jnp.sum(maskf, axis=0, keepdims=True)
    n0 = jnp.sum(per_col[:, :tok], axis=1, keepdims=True)
    n1 = jnp.sum(per_col[:, tok:], axis=1, keepdims=True)
    counts = jnp.concatenate([jnp.broadcast_to(n0, (1, tok)), jnp.broadcast_to(n1, (1, tok))], axis=1)
    wgt_v[...] = maskf / counts
    tot_v[0:1, :] = jnp.zeros((1, cols), F32)
    tot_v[1:2, :] = counts
    gsrc_v[...] = jnp.zeros_like(gsrc_v)
    with jax.named_scope('p_in3'):
        in3(0, 0)
    with jax.named_scope('p_fetch'):
        gather4(aall_ref.at[0, 0], h_send.at[0, 0], h_recv.at[0, 0])
        first = [a_copy(0, 0, kk, c) for kk in range(2) for c in range(CHIPS)]
        for c in first:
            c.start()
        wait_bytes(a_v.at[pl.ds(0, tok)], a_sem)
    with jax.named_scope('p_proj0'):
        project(a_v.at[pl.ds(0, tok)], a_v.at[pl.ds(tok, tok)])
    ld_e[1].start()
    ld_e[0].wait()

    def last_stage(b):
        rs4(b)
        dg1(b)

    def gather_b0():
        span(in2, 1, 2)
        span(in1, 3, 4)

    def gather_d0():
        ld_e[1].wait()
        span(in3, 1, 2)
        span(in2, 2, 3)
        span(in1, 4, 5)

    def gather_e0():
        span(in3, 2, 3)
        span(in2, 3, 4)
        span(in1, 5, 6)

    def gather_e1():
        span(in3, 3, 4)
        span(in2, 4, 6)
        span(in1, 6, 8)

    def gather_b2():
        span(in3, 4, 6)

    def gather_e2():
        span(in2, 6, 8)

    def gather_b3():
        span(in3, 6, 8)

    def step(t, _):
        j = t - 1
        def last_dg3():
            dg3(BLOCKS - 2)
            dg3(BLOCKS - 1)

        def block_wait():
            wait_bytes(a_v, a_sem)
        between(j, 0, BLOCKS - 2, block_wait, 'bwait')
        between(j, 1, BLOCKS, lambda: x_wait(j), 'xwait')

        def full_a():
            def body(i):
                dx_part(i, (j - 1) % 3)
                norm_part(i)
            loop(npart, body)
        between(j, -1, 0, lambda: loop(npart, norm_part), 'norm')
        between(j, 1, BLOCKS - 2, full_a, 'full_a')
        between(j, BLOCKS, BLOCKS, start_tail, 'start_tail')

        def last_a(i):
            dx_part(i, (j - 1) % 3)

            @pl.when(j == BLOCKS)
            def _():
                xin_copy(i).start()
        between(j, BLOCKS - 1, BLOCKS, lambda: loop(npart, last_a), 'last_a')
        between(j, BLOCKS + 1, BLOCKS + 3, lambda: de_chunk(2 * (j - BLOCKS) - 1, True, last_dg3), 'de_a')
        between(j, -1, BLOCKS - 2, lambda: x_copy(j + 1).start(), 'xstart')
        between(j, BLOCKS, BLOCKS, start_odd, 'start_odd')
        inside(j - 1, rs1, 'rs1')
        between(j, -1, -1, gather_b0, 'gb0')
        between(j, 1, 1, gather_b2, 'gb2')
        between(j, 2, 2, gather_b3, 'gb3')
        between(j, 1, BLOCKS - 3, lambda: fetch_block(j + 2), 'fetch')
        between(j, BLOCKS, BLOCKS, lambda: rs3(BLOCKS - 3), 'rs3')
        def late_stages():
            def body(b, _):
                last_stage(b)
                return 0
            lax.fori_loop(j - 4, 2 * j - BLOCKS - 4, body, 0)
        between(j, BLOCKS + 1, BLOCKS + 2, late_stages, 'rs4late')
        inside(j, join_stats, 'join')
        between(j, 1, BLOCKS - 1, lambda: dz_copy(j - 1).wait(), 'dzwait')
        between(j, BLOCKS, BLOCKS + 2, lambda: de_chunk(2 * (j - BLOCKS), False), 'de_d')

        def start_stats():
            ms_v[0] = jnp.full((8, cols), -3.0e38, F32)
            ms_v[1] = jnp.zeros((8, cols), F32)
            ms_v[2] = jnp.zeros((8, cols), F32)
            tgt_v[pl.ds(9, 1), :] = tgt_v[pl.ds(j + 1, 1), :]
        between(j, -1, BLOCKS - 2, start_stats)

        def first_d(i):
            d_body(i, False, True)

            @pl.when(i == 0)
            def _():
                gather_d0()
        between(j, -1, -1, lambda: loop(nr, first_d), 'only_z')
        def mid_d(i):
            d_body(i, True, True)

            @pl.when(i == 0)
            def _():
                between(j, 0, 0, lambda: fetch_block(2), 'fetch')
        between(j, 0, BLOCKS - 2, lambda: loop(nr, mid_d), 'full_d')
        between(j, BLOCKS - 1, BLOCKS - 1, lambda: loop(nr, lambda i: d_body(i, True, False)), 'back')
        between(j, -1, -1, lambda: fetch_block(1), 'fetch')
        between(j, -1, BLOCKS - 2, lambda: send_stats(j + 1), 'stats')
        inside(j, lambda b: dz_copy(b).start(), 'dzstart')
        between(j, 2, BLOCKS - 2, lambda: rs3(j - 2), 'rs3')
        between(j, BLOCKS, BLOCKS + 1, lambda: rs3(j - 2), 'rs3')
        between(j, 3, BLOCKS - 1, lambda: last_stage(j - 3), 'rs4g1')
        between(j, 4, BLOCKS + 2, lambda: dg2(j - 4), 'dg2')
        between(j, -1, -1, gather_e0, 'ge0')
        between(j, 0, 0, gather_e1, 'ge1')
        between(j, 1, 1, gather_e2, 'ge2')
        between(j, 5, BLOCKS + 2, lambda: dg3(j - 5), 'dg3')
        inside(j - 1, rs2, 'rs2')
        between(j, BLOCKS + 2, BLOCKS + 2, lambda: dg2(BLOCKS - 1), 'dg2last')
        between(j, BLOCKS + 2, BLOCKS + 2, gb_start, 'gbstart')
        return 0

    def gb_copy(r):
        return remote(gsrc_v, grcv_v.at[r], gb_send, gb_recv, (me + r) % n)

    def gb_start():
        for r in range(1, n):
            gb_copy(r).start()

    def start_tail():
        dz_copy(BLOCKS - 1).wait()
        for d in dzin_copies(0, False):
            d.start()

    def start_odd():
        for d in dzin_copies(1, True):
            d.start()

    def x_wait(j):
        @pl.when(j <= BLOCKS - 1)
        def _():
            x_copy(j).wait()

    def first_x(j):
        x_copy(j).wait()

    def step_outer(t, c):
        @pl.when(t == 1)
        def _():
            first_x(0)
        return step(t, c)

    lax.fori_loop(0, BLOCKS + 5, step_outer, 0)

    with jax.named_scope('e_g4'):
        for b in range(BLOCKS):
            gather4(dgall_ref.at[b], g_send.at[b], g_recv.at[b])
    with jax.named_scope('e_out'):
        for c in out_copies(BLOCKS - 1):
            c.wait()
    with jax.named_scope('e_de'):
        for i in range(npart):
            de_copy(KEEP - 1, i).wait()
    with jax.named_scope('e_gb'):
        wait_bytes(grcv_v.at[pl.ds(1, n - 1)], gb_send)
        wait_bytes(grcv_v.at[pl.ds(1, n - 1)], gb_recv)
    with jax.named_scope('e_sum'):
        acc = gsrc_v[...]
        for r in range(1, n):
            acc = acc + grcv_v[r]
        dgb_ref[...] = acc
        total_ref[...] = jnp.broadcast_to(jnp.sum(tot_v[0:1, :], axis=1, keepdims=True), total_ref.shape)


def stream(n, hidden, w_two, gain, bias, embed, code):
    tokens, depth = hidden.shape
    rows = embed.shape[0]
    q = tokens // BLOCKS
    half = CHIPS * q
    tok = 2 * half
    cols = 2 * tok
    nc = depth // 4
    rc, sub = rows // 2, rows // 8
    assert BLOCKS * cols == rows == 2 * depth and nc == cols
    dims = (n, q, depth, rows, rc, nc, sub)
    any_spec = pl.BlockSpec(memory_space=pl.ANY)
    vmem = pl.BlockSpec(memory_space=pltpu.VMEM)
    dma = pltpu.SemaphoreType.DMA
    sds = jax.ShapeDtypeStruct
    return pl.pallas_call(
        functools.partial(stream_kernel, dims),
        out_shape=(sds((BLOCKS, 2, 2, CHIPS, q, depth), BF16), sds((BLOCKS * cols, depth), BF16),
                   sds((rows, BLOCKS * cols), BF16), sds((BLOCKS, 2, CHIPS, q, depth), BF16),
                   sds((BLOCKS, q, depth), F32), sds((BLOCKS, q, depth), BF16),
                   sds((BLOCKS, cols), F32), sds((8, 128), F32), sds((8, depth), F32),
                   sds((KEEP * (rows // BLOCKS), depth), F32)),
        in_specs=[any_spec, any_spec, vmem, vmem, any_spec, vmem],
        out_specs=(any_spec,) * 6 + (vmem,) * 3 + (any_spec,),
        scratch_shapes=[
            pltpu.VMEM((rows, depth), BF16),
            pltpu.VMEM((cols, depth), BF16), pltpu.VMEM((cols, depth), BF16),
            pltpu.VMEM((rows, cols), F32), pltpu.VMEM((rows, cols), BF16),
            pltpu.VMEM((3, 2, 2, half, depth), F32), pltpu.VMEM((2, 2, half, depth), F32),
            pltpu.VMEM((4, 2, q, depth), F32), pltpu.VMEM((5, 2, 2, q, depth), F32),
            pltpu.VMEM((2, tokens, depth), BF16),
            pltpu.VMEM((4, q, depth), BF16), pltpu.VMEM((q, depth), F32),
            pltpu.VMEM((2, 8, cols), F32), pltpu.VMEM((2, n, 8, cols), F32),
            pltpu.VMEM((n, BLOCKS, cols), jnp.int32), pltpu.VMEM((16, cols), jnp.int32),
            pltpu.VMEM((BLOCKS, cols), F32), pltpu.VMEM((BLOCKS, cols), F32),
            pltpu.VMEM((3, 8, cols), F32), pltpu.VMEM((8, cols), F32), pltpu.VMEM((8, cols), F32),
            pltpu.VMEM((8, depth), F32), pltpu.VMEM((n, 8, depth), F32),
            dma((4,)), dma((4, 2, 3)), dma((BLOCKS, 2, 4)), dma((4, 2)), dma((BLOCKS, 3)), dma((BLOCKS, 4)),
            dma((BLOCKS,)), dma((2,)), dma((2,)), dma((2,)), dma((2,)), dma((3,)), dma((3,)),
            dma((4,)), dma((5,)), pltpu.SemaphoreType.REGULAR,
            dma, dma, dma, dma, dma, dma((2,)), dma, dma,
            dma((depth // nc,)), dma((2,)), dma((depth // nc,)),
        ],
        compiler_params=pltpu.CompilerParams(collective_id=0, has_side_effects=True, vmem_limit_bytes=67043328),
        name='stream',
    )(hidden, w_two, gain, bias, embed, code)


def dense_kernel(part_ref, dzt_ref, xall_ref, aall_ref, gall_ref, da_ref, go_ref, w_ref, loss_hbm, sum_hbm, dgb_hbm,
                 de_ref, dw_ref, dh_ref, tl_ref, total_ref, gs_ref, gb_ref,
                 da_v, go_v, w_v, g_v, x_v, h_v, dw_v, dz_v, de_v, st_v, w_sem, g_sem, x_sem, h_sem, dw_sem, dz_sem, de_sem, in_sem, out_sem, a_sem, loss_ref, sum_ref, dgb_ref, s_sem):
    depth = x_v.shape[1]
    nc, wb = depth // 4, depth // BLOCKS
    re = dzt_ref.shape[0] // BLOCKS
    xr = x_v.shape[0] // BLOCKS
    todo = BLOCKS - KEEP
    pieces = BLOCKS + 8 * todo
    pr = KEEP * re // pieces

    def at(i, size):
        return pl.ds(pl.multiple_of(i * size, size), size)

    def w_copy(i):
        return pltpu.make_async_copy(w_ref.at[at(i, nc)], w_v.at[at(i, nc)], w_sem.at[i])

    def h_copy(i):
        return pltpu.make_async_copy(aall_ref.at[:, 0:h_v.shape[2], at(i, wb)], h_v.at[i % 2], h_sem.at[i % 2])

    def dw_copy(i):
        return pltpu.make_async_copy(dw_v.at[i % 2], dw_ref.at[at(i, wb)], dw_sem.at[i % 2])

    def x_copy(i):
        return pltpu.make_async_copy(xall_ref.at[at(i, xr)], x_v.at[at(i, xr)], x_sem.at[i])

    def dz_copy(c):
        return pltpu.make_async_copy(dzt_ref.at[at(KEEP + c, re)], dz_v.at[c % 2], dz_sem.at[c % 2])

    def de_copy(u):
        return pltpu.make_async_copy(de_v.at[u % 2], de_ref.at[at(KEEP + u // 4, re), at(u % 4, nc)], de_sem.at[u % 2])

    def pin(t):
        return pltpu.make_async_copy(part_ref.at[at(t, pr)], st_v.at[t % 4], in_sem.at[t % 4])

    def pout(t):
        return pltpu.make_async_copy(st_v.at[t % 4], de_ref.at[at(t, pr)], out_sem.at[t % 4])

    def carry(t):
        pin(t).wait()
        pout(t).start()

        @pl.when(t >= 2)
        def _():
            pout(t - 2).wait()

        @pl.when(t + 2 < pieces)
        def _():
            pin(t + 2).start()

    g_load = pltpu.make_async_copy(gall_ref, g_v, g_sem)
    da_load = pltpu.make_async_copy(da_ref, da_v, a_sem.at[0])
    go_load = pltpu.make_async_copy(go_ref, go_v, a_sem.at[1])
    go_load.start()
    w_copy(0).start()
    small = [pltpu.make_async_copy(a, b, s_sem.at[i]) for i, (a, b) in
             enumerate(((loss_hbm, loss_ref), (sum_hbm, sum_ref), (dgb_hbm, dgb_ref)))]
    for c in small:
        c.start()
    da_load.start()
    for i in range(1, 4):
        w_copy(i).start()
    g_load.start()
    h_copy(0).start()
    h_copy(1).start()
    pin(0).start()
    pin(1).start()

    go_load.wait()
    da_load.wait()

    def hidden_part(i, _):
        w_copy(i).wait()
        sl = at(i, nc)
        back = lax.dot_general(go_v[...], w_v[sl, :], (((1,), (1,)), ((), ())), preferred_element_type=F32)
        dh_ref[:, sl] = (da_v[:, sl] + back).astype(BF16)
        return 0
    with jax.named_scope('k2_dh'):
        lax.fori_loop(0, 4, hidden_part, 0)
    for c in small:
        c.wait()
    gs_ref[...] = dgb_ref[0:2, :]
    gb_ref[...] = dgb_ref[2:4, :]
    total_ref[0] = sum_ref[0, 0]
    me = lax.axis_index('tp')
    lanes = loss_ref.shape[1]
    q = lanes // 2 // (2 * CHIPS)
    place = (me % 2) * CHIPS + me // 2
    for h in range(2):
        turned = pltpu.roll(loss_ref[...], (lanes - h * (lanes // 2) - place * q) % lanes, 1)
        tl_ref[h:h + 1, :] = jnp.concatenate([turned[b:b + 1, :q] for b in range(BLOCKS)], axis=1)
    with jax.named_scope('k2_g'):
        g_load.wait()

    def dw_part(i, _):
        h_copy(i).wait()
        carry(i)

        @pl.when(i < BLOCKS // 2)
        def _():
            x_copy(2 * i).start()
            x_copy(2 * i + 1).start()

        @pl.when(i == BLOCKS // 2)
        def _():
            dz_copy(0).start()

        @pl.when(i == BLOCKS // 2 + 2)
        def _():
            dz_copy(1).start()
        @pl.when(i >= 2)
        def _():
            dw_copy(i - 2).wait()
        h = h_v[i % 2].reshape(g_v.shape[0], wb)
        dw_v[i % 2] = lax.dot_general(h, g_v[...], (((0,), (0,)), ((), ())), preferred_element_type=F32)
        dw_copy(i).start()

        @pl.when(i + 2 < BLOCKS)
        def _():
            h_copy(i + 2).start()
        return 0
    with jax.named_scope('k2_dw'):
        lax.fori_loop(0, BLOCKS, dw_part, 0)
    with jax.named_scope('k2_x'):
        for i in range(BLOCKS):
            x_copy(i).wait()

    def de_part(u, _):
        c = u // 4

        @pl.when(u % 4 == 0)
        def _():
            dz_copy(c).wait()
        carry(BLOCKS + 2 * u)

        @pl.when(u >= 2)
        def _():
            de_copy(u - 2).wait()
        de_v[u % 2] = jnp.dot(dz_v[c % 2], x_v[:, at(u % 4, nc)], preferred_element_type=F32)
        de_copy(u).start()
        carry(BLOCKS + 2 * u + 1)

        @pl.when(jnp.logical_and(u % 4 == 3, c + 2 < todo))
        def _():
            dz_copy(c + 2).start()
        return 0
    with jax.named_scope('k2_de'):
        lax.fori_loop(0, 4 * todo, de_part, 0)
    for i in (BLOCKS - 2, BLOCKS - 1):
        dw_copy(i).wait()
    for i in (4 * todo - 2, 4 * todo - 1):
        de_copy(i).wait()
    for t in (pieces - 2, pieces - 1):
        pout(t).wait()


def dense(part, dzt, xall, aall, gall, da1, dgown, w_two, loss, total_loss, dgb):
    rows, kk = dzt.shape
    depth = xall.shape[1]
    total, tokens = gall.shape[0], da1.shape[0]
    re, wb, nc = rows // BLOCKS, depth // BLOCKS, depth // 4
    pieces = BLOCKS + 8 * (BLOCKS - KEEP)
    sds = jax.ShapeDtypeStruct
    dma = pltpu.SemaphoreType.DMA
    any_spec = pl.BlockSpec(memory_space=pl.ANY)
    vmem = pl.BlockSpec(memory_space=pltpu.VMEM)
    return pl.pallas_call(
        dense_kernel,
        out_shape=(sds((rows, depth), F32), sds((depth, depth), F32), sds((tokens, depth), BF16), sds((2, tokens), F32),
                   sds((1,), F32), sds((2, depth), F32), sds((2, depth), F32)),
        in_specs=[any_spec] * 11,
        out_specs=(any_spec, any_spec, vmem, vmem, pl.BlockSpec(memory_space=pltpu.SMEM), vmem, vmem),
        scratch_shapes=[pltpu.VMEM((tokens, depth), F32), pltpu.VMEM((tokens, depth), BF16), pltpu.VMEM((depth, depth), BF16), pltpu.VMEM((total, depth), BF16), pltpu.VMEM((kk, depth), BF16),
                        pltpu.VMEM((2, BLOCKS, total // BLOCKS, wb), BF16), pltpu.VMEM((2, wb, depth), F32),
                        pltpu.VMEM((2, re, kk), BF16), pltpu.VMEM((2, re, nc), F32),
                        pltpu.VMEM((4, KEEP * re // pieces, depth), F32),
                        dma((4,)), dma, dma((BLOCKS,)), dma((2,)), dma((2,)), dma((2,)), dma((2,)), dma((4,)), dma((4,)), dma((2,)), pltpu.VMEM(loss.shape, F32), pltpu.VMEM(total_loss.shape, F32),
                        pltpu.VMEM(dgb.shape, F32), dma((3,))],
        compiler_params=pltpu.CompilerParams(vmem_limit_bytes=67043328),
        name='dense',
    )(part, dzt, xall, aall, gall, da1, dgown, w_two, loss, total_loss, dgb)


def solution(mesh):
    n = mesh.shape['tp']
    tok_spec = P(('dp', 'tp'), None)
    row_spec = P(None, ('dp', 'tp'))

    def device_step(hidden, w_two, ln_scale, ln_shift, embed, targets, loss_mask):
        tokens, depth = hidden.shape
        q = tokens // BLOCKS
        me = lax.axis_index('tp')
        code = (targets + 65536 * loss_mask).reshape(2, BLOCKS, q).transpose(1, 0, 2)
        place = (me % 2) * CHIPS + me // 2
        seat = lax.broadcasted_iota(jnp.int32, (1, 1, 2 * CHIPS, 1), 2) == place
        code = jnp.where(seat, code[:, :, None, :], 0).reshape(BLOCKS, 2 * 2 * CHIPS * q)
        aall, xall, dzt, dgall, da1, dgown, loss, total, dgb, part = stream(
            n, hidden, w_two, ln_scale, ln_shift, embed, code)
        d_embed, d_w, d_hidden, token_loss, total_loss, d_scale, d_shift = dense(
            part, dzt, xall, aall.reshape(BLOCKS, 2 * n * q, depth), dgall.reshape(n * tokens, depth),
            da1.reshape(tokens, depth), dgown.reshape(tokens, depth), w_two, loss, total, dgb)
        return token_loss, total_loss, d_hidden, d_embed, d_w, d_scale, d_shift

    return jax.shard_map(device_step, mesh=mesh,
                         in_specs=(tok_spec, P(), P(), P(), P('tp', None), row_spec, row_spec),
                         out_specs=(row_spec, P('dp'), tok_spec, tok_spec, P('dp', None), P('dp', None), P('dp', None)),
                         check_vma=False)
```

```python
import functools

import jax
import jax.numpy as jnp
from jax import lax
from jax.experimental import pallas as pl
from jax.experimental.pallas import tpu as pltpu
from jax.sharding import PartitionSpec as P

LN_EPS = 1e-5
CHIPS = 4
BLOCKS = 8
KEEP = 6
WAYS = 4
LANES = 2
F32 = jnp.float32
BF16 = jnp.bfloat16


def to(idx):
    return dict(device_id={'tp': idx}, device_id_type=pl.DeviceIdType.MESH)


def remote(src, dst, send, recv, idx):
    return pltpu.make_async_remote_copy(src_ref=src, dst_ref=dst, send_sem=send, recv_sem=recv, **to(idx))


def stream_kernel(dims, h_ref, w_ref, gain_ref, bias_ref, e_ref, code_ref,
                  aall_ref, xall_ref, dzt_ref, dgall_ref, da1_ref, dgown_ref, loss_ref, total_ref, dgb_ref, de_ref,
                  e_v, a_v, x_v, z_v, dz_v, dx_v, pr_v, mg_v, ow_v, own_v, dg_v, da_v,
                  stsrc_v, strcv_v, crcv_v, tgt_v, msk_v, wgt_v, ms_v, row_v, tot_v, gsrc_v, grcv_v,
                  ld_sem, h_send, h_recv, h_loc, g_send, g_recv, g_loc,
                  st_send, st_recv, pr_send, pr_recv, r2_send, r3_send, mg_recv, ow_recv, pair_free,
                  cd_send, cd_recv, x_sem, dz_sem, a_sem, out_sem, gb_send, gb_recv, xin_sem, dzin_sem, de_sem):
    n, q, depth, rows, rc, nc, sub = dims
    re = rows // BLOCKS
    half = CHIPS * q
    tok = 2 * half
    cols = 2 * tok
    me = lax.axis_index('tp')
    chip = me // 2
    core = me % 2
    peer = me + 1 - 2 * core
    right_chip = (chip + 1) % CHIPS
    left_chip = (chip + CHIPS - 1) % CHIPS
    far_chip = (chip + 2) % CHIPS
    right = right_chip * 2 + core
    left = left_chip * 2 + core

    top, bottom = pl.ds(0, depth), pl.ds(depth, rows - depth)
    ld_e = [pltpu.make_async_copy(e_ref.at[d], e_v.at[d], ld_sem.at[i]) for i, d in ((0, top), (3, bottom))]
    ld_w = pltpu.make_async_copy(w_ref, e_v.at[bottom], ld_sem.at[1])
    ld_h = pltpu.make_async_copy(h_ref, own_v.at[0], ld_sem.at[2])
    ld_h.start()
    ld_w.start()

    barrier = pltpu.get_barrier_semaphore()
    for r in range(1, n):
        pl.semaphore_signal(barrier, inc=1, **to((me + r) % n))
    pl.semaphore_wait(barrier, n - 1)

    def wait_bytes(ref, sem):
        pltpu.make_async_copy(ref, ref, sem).wait()

    def code_copy(r):
        return remote(code_ref, crcv_v.at[r], cd_send, cd_recv, (me + r) % n)

    for r in range(1, n):
        code_copy(r).start()

    lo, hi = pl.ds(0, q // 2), pl.ds(q // 2, q // 2)

    def g1_copies(src, dst, send, recv):
        piece = dst.at[core, chip]
        return (remote(src, piece, send.at[0], recv.at[0], right),
                remote(src, piece, send.at[0], recv.at[1], left),
                remote(src, piece, send.at[0], recv.at[3], peer))

    def g2_copies(dst, send, recv):
        fl, fr = dst.at[core, left_chip], dst.at[core, right_chip]
        return (remote(fl.at[lo], fl.at[lo], send.at[1], recv.at[2], right),
                remote(fr.at[hi], fr.at[hi], send.at[1], recv.at[2], left),
                remote(fl, fl, send.at[1], recv.at[3], peer),
                remote(fr, fr, send.at[1], recv.at[3], peer))

    def gather1(src, dst, send, recv, loc):
        for c in g1_copies(src, dst, send, recv):
            c.start()
        pltpu.make_async_copy(src, dst.at[core, chip], loc).start()

    def gather2(src, dst, send, recv, loc):
        wait_bytes(dst.at[core, left_chip], recv.at[0])
        wait_bytes(dst.at[core, right_chip], recv.at[1])
        for c in g2_copies(dst, send, recv):
            c.start()
        wait_bytes(dst.at[core, pl.ds(0, 3)], send.at[0])
        pltpu.make_async_copy(src, dst.at[core, chip], loc).wait()

    def gather3(dst, send, recv):
        far = dst.at[core, far_chip]
        wait_bytes(far, recv.at[2])
        remote(far, far, send.at[2], recv.at[3], peer).start()
        wait_bytes(dst.at[core, pl.ds(0, 3)], send.at[1])

    def gather4(dst, send, recv):
        wait_bytes(dst.at[1 - core], recv.at[3])
        wait_bytes(dst.at[core, far_chip], send.at[2])

    def own(b, h):
        return own_v.at[h, pl.ds(pl.multiple_of(b * q, q), q)]

    def in1(b, h):
        gather1(own(b, h), aall_ref.at[b, h], h_send.at[b % 4, h], h_recv.at[b, h], h_loc.at[b % 4, h])

    def in2(b, h):
        gather2(own(b, h), aall_ref.at[b, h], h_send.at[b % 4, h], h_recv.at[b, h], h_loc.at[b % 4, h])

    def in3(b, h):
        gather3(aall_ref.at[b, h], h_send.at[b % 4, h], h_recv.at[b, h])

    def dg1(b):
        gather1(dg_v.at[b % 4], dgall_ref.at[b], g_send.at[b], g_recv.at[b], g_loc.at[b])

    def dg2(b):
        gather2(dg_v.at[b % 4], dgall_ref.at[b], g_send.at[b], g_recv.at[b], g_loc.at[b])

    def dg3(b):
        gather3(dgall_ref.at[b], g_send.at[b], g_recv.at[b])

    def span(fn, lo, hi):
        def body(u, _):
            fn(u // 2, u % 2)
            return 0
        lax.fori_loop(2 * lo, 2 * hi, body, 0)

    def a_copy(b, h, kk, c):
        at = pl.ds(((h * 2 + kk) * CHIPS + c) * q, q)
        return pltpu.make_async_copy(aall_ref.at[b, h, kk, c], a_v.at[at], a_sem)

    def block_copies(b):
        return [a_copy(b, h, kk, c) for h in range(2) for kk in range(2) for c in range(CHIPS)]

    def fetch_block(b):
        for h in range(2):
            gather4(aall_ref.at[b, h], h_send.at[b % 4, h], h_recv.at[b, h])
        for c in block_copies(b):
            c.start()

    def project(src, dst):
        def proj(i, _):
            sl = pl.ds(pl.multiple_of(i * nc, nc), nc)
            dst[:, sl] = jnp.dot(src[...], e_v[bottom, sl], preferred_element_type=F32).astype(BF16)
            return 0
        lax.fori_loop(0, depth // nc, proj, 0)

    def norm_rows(start, head):
        a = a_v[pl.ds(start, 16), :].astype(F32)
        mean = jnp.mean(a, axis=-1, keepdims=True)
        cent = a - mean
        var = jnp.mean(cent * cent, axis=-1, keepdims=True)
        y = cent * lax.rsqrt(var + LN_EPS) * gain_ref[pl.ds(head, 1), :] + bias_ref[pl.ds(head, 1), :]
        x_v[pl.ds(start, 16), :] = y.astype(BF16)

    npart = depth // nc
    lrows = cols // npart

    def norm_part(i):
        head = (i * lrows) // tok
        for s in range(lrows // 16):
            norm_rows(pl.multiple_of(i * lrows + s * 16, 16), head)

    def dx_part(i, slot):
        sl = pl.ds(pl.multiple_of(i * nc, nc), nc)
        val = lax.dot_general(dz_v[...], e_v[:, sl], (((0,), (0,)), ((), ())), preferred_element_type=F32)
        for h in range(2):
            for kk in range(2):
                base = h * tok + kk * half
                dx_v[slot, kk, h, :, sl] = val[base:base + half, :]

    nr = rows // rc

    def tree(parts, op):
        while len(parts) > 1:
            parts = [op(a, b) for a, b in zip(parts[::2], parts[1::2])]
        return parts[0]

    def part_view(ref, i):
        return ref.at[pl.ds(pl.multiple_of(i * rc, rc), rc)]

    def back_part(i, p, lanes, td):
        shift, w = row_v[0:1, lanes], row_v[1:2, lanes]
        zc, dc = part_view(z_v, i), part_view(dz_v, i)
        for s in range(p * sub, p * sub + sub, 16):
            both = []
            for t in (s, s + 8):
                pw = jnp.exp(zc[t:t + 8, lanes] - shift)
                both.append(jnp.where(td == t, pw - w, pw))
            dc[s:s + 16, lanes] = jnp.concatenate(both, axis=0).astype(BF16)

    def z_part(i, p):
        ec = part_view(e_v, i)
        part_view(z_v, i)[p * sub:p * sub + sub, :] = lax.dot_general(
            ec[p * sub:p * sub + sub, :], x_v[...], (((1,), (1,)), ((), ())), preferred_element_type=F32)

    def stat_part(i, p, lanes, td, state):
        zc = part_view(z_v, i)
        m_old, acc, tl = state
        at = range(p * sub, p * sub + sub, 8)
        tops = [zc[s:s + 8, lanes] for s in at[:WAYS]]
        for k, s in enumerate(at[WAYS:]):
            tops[k % WAYS] = jnp.maximum(tops[k % WAYS], zc[s:s + 8, lanes])
        m = jnp.maximum(m_old, tree(tops, jnp.maximum))
        accs = [None] * WAYS
        for k, s in enumerate(at):
            z = zc[s:s + 8, lanes]
            e = jnp.exp(z - m)
            accs[k % WAYS] = e if accs[k % WAYS] is None else accs[k % WAYS] + e
            tl = jnp.where(td == s, z, tl)
        return m, acc * jnp.exp(m_old - m) + tree(accs, jnp.add), tl

    def d_body(i, back, new):
        span = cols // LANES
        iota = lax.broadcasted_iota(jnp.int32, (8, span), 0)
        cut = [slice(k * span, k * span + span) for k in range(LANES)]
        td_old = [tgt_v[pl.ds(8, 1), c] - i * rc - iota for c in cut]
        td_new = [tgt_v[pl.ds(9, 1), c] - i * rc - iota for c in cut]
        state = [tuple(ms_v[k, :, c] for k in range(3)) for c in cut]
        for p in range(rc // sub):
            if back:
                for k in range(LANES):
                    back_part(i, p, cut[k], td_old[k])
            if new:
                z_part(i, p)
                for k in range(LANES):
                    state[k] = stat_part(i, p, cut[k], td_new[k], state[k])
        if new:
            for k in range(LANES):
                for q_ in range(3):
                    ms_v[q_, :, cut[k]] = state[k][q_]

    def stat_copy(slot, r):
        return remote(stsrc_v.at[slot], strcv_v.at[slot, r], st_send.at[slot], st_recv.at[slot], (me + r) % n)

    def send_stats(b):
        slot = b % 2
        m = ms_v[0]
        top = jnp.max(m, axis=0, keepdims=True)
        stsrc_v[slot, 0:1, :] = top
        stsrc_v[slot, 1:2, :] = jnp.sum(ms_v[1] * jnp.exp(m - top), axis=0, keepdims=True)
        stsrc_v[slot, 2:3, :] = jnp.sum(ms_v[2], axis=0, keepdims=True)
        for r in range(1, n):
            stat_copy(slot, r).start()

    def join_stats(b):
        slot = b % 2
        wait_bytes(strcv_v.at[slot, pl.ds(1, n - 1)], st_send.at[slot])
        wait_bytes(strcv_v.at[slot, pl.ds(1, n - 1)], st_recv.at[slot])
        parts = [stsrc_v[slot]] + [strcv_v[slot, r] for r in range(1, n)]
        top = parts[0][0:1]
        for p in parts[1:]:
            top = jnp.maximum(top, p[0:1])
        total = jnp.zeros_like(top)
        hit = jnp.zeros_like(top)
        for p in parts:
            total = total + p[1:2] * jnp.exp(p[0:1] - top)
            hit = hit + p[2:3]
        lse = top + jnp.log(total)
        w = wgt_v[pl.ds(b, 1), :]
        row_v[0:1, :] = jnp.where(w > 0.0, lse - jnp.log(jnp.where(w > 0.0, w, 1.0)), 3.0e38)
        row_v[1:2, :] = w
        tgt_v[pl.ds(8, 1), :] = tgt_v[pl.ds(b, 1), :]
        loss = (lse - hit) * msk_v[pl.ds(b, 1), :]
        loss_ref[pl.ds(b, 1), :] = loss
        tot_v[0:1, :] = tot_v[0:1, :] + loss / tot_v[1:2, :]

    def pair_copy(b):
        slot = b % 2
        return remote(dx_v.at[b % 3, 1 - core], pr_v.at[slot], pr_send.at[slot], pr_recv.at[slot], peer)

    def rs1(b):
        @pl.when(b >= 2)
        def _():
            pl.semaphore_wait(pair_free, 1)
        pair_copy(b).start()

    def crow(c):
        return pl.ds(pl.multiple_of(c * q, q), q)

    def r2_copies(b):
        mine, s3, mg, ow = dx_v.at[b % 3, core], b % 3, b % 4, b % 5
        return (remote(mine.at[0, crow(far_chip)], mg_v.at[mg, 0], r2_send.at[s3], mg_recv.at[mg], right),
                remote(mine.at[1, crow(far_chip)], mg_v.at[mg, 1], r2_send.at[s3], mg_recv.at[mg], left),
                remote(mine.at[1, crow(right_chip)], ow_v.at[ow, 0, 1], r2_send.at[s3], ow_recv.at[ow], right),
                remote(mine.at[0, crow(left_chip)], ow_v.at[ow, 1, 0], r2_send.at[s3], ow_recv.at[ow], left))

    def rs2(b):
        slot, s3 = b % 2, b % 3
        pair_copy(b).wait()

        def add(i, _):
            h = i // CHIPS
            c = i % CHIPS
            dx_v[s3, core, h, crow(c), :] += pr_v[slot, h, crow(c), :]
            return 0
        lax.fori_loop(0, 2 * CHIPS, add, 0)

        @pl.when(b < BLOCKS - 2)
        def _():
            pl.semaphore_signal(pair_free, inc=1, **to(peer))
        for c in r2_copies(b):
            c.start()

    def r3_copies(b):
        mine, s3, ow = dx_v.at[b % 3, core], b % 3, b % 5
        return (remote(mine.at[0, crow(right_chip)], ow_v.at[ow, 0, 0], r3_send.at[s3], ow_recv.at[ow], right),
                remote(mine.at[1, crow(left_chip)], ow_v.at[ow, 1, 1], r3_send.at[s3], ow_recv.at[ow], left))

    def rs3(b):
        s3, mg = b % 3, b % 4
        wait_bytes(mg_v.at[mg], mg_recv.at[mg])
        dx_v[s3, core, 0, crow(right_chip), :] += mg_v[mg, 0]
        dx_v[s3, core, 1, crow(left_chip), :] += mg_v[mg, 1]
        for c in r3_copies(b):
            c.start()

    def rs4(b):
        ow = b % 5
        wait_bytes(ow_v.at[ow], ow_recv.at[ow])

        @pl.when(b >= 1)
        def _():
            out_copies(b - 1)[0].wait()
            out_copies(b - 1)[1].wait()
        for h in range(2):
            dy = dx_v[b % 3, core, h, crow(chip), :] + ow_v[ow, 0, h] + ow_v[ow, 1, h]
            a = own(b, h)[...].astype(F32)
            mean = jnp.mean(a, axis=-1, keepdims=True)
            cent = a - mean
            rstd = lax.rsqrt(jnp.mean(cent * cent, axis=-1, keepdims=True) + LN_EPS)
            xhat = cent * rstd
            gsrc_v[h:h + 1, :] += jnp.sum(dy * xhat, axis=0, keepdims=True)
            gsrc_v[2 + h:3 + h, :] += jnp.sum(dy, axis=0, keepdims=True)
            dxh = dy * gain_ref[h:h + 1, :]
            c1 = jnp.mean(dxh, axis=-1, keepdims=True)
            c2_ = jnp.mean(dxh * xhat, axis=-1, keepdims=True)
            da = rstd * (dxh - c1 - xhat * c2_)
            if h == 0:
                da_v[...] = da
            else:
                dg_v[b % 4] = da.astype(BF16)
        for c in out_copies(b):
            c.start()
        wait_bytes(ow_v.at[ow], r2_send.at[b % 3])
        wait_bytes(mg_v.at[b % 4], r3_send.at[b % 3])

    def out_copies(b):
        return (pltpu.make_async_copy(da_v, da1_ref.at[b], out_sem.at[0]),
                pltpu.make_async_copy(dg_v.at[b % 4], dgown_ref.at[b], out_sem.at[1]))

    def xin_copy(i):
        sl = pl.ds(pl.multiple_of(i * nc, nc), nc)
        return pltpu.make_async_copy(xall_ref.at[:, sl], e_v.at[:, sl], xin_sem.at[i])

    def dzin_copies(c, odd):
        at = pl.ds(pl.multiple_of(c * re, re), re)
        if odd:
            return [pltpu.make_async_copy(dzt_ref.at[at, pl.ds(k * cols, cols)], dz_v.at[pl.ds(k * re, re)], dzin_sem.at[1])
                    for k in range(BLOCKS)]
        return [pltpu.make_async_copy(dzt_ref.at[at, pl.ds(k * depth, depth)], (a_v, x_v)[k], dzin_sem.at[0])
                for k in range(2)]

    def de_copy(c, i):
        return pltpu.make_async_copy(
            z_v.at[pl.ds(pl.multiple_of(i * re, re), re)],
            de_ref.at[pl.ds(pl.multiple_of(c * re, re), re), pl.ds(pl.multiple_of(i * nc, nc), nc)], de_sem.at[i])

    def de_chunk(c, odd, extra=None):
        if odd:
            wait_bytes(dz_v, dzin_sem.at[1])
        else:
            wait_bytes(e_v.at[pl.ds(0, 2 * re)], dzin_sem.at[0])

        def part(i, _):
            sl = pl.ds(pl.multiple_of(i * nc, nc), nc)

            @pl.when(c == 0)
            def _():
                xin_copy(i).wait()

            @pl.when(c >= 1)
            def _():
                de_copy(c - 1, i).wait()
            if odd:
                val = jnp.dot(dz_v[:re, :], e_v[:cols, sl], preferred_element_type=F32)
                for k in range(1, BLOCKS):
                    val = val + jnp.dot(dz_v[k * re:k * re + re, :], e_v[k * cols:k * cols + cols, sl], preferred_element_type=F32)
            else:
                val = jnp.dot(a_v[...], e_v[:depth, sl], preferred_element_type=F32)
                val = val + jnp.dot(x_v[...], e_v[depth:, sl], preferred_element_type=F32)
            z_v[pl.ds(pl.multiple_of(i * re, re), re), :] = val
            de_copy(c, i).start()
            if extra is not None:
                @pl.when(jnp.logical_and(c == KEEP - 1, i == npart - 2))
                def _():
                    extra()
            return 0
        lax.fori_loop(0, npart, part, 0)

        @pl.when(c + 2 < KEEP)
        def _():
            for d in dzin_copies(c + 2, odd):
                d.start()

    def inside(b, fn, name='svc'):
        @pl.when(jnp.logical_and(b >= 0, b < BLOCKS))
        def _():
            with jax.named_scope(name):
                fn(b)

    def between(j, lo, hi, fn, name='svc'):
        @pl.when(jnp.logical_and(j >= lo, j <= hi))
        def _():
            with jax.named_scope(name):
                fn()

    def x_copy(b):
        return pltpu.make_async_copy(x_v, xall_ref.at[pl.ds(pl.multiple_of(b * cols, cols), cols)], x_sem)

    def dz_copy(b):
        return pltpu.make_async_copy(dz_v, dzt_ref.at[:, pl.ds(pl.multiple_of(b * cols, cols), cols)], dz_sem)

    def loop(k, fn):
        def body(i, _):
            fn(i)
            return 0
        lax.fori_loop(0, k, body, 0)

    with jax.named_scope('p_h'):
        ld_h.wait()
    in1(0, 0)
    in1(1, 0)
    with jax.named_scope('p_w'):
        ld_w.wait()
    ld_e[0].start()
    with jax.named_scope('p_proj'):
        project(own_v.at[0], own_v.at[1])
    with jax.named_scope('p_in2'):
        in2(0, 0)
    in1(1, 1)
    span(in1, 2, 3)
    with jax.named_scope('p_code'):
        wait_bytes(crcv_v.at[pl.ds(1, n - 1)], cd_send)
        wait_bytes(crcv_v.at[pl.ds(1, n - 1)], cd_recv)
    code = code_ref[...]
    for r in range(1, n):
        code = code + crcv_v[r]
    mask = (code >= 65536).astype(jnp.int32)
    local = code - mask * 65536 - me * rows
    tgt_v[0:BLOCKS, :] = jnp.where(jnp.logical_and(local >= 0, local < rows), local, -(1 << 24))
    maskf = mask.astype(F32)
    msk_v[...] = maskf
    per_col = jnp.sum(maskf, axis=0, keepdims=True)
    n0 = jnp.sum(per_col[:, :tok], axis=1, keepdims=True)
    n1 = jnp.sum(per_col[:, tok:], axis=1, keepdims=True)
    counts = jnp.concatenate([jnp.broadcast_to(n0, (1, tok)), jnp.broadcast_to(n1, (1, tok))], axis=1)
    wgt_v[...] = maskf / counts
    tot_v[0:1, :] = jnp.zeros((1, cols), F32)
    tot_v[1:2, :] = counts
    gsrc_v[...] = jnp.zeros_like(gsrc_v)
    with jax.named_scope('p_in3'):
        in3(0, 0)
    with jax.named_scope('p_fetch'):
        gather4(aall_ref.at[0, 0], h_send.at[0, 0], h_recv.at[0, 0])
        first = [a_copy(0, 0, kk, c) for kk in range(2) for c in range(CHIPS)]
        for c in first:
            c.start()
        wait_bytes(a_v.at[pl.ds(0, tok)], a_sem)
    with jax.named_scope('p_proj0'):
        project(a_v.at[pl.ds(0, tok)], a_v.at[pl.ds(tok, tok)])
    ld_e[1].start()
    ld_e[0].wait()

    def last_stage(b):
        rs4(b)
        dg1(b)

    def gather_b0():
        span(in2, 1, 2)
        span(in1, 3, 4)

    def gather_d0():
        ld_e[1].wait()
        span(in3, 1, 2)
        span(in2, 2, 3)
        span(in1, 4, 5)

    def gather_e0():
        span(in3, 2, 3)
        span(in2, 3, 4)
        span(in1, 5, 6)

    def gather_b1():
        span(in1, 6, 8)

    def gather_e1():
        span(in3, 3, 4)
        span(in2, 4, 6)

    def gather_b2():
        span(in3, 4, 6)
        span(in2, 6, 8)

    def gather_e2():
        span(in3, 6, 8)

    def step(t, _):
        j = t - 1
        def last_dg3():
            dg3(BLOCKS - 2)
            dg3(BLOCKS - 1)

        def block_wait():
            wait_bytes(a_v, a_sem)
        between(j, 0, BLOCKS - 2, block_wait, 'bwait')
        between(j, 1, BLOCKS, lambda: x_wait(j), 'xwait')

        def full_a():
            def body(i):
                dx_part(i, (j - 1) % 3)
                norm_part(i)
            loop(npart, body)
        between(j, -1, 0, lambda: loop(npart, norm_part), 'norm')
        between(j, 1, BLOCKS - 2, full_a, 'full_a')
        between(j, BLOCKS, BLOCKS, start_tail, 'start_tail')

        def last_a(i):
            dx_part(i, (j - 1) % 3)

            @pl.when(j == BLOCKS)
            def _():
                xin_copy(i).start()
        between(j, BLOCKS - 1, BLOCKS, lambda: loop(npart, last_a), 'last_a')
        between(j, BLOCKS + 1, BLOCKS + 3, lambda: de_chunk(2 * (j - BLOCKS) - 1, True, last_dg3), 'de_a')
        between(j, -1, BLOCKS - 2, lambda: x_copy(j + 1).start(), 'xstart')
        between(j, BLOCKS, BLOCKS, start_odd, 'start_odd')
        inside(j - 1, rs1, 'rs1')
        between(j, -1, -1, gather_b0, 'gb0')
        between(j, 1, 1, gather_b2, 'gb2')
        between(j, 0, 0, gather_b1, 'gb1')
        between(j, 1, BLOCKS - 3, lambda: fetch_block(j + 2), 'fetch')
        between(j, BLOCKS, BLOCKS, lambda: rs3(BLOCKS - 3), 'rs3')
        def late_stages():
            def body(b, _):
                last_stage(b)
                return 0
            lax.fori_loop(j - 4, 2 * j - BLOCKS - 4, body, 0)
        between(j, BLOCKS + 1, BLOCKS + 2, late_stages, 'rs4late')
        inside(j, join_stats, 'join')
        between(j, 1, BLOCKS - 1, lambda: dz_copy(j - 1).wait(), 'dzwait')
        between(j, BLOCKS, BLOCKS + 2, lambda: de_chunk(2 * (j - BLOCKS), False), 'de_d')

        def start_stats():
            ms_v[0] = jnp.full((8, cols), -3.0e38, F32)
            ms_v[1] = jnp.zeros((8, cols), F32)
            ms_v[2] = jnp.zeros((8, cols), F32)
            tgt_v[pl.ds(9, 1), :] = tgt_v[pl.ds(j + 1, 1), :]
        between(j, -1, BLOCKS - 2, start_stats)

        def first_d(i):
            d_body(i, False, True)

            @pl.when(i == 0)
            def _():
                gather_d0()
        between(j, -1, -1, lambda: loop(nr, first_d), 'only_z')
        def mid_d(i):
            d_body(i, True, True)

            @pl.when(i == 0)
            def _():
                between(j, 0, 0, lambda: fetch_block(2), 'fetch')
                between(j, 1, 1, lambda: rs2(0), 'rs2')
        between(j, 0, BLOCKS - 2, lambda: loop(nr, mid_d), 'full_d')
        between(j, BLOCKS - 1, BLOCKS - 1, lambda: loop(nr, lambda i: d_body(i, True, False)), 'back')
        between(j, -1, -1, lambda: fetch_block(1), 'fetch')
        between(j, -1, BLOCKS - 2, lambda: send_stats(j + 1), 'stats')
        inside(j, lambda b: dz_copy(b).start(), 'dzstart')
        between(j, 2, BLOCKS - 2, lambda: rs3(j - 2), 'rs3')
        between(j, BLOCKS, BLOCKS + 1, lambda: rs3(j - 2), 'rs3')
        between(j, 3, BLOCKS - 1, lambda: last_stage(j - 3), 'rs4g1')
        between(j, 4, BLOCKS + 2, lambda: dg2(j - 4), 'dg2')
        between(j, -1, -1, gather_e0, 'ge0')
        between(j, 0, 0, gather_e1, 'ge1')
        between(j, 1, 1, gather_e2, 'ge2')
        between(j, 5, BLOCKS + 2, lambda: dg3(j - 5), 'dg3')
        between(j, 2, BLOCKS, lambda: rs2(j - 1), 'rs2')
        between(j, BLOCKS + 2, BLOCKS + 2, lambda: dg2(BLOCKS - 1), 'dg2last')
        between(j, BLOCKS + 2, BLOCKS + 2, gb_start, 'gbstart')
        return 0

    def gb_copy(r):
        return remote(gsrc_v, grcv_v.at[r], gb_send, gb_recv, (me + r) % n)

    def gb_start():
        for r in range(1, n):
            gb_copy(r).start()

    def start_tail():
        dz_copy(BLOCKS - 1).wait()
        for d in dzin_copies(0, False):
            d.start()

    def start_odd():
        for d in dzin_copies(1, True):
            d.start()

    def x_wait(j):
        @pl.when(j <= BLOCKS - 1)
        def _():
            x_copy(j).wait()

    def first_x(j):
        x_copy(j).wait()

    def step_outer(t, c):
        @pl.when(t == 1)
        def _():
            first_x(0)
        return step(t, c)

    lax.fori_loop(0, BLOCKS + 5, step_outer, 0)

    with jax.named_scope('e_g4'):
        for b in range(BLOCKS):
            gather4(dgall_ref.at[b], g_send.at[b], g_recv.at[b])
    with jax.named_scope('e_out'):
        for c in out_copies(BLOCKS - 1):
            c.wait()
    with jax.named_scope('e_de'):
        for i in range(npart):
            de_copy(KEEP - 1, i).wait()
    with jax.named_scope('e_gb'):
        wait_bytes(grcv_v.at[pl.ds(1, n - 1)], gb_send)
        wait_bytes(grcv_v.at[pl.ds(1, n - 1)], gb_recv)
    with jax.named_scope('e_sum'):
        acc = gsrc_v[...]
        for r in range(1, n):
            acc = acc + grcv_v[r]
        dgb_ref[...] = acc
        total_ref[...] = jnp.broadcast_to(jnp.sum(tot_v[0:1, :], axis=1, keepdims=True), total_ref.shape)


def stream(n, hidden, w_two, gain, bias, embed, code):
    tokens, depth = hidden.shape
    rows = embed.shape[0]
    q = tokens // BLOCKS
    half = CHIPS * q
    tok = 2 * half
    cols = 2 * tok
    nc = depth // 4
    rc, sub = rows // 2, rows // 8
    assert BLOCKS * cols == rows == 2 * depth and nc == cols
    dims = (n, q, depth, rows, rc, nc, sub)
    any_spec = pl.BlockSpec(memory_space=pl.ANY)
    vmem = pl.BlockSpec(memory_space=pltpu.VMEM)
    dma = pltpu.SemaphoreType.DMA
    sds = jax.ShapeDtypeStruct
    return pl.pallas_call(
        functools.partial(stream_kernel, dims),
        out_shape=(sds((BLOCKS, 2, 2, CHIPS, q, depth), BF16), sds((BLOCKS * cols, depth), BF16),
                   sds((rows, BLOCKS * cols), BF16), sds((BLOCKS, 2, CHIPS, q, depth), BF16),
                   sds((BLOCKS, q, depth), F32), sds((BLOCKS, q, depth), BF16),
                   sds((BLOCKS, cols), F32), sds((8, 128), F32), sds((8, depth), F32),
                   sds((KEEP * (rows // BLOCKS), depth), F32)),
        in_specs=[any_spec, any_spec, vmem, vmem, any_spec, vmem],
        out_specs=(any_spec,) * 6 + (vmem,) * 3 + (any_spec,),
        scratch_shapes=[
            pltpu.VMEM((rows, depth), BF16),
            pltpu.VMEM((cols, depth), BF16), pltpu.VMEM((cols, depth), BF16),
            pltpu.VMEM((rows, cols), F32), pltpu.VMEM((rows, cols), BF16),
            pltpu.VMEM((3, 2, 2, half, depth), F32), pltpu.VMEM((2, 2, half, depth), F32),
            pltpu.VMEM((4, 2, q, depth), F32), pltpu.VMEM((5, 2, 2, q, depth), F32),
            pltpu.VMEM((2, tokens, depth), BF16),
            pltpu.VMEM((4, q, depth), BF16), pltpu.VMEM((q, depth), F32),
            pltpu.VMEM((2, 8, cols), F32), pltpu.VMEM((2, n, 8, cols), F32),
            pltpu.VMEM((n, BLOCKS, cols), jnp.int32), pltpu.VMEM((16, cols), jnp.int32),
            pltpu.VMEM((BLOCKS, cols), F32), pltpu.VMEM((BLOCKS, cols), F32),
            pltpu.VMEM((3, 8, cols), F32), pltpu.VMEM((8, cols), F32), pltpu.VMEM((8, cols), F32),
            pltpu.VMEM((8, depth), F32), pltpu.VMEM((n, 8, depth), F32),
            dma((4,)), dma((4, 2, 3)), dma((BLOCKS, 2, 4)), dma((4, 2)), dma((BLOCKS, 3)), dma((BLOCKS, 4)),
            dma((BLOCKS,)), dma((2,)), dma((2,)), dma((2,)), dma((2,)), dma((3,)), dma((3,)),
            dma((4,)), dma((5,)), pltpu.SemaphoreType.REGULAR,
            dma, dma, dma, dma, dma, dma((2,)), dma, dma,
            dma((depth // nc,)), dma((2,)), dma((depth // nc,)),
        ],
        compiler_params=pltpu.CompilerParams(collective_id=0, has_side_effects=True, vmem_limit_bytes=67043328),
        name='stream',
    )(hidden, w_two, gain, bias, embed, code)


def dense_kernel(part_ref, dzt_ref, xall_ref, aall_ref, gall_ref, da_ref, go_ref, w_ref, loss_hbm, sum_hbm, dgb_hbm,
                 de_ref, dw_ref, dh_ref, tl_ref, total_ref, gs_ref, gb_ref,
                 da_v, go_v, w_v, g_v, x_v, h_v, dw_v, dz_v, de_v, st_v, w_sem, g_sem, x_sem, h_sem, dw_sem, dz_sem, de_sem, in_sem, out_sem, a_sem, loss_ref, sum_ref, dgb_ref, s_sem):
    depth = x_v.shape[1]
    nc, wb = depth // 4, depth // BLOCKS
    re = dzt_ref.shape[0] // BLOCKS
    xr = x_v.shape[0] // BLOCKS
    todo = BLOCKS - KEEP
    pieces = BLOCKS + 8 * todo
    pr = KEEP * re // pieces

    def at(i, size):
        return pl.ds(pl.multiple_of(i * size, size), size)

    def w_copy(i):
        return pltpu.make_async_copy(w_ref.at[at(i, nc)], w_v.at[at(i, nc)], w_sem.at[i])

    def h_copy(i):
        return pltpu.make_async_copy(aall_ref.at[:, 0:h_v.shape[2], at(i, wb)], h_v.at[i % 2], h_sem.at[i % 2])

    def dw_copy(i):
        return pltpu.make_async_copy(dw_v.at[i % 2], dw_ref.at[at(i, wb)], dw_sem.at[i % 2])

    def x_copy(i):
        return pltpu.make_async_copy(xall_ref.at[at(i, xr)], x_v.at[at(i, xr)], x_sem.at[i])

    def dz_copy(c):
        return pltpu.make_async_copy(dzt_ref.at[at(KEEP + c, re)], dz_v.at[c % 2], dz_sem.at[c % 2])

    def de_copy(u):
        return pltpu.make_async_copy(de_v.at[u % 2], de_ref.at[at(KEEP + u // 4, re), at(u % 4, nc)], de_sem.at[u % 2])

    def pin(t):
        return pltpu.make_async_copy(part_ref.at[at(t, pr)], st_v.at[t % 6], in_sem.at[t % 6])

    def pout(t):
        return pltpu.make_async_copy(st_v.at[t % 6], de_ref.at[at(t, pr)], out_sem.at[t % 6])

    def carry(t):
        pin(t).wait()
        pout(t).start()

        @pl.when(t >= 2)
        def _():
            pout(t - 2).wait()

        @pl.when(t + 4 < pieces)
        def _():
            pin(t + 4).start()

    g_load = pltpu.make_async_copy(gall_ref, g_v, g_sem)
    da_load = pltpu.make_async_copy(da_ref, da_v, a_sem.at[0])
    go_load = pltpu.make_async_copy(go_ref, go_v, a_sem.at[1])
    go_load.start()
    w_copy(0).start()
    small = [pltpu.make_async_copy(a, b, s_sem.at[i]) for i, (a, b) in
             enumerate(((loss_hbm, loss_ref), (sum_hbm, sum_ref), (dgb_hbm, dgb_ref)))]
    for c in small:
        c.start()
    da_load.start()
    for i in range(1, 4):
        w_copy(i).start()
    g_load.start()
    h_copy(0).start()
    h_copy(1).start()
    for t in range(4):
        pin(t).start()

    go_load.wait()
    da_load.wait()

    def hidden_part(i, _):
        w_copy(i).wait()
        sl = at(i, nc)
        back = lax.dot_general(go_v[...], w_v[sl, :], (((1,), (1,)), ((), ())), preferred_element_type=F32)
        dh_ref[:, sl] = (da_v[:, sl] + back).astype(BF16)
        return 0
    with jax.named_scope('k2_dh'):
        lax.fori_loop(0, 4, hidden_part, 0)
    for c in small:
        c.wait()
    gs_ref[...] = dgb_ref[0:2, :]
    gb_ref[...] = dgb_ref[2:4, :]
    total_ref[0] = sum_ref[0, 0]
    me = lax.axis_index('tp')
    lanes = loss_ref.shape[1]
    q = lanes // 2 // (2 * CHIPS)
    place = (me % 2) * CHIPS + me // 2
    for h in range(2):
        turned = pltpu.roll(loss_ref[...], (lanes - h * (lanes // 2) - place * q) % lanes, 1)
        tl_ref[h:h + 1, :] = jnp.concatenate([turned[b:b + 1, :q] for b in range(BLOCKS)], axis=1)
    with jax.named_scope('k2_g'):
        g_load.wait()

    def dw_part(i, _):
        h_copy(i).wait()
        @pl.when(i % 2 == 1)
        def _():
            carry(i // 2)

        @pl.when(i < BLOCKS // 2)
        def _():
            x_copy(2 * i).start()
            x_copy(2 * i + 1).start()

        @pl.when(i == BLOCKS // 2)
        def _():
            dz_copy(0).start()

        @pl.when(i == BLOCKS // 2 + 2)
        def _():
            dz_copy(1).start()
        @pl.when(i >= 2)
        def _():
            dw_copy(i - 2).wait()
        h = h_v[i % 2].reshape(g_v.shape[0], wb)
        dw_v[i % 2] = lax.dot_general(h, g_v[...], (((0,), (0,)), ((), ())), preferred_element_type=F32)
        dw_copy(i).start()

        @pl.when(i + 2 < BLOCKS)
        def _():
            h_copy(i + 2).start()
        return 0
    with jax.named_scope('k2_dw'):
        lax.fori_loop(0, BLOCKS, dw_part, 0)
    with jax.named_scope('k2_x'):
        for i in range(BLOCKS):
            x_copy(i).wait()

    def de_part(u, _):
        c = u // 4

        @pl.when(u % 4 == 0)
        def _():
            dz_copy(c).wait()
        t = BLOCKS // 2 + 2 * u + jnp.minimum(u, BLOCKS // 2)
        carry(t)

        @pl.when(u >= 2)
        def _():
            de_copy(u - 2).wait()
        de_v[u % 2] = jnp.dot(dz_v[c % 2], x_v[:, at(u % 4, nc)], preferred_element_type=F32)
        de_copy(u).start()
        carry(t + 1)

        @pl.when(u < BLOCKS // 2)
        def _():
            carry(t + 2)

        @pl.when(jnp.logical_and(u % 4 == 3, c + 2 < todo))
        def _():
            dz_copy(c + 2).start()
        return 0
    with jax.named_scope('k2_de'):
        lax.fori_loop(0, 4 * todo, de_part, 0)
    for i in (BLOCKS - 2, BLOCKS - 1):
        dw_copy(i).wait()
    for i in (4 * todo - 2, 4 * todo - 1):
        de_copy(i).wait()
    for t in (pieces - 2, pieces - 1):
        pout(t).wait()


def dense(part, dzt, xall, aall, gall, da1, dgown, w_two, loss, total_loss, dgb):
    rows, kk = dzt.shape
    depth = xall.shape[1]
    total, tokens = gall.shape[0], da1.shape[0]
    re, wb, nc = rows // BLOCKS, depth // BLOCKS, depth // 4
    pieces = BLOCKS + 8 * (BLOCKS - KEEP)
    sds = jax.ShapeDtypeStruct
    dma = pltpu.SemaphoreType.DMA
    any_spec = pl.BlockSpec(memory_space=pl.ANY)
    vmem = pl.BlockSpec(memory_space=pltpu.VMEM)
    return pl.pallas_call(
        dense_kernel,
        out_shape=(sds((rows, depth), F32), sds((depth, depth), F32), sds((tokens, depth), BF16), sds((2, tokens), F32),
                   sds((1,), F32), sds((2, depth), F32), sds((2, depth), F32)),
        in_specs=[any_spec] * 11,
        out_specs=(any_spec, any_spec, vmem, vmem, pl.BlockSpec(memory_space=pltpu.SMEM), vmem, vmem),
        scratch_shapes=[pltpu.VMEM((tokens, depth), F32), pltpu.VMEM((tokens, depth), BF16), pltpu.VMEM((depth, depth), BF16), pltpu.VMEM((total, depth), BF16), pltpu.VMEM((kk, depth), BF16),
                        pltpu.VMEM((2, BLOCKS, total // BLOCKS, wb), BF16), pltpu.VMEM((2, wb, depth), F32),
                        pltpu.VMEM((2, re, kk), BF16), pltpu.VMEM((2, re, nc), F32),
                        pltpu.VMEM((6, KEEP * re // pieces, depth), F32),
                        dma((4,)), dma, dma((BLOCKS,)), dma((2,)), dma((2,)), dma((2,)), dma((2,)), dma((6,)), dma((6,)), dma((2,)), pltpu.VMEM(loss.shape, F32), pltpu.VMEM(total_loss.shape, F32),
                        pltpu.VMEM(dgb.shape, F32), dma((3,))],
        compiler_params=pltpu.CompilerParams(vmem_limit_bytes=67043328),
        name='dense',
    )(part, dzt, xall, aall, gall, da1, dgown, w_two, loss, total_loss, dgb)


def solution(mesh):
    n = mesh.shape['tp']
    tok_spec = P(('dp', 'tp'), None)
    row_spec = P(None, ('dp', 'tp'))

    def device_step(hidden, w_two, ln_scale, ln_shift, embed, targets, loss_mask):
        tokens, depth = hidden.shape
        q = tokens // BLOCKS
        me = lax.axis_index('tp')
        code = (targets + 65536 * loss_mask).reshape(2, BLOCKS, q).transpose(1, 0, 2)
        place = (me % 2) * CHIPS + me // 2
        seat = lax.broadcasted_iota(jnp.int32, (1, 1, 2 * CHIPS, 1), 2) == place
        code = jnp.where(seat, code[:, :, None, :], 0).reshape(BLOCKS, 2 * 2 * CHIPS * q)
        aall, xall, dzt, dgall, da1, dgown, loss, total, dgb, part = stream(
            n, hidden, w_two, ln_scale, ln_shift, embed, code)
        d_embed, d_w, d_hidden, token_loss, total_loss, d_scale, d_shift = dense(
            part, dzt, xall, aall.reshape(BLOCKS, 2 * n * q, depth), dgall.reshape(n * tokens, depth),
            da1.reshape(tokens, depth), dgown.reshape(tokens, depth), w_two, loss, total, dgb)
        return token_loss, total_loss, d_hidden, d_embed, d_w, d_scale, d_shift

    return jax.shard_map(device_step, mesh=mesh,
                         in_specs=(tok_spec, P(), P(), P(), P('tp', None), row_spec, row_spec),
                         out_specs=(row_spec, P('dp'), tok_spec, tok_spec, P('dp', None), P('dp', None), P('dp', None)),
                         check_vma=False)
```

```python
import functools

import jax
import jax.numpy as jnp
from jax import lax
from jax.experimental import pallas as pl
from jax.experimental.pallas import tpu as pltpu
from jax.sharding import PartitionSpec as P

LN_EPS = 1e-5
CHIPS = 4
BLOCKS = 8
KEEP = 6
WAYS = 4
LANES = 2
F32 = jnp.float32
BF16 = jnp.bfloat16


def to(idx):
    return dict(device_id={'tp': idx}, device_id_type=pl.DeviceIdType.MESH)


def remote(src, dst, send, recv, idx):
    return pltpu.make_async_remote_copy(src_ref=src, dst_ref=dst, send_sem=send, recv_sem=recv, **to(idx))


def stream_kernel(dims, h_ref, w_ref, gain_ref, bias_ref, e_ref, code_ref,
                  aall_ref, xall_ref, dzt_ref, dgall_ref, da1_ref, dgown_ref, loss_ref, total_ref, dgb_ref, de_ref,
                  e_v, a_v, x_v, z_v, dz_v, dx_v, pr_v, mg_v, ow_v, own_v, dg_v, da_v,
                  stsrc_v, strcv_v, crcv_v, tgt_v, msk_v, wgt_v, ms_v, row_v, tot_v, gsrc_v, grcv_v,
                  ld_sem, h_send, h_recv, h_loc, g_send, g_recv, g_loc,
                  st_send, st_recv, pr_send, pr_recv, r2_send, r3_send, mg_recv, ow_recv, pair_free,
                  cd_send, cd_recv, x_sem, dz_sem, a_sem, out_sem, gb_send, gb_recv, xin_sem, dzin_sem, de_sem):
    n, q, depth, rows, rc, nc, sub = dims
    re = rows // BLOCKS
    half = CHIPS * q
    tok = 2 * half
    cols = 2 * tok
    me = lax.axis_index('tp')
    chip = me // 2
    core = me % 2
    peer = me + 1 - 2 * core
    right_chip = (chip + 1) % CHIPS
    left_chip = (chip + CHIPS - 1) % CHIPS
    far_chip = (chip + 2) % CHIPS
    right = right_chip * 2 + core
    left = left_chip * 2 + core

    top, bottom = pl.ds(0, depth), pl.ds(depth, rows - depth)
    ld_e = [pltpu.make_async_copy(e_ref.at[d], e_v.at[d], ld_sem.at[i]) for i, d in ((0, top), (3, bottom))]
    ld_w = pltpu.make_async_copy(w_ref, e_v.at[bottom], ld_sem.at[1])
    ld_h = pltpu.make_async_copy(h_ref, own_v.at[0], ld_sem.at[2])
    ld_h.start()
    ld_w.start()

    barrier = pltpu.get_barrier_semaphore()
    for r in range(1, n):
        pl.semaphore_signal(barrier, inc=1, **to((me + r) % n))
    pl.semaphore_wait(barrier, n - 1)

    def wait_bytes(ref, sem):
        pltpu.make_async_copy(ref, ref, sem).wait()

    def code_copy(r):
        return remote(code_ref, crcv_v.at[r], cd_send, cd_recv, (me + r) % n)

    for r in range(1, n):
        code_copy(r).start()

    lo, hi = pl.ds(0, q // 2), pl.ds(q // 2, q // 2)

    def g1_copies(src, dst, send, recv):
        piece = dst.at[core, chip]
        return (remote(src, piece, send.at[0], recv.at[0], right),
                remote(src, piece, send.at[0], recv.at[1], left),
                remote(src, piece, send.at[0], recv.at[3], peer))

    def g2_copies(dst, send, recv):
        fl, fr = dst.at[core, left_chip], dst.at[core, right_chip]
        return (remote(fl.at[lo], fl.at[lo], send.at[1], recv.at[2], right),
                remote(fr.at[hi], fr.at[hi], send.at[1], recv.at[2], left),
                remote(fl, fl, send.at[1], recv.at[3], peer),
                remote(fr, fr, send.at[1], recv.at[3], peer))

    def gather1(src, dst, send, recv, loc):
        for c in g1_copies(src, dst, send, recv):
            c.start()
        pltpu.make_async_copy(src, dst.at[core, chip], loc).start()

    def gather2(src, dst, send, recv, loc):
        wait_bytes(dst.at[core, left_chip], recv.at[0])
        wait_bytes(dst.at[core, right_chip], recv.at[1])
        for c in g2_copies(dst, send, recv):
            c.start()
        wait_bytes(dst.at[core, pl.ds(0, 3)], send.at[0])
        pltpu.make_async_copy(src, dst.at[core, chip], loc).wait()

    def gather3(dst, send, recv):
        far = dst.at[core, far_chip]
        wait_bytes(far, recv.at[2])
        remote(far, far, send.at[2], recv.at[3], peer).start()
        wait_bytes(dst.at[core, pl.ds(0, 3)], send.at[1])

    def gather4(dst, send, recv):
        wait_bytes(dst.at[1 - core], recv.at[3])
        wait_bytes(dst.at[core, far_chip], send.at[2])

    def own(b, h):
        return own_v.at[h, pl.ds(pl.multiple_of(b * q, q), q)]

    def in1(b, h):
        gather1(own(b, h), aall_ref.at[b, h], h_send.at[b % 4, h], h_recv.at[b, h], h_loc.at[b % 4, h])

    def in2(b, h):
        gather2(own(b, h), aall_ref.at[b, h], h_send.at[b % 4, h], h_recv.at[b, h], h_loc.at[b % 4, h])

    def in3(b, h):
        gather3(aall_ref.at[b, h], h_send.at[b % 4, h], h_recv.at[b, h])

    def dg1(b):
        gather1(dg_v.at[b % 4], dgall_ref.at[b], g_send.at[b], g_recv.at[b], g_loc.at[b])

    def dg2(b):
        gather2(dg_v.at[b % 4], dgall_ref.at[b], g_send.at[b], g_recv.at[b], g_loc.at[b])

    def dg3(b):
        gather3(dgall_ref.at[b], g_send.at[b], g_recv.at[b])

    def span(fn, lo, hi):
        def body(u, _):
            fn(u // 2, u % 2)
            return 0
        lax.fori_loop(2 * lo, 2 * hi, body, 0)

    def a_copy(b, h, kk, c):
        at = pl.ds(((h * 2 + kk) * CHIPS + c) * q, q)
        return pltpu.make_async_copy(aall_ref.at[b, h, kk, c], a_v.at[at], a_sem)

    def block_copies(b):
        return [a_copy(b, h, kk, c) for h in range(2) for kk in range(2) for c in range(CHIPS)]

    def fetch_block(b):
        for h in range(2):
            gather4(aall_ref.at[b, h], h_send.at[b % 4, h], h_recv.at[b, h])
        for c in block_copies(b):
            c.start()

    def project(src, dst):
        def proj(i, _):
            sl = pl.ds(pl.multiple_of(i * nc, nc), nc)
            dst[:, sl] = jnp.dot(src[...], e_v[bottom, sl], preferred_element_type=F32).astype(BF16)
            return 0
        lax.fori_loop(0, depth // nc, proj, 0)

    def norm_rows(start, head):
        a = a_v[pl.ds(start, 16), :].astype(F32)
        mean = jnp.mean(a, axis=-1, keepdims=True)
        cent = a - mean
        var = jnp.mean(cent * cent, axis=-1, keepdims=True)
        y = cent * lax.rsqrt(var + LN_EPS) * gain_ref[pl.ds(head, 1), :] + bias_ref[pl.ds(head, 1), :]
        x_v[pl.ds(start, 16), :] = y.astype(BF16)

    npart = depth // nc
    lrows = cols // npart

    def norm_part(i):
        head = (i * lrows) // tok
        for s in range(lrows // 16):
            norm_rows(pl.multiple_of(i * lrows + s * 16, 16), head)

    def dx_part(i, slot):
        sl = pl.ds(pl.multiple_of(i * nc, nc), nc)
        val = lax.dot_general(dz_v[...], e_v[:, sl], (((0,), (0,)), ((), ())), preferred_element_type=F32)
        for h in range(2):
            for kk in range(2):
                base = h * tok + kk * half
                dx_v[slot, kk, h, :, sl] = val[base:base + half, :]

    nr = rows // rc

    def tree(parts, op):
        while len(parts) > 1:
            parts = [op(a, b) for a, b in zip(parts[::2], parts[1::2])]
        return parts[0]

    def part_view(ref, i):
        return ref.at[pl.ds(pl.multiple_of(i * rc, rc), rc)]

    def back_part(i, p, lanes, td):
        shift, w = row_v[0:1, lanes], row_v[1:2, lanes]
        zc, dc = part_view(z_v, i), part_view(dz_v, i)
        for s in range(p * sub, p * sub + sub, 16):
            both = []
            for t in (s, s + 8):
                pw = jnp.exp(zc[t:t + 8, lanes] - shift)
                both.append(jnp.where(td == t, pw - w, pw))
            dc[s:s + 16, lanes] = jnp.concatenate(both, axis=0).astype(BF16)

    def z_part(i, p):
        ec = part_view(e_v, i)
        part_view(z_v, i)[p * sub:p * sub + sub, :] = lax.dot_general(
            ec[p * sub:p * sub + sub, :], x_v[...], (((1,), (1,)), ((), ())), preferred_element_type=F32)

    def stat_part(i, p, lanes, td, state):
        zc = part_view(z_v, i)
        m_old, acc, tl = state
        at = range(p * sub, p * sub + sub, 8)
        tops = [zc[s:s + 8, lanes] for s in at[:WAYS]]
        for k, s in enumerate(at[WAYS:]):
            tops[k % WAYS] = jnp.maximum(tops[k % WAYS], zc[s:s + 8, lanes])
        m = jnp.maximum(m_old, tree(tops, jnp.maximum))
        accs = [None] * WAYS
        for k, s in enumerate(at):
            z = zc[s:s + 8, lanes]
            e = jnp.exp(z - m)
            accs[k % WAYS] = e if accs[k % WAYS] is None else accs[k % WAYS] + e
            tl = jnp.where(td == s, z, tl)
        return m, acc * jnp.exp(m_old - m) + tree(accs, jnp.add), tl

    def d_body(i, back, new):
        span = cols // LANES
        iota = lax.broadcasted_iota(jnp.int32, (8, span), 0)
        cut = [slice(k * span, k * span + span) for k in range(LANES)]
        td_old = [tgt_v[pl.ds(8, 1), c] - i * rc - iota for c in cut]
        td_new = [tgt_v[pl.ds(9, 1), c] - i * rc - iota for c in cut]
        state = [tuple(ms_v[k, :, c] for k in range(3)) for c in cut]
        for p in range(rc // sub):
            if back:
                for k in range(LANES):
                    back_part(i, p, cut[k], td_old[k])
            if new:
                z_part(i, p)
                for k in range(LANES):
                    state[k] = stat_part(i, p, cut[k], td_new[k], state[k])
        if new:
            for k in range(LANES):
                for q_ in range(3):
                    ms_v[q_, :, cut[k]] = state[k][q_]

    def stat_copy(slot, r):
        return remote(stsrc_v.at[slot], strcv_v.at[slot, r], st_send.at[slot], st_recv.at[slot], (me + r) % n)

    def send_stats(b):
        slot = b % 2
        m = ms_v[0]
        top = jnp.max(m, axis=0, keepdims=True)
        stsrc_v[slot, 0:1, :] = top
        stsrc_v[slot, 1:2, :] = jnp.sum(ms_v[1] * jnp.exp(m - top), axis=0, keepdims=True)
        stsrc_v[slot, 2:3, :] = jnp.sum(ms_v[2], axis=0, keepdims=True)
        for r in range(1, n):
            stat_copy(slot, r).start()

    def join_stats(b):
        slot = b % 2
        wait_bytes(strcv_v.at[slot, pl.ds(1, n - 1)], st_send.at[slot])
        wait_bytes(strcv_v.at[slot, pl.ds(1, n - 1)], st_recv.at[slot])
        parts = [stsrc_v[slot]] + [strcv_v[slot, r] for r in range(1, n)]
        top = parts[0][0:1]
        for p in parts[1:]:
            top = jnp.maximum(top, p[0:1])
        total = jnp.zeros_like(top)
        hit = jnp.zeros_like(top)
        for p in parts:
            total = total + p[1:2] * jnp.exp(p[0:1] - top)
            hit = hit + p[2:3]
        lse = top + jnp.log(total)
        w = wgt_v[pl.ds(b, 1), :]
        row_v[0:1, :] = jnp.where(w > 0.0, lse - jnp.log(jnp.where(w > 0.0, w, 1.0)), 3.0e38)
        row_v[1:2, :] = w
        tgt_v[pl.ds(8, 1), :] = tgt_v[pl.ds(b, 1), :]
        loss = (lse - hit) * msk_v[pl.ds(b, 1), :]
        loss_ref[pl.ds(b, 1), :] = loss
        tot_v[0:1, :] = tot_v[0:1, :] + loss / tot_v[1:2, :]

    def pair_copy(b):
        slot = b % 2
        return remote(dx_v.at[b % 3, 1 - core], pr_v.at[slot], pr_send.at[slot], pr_recv.at[slot], peer)

    def rs1(b):
        @pl.when(b >= 2)
        def _():
            pl.semaphore_wait(pair_free, 1)
        pair_copy(b).start()

    def crow(c):
        return pl.ds(pl.multiple_of(c * q, q), q)

    def r2_copies(b):
        mine, s3, mg, ow = dx_v.at[b % 3, core], b % 3, b % 4, b % 5
        return (remote(mine.at[0, crow(far_chip)], mg_v.at[mg, 0], r2_send.at[s3], mg_recv.at[mg], right),
                remote(mine.at[1, crow(far_chip)], mg_v.at[mg, 1], r2_send.at[s3], mg_recv.at[mg], left),
                remote(mine.at[1, crow(right_chip)], ow_v.at[ow, 0, 1], r2_send.at[s3], ow_recv.at[ow], right),
                remote(mine.at[0, crow(left_chip)], ow_v.at[ow, 1, 0], r2_send.at[s3], ow_recv.at[ow], left))

    def rs2(b):
        slot, s3 = b % 2, b % 3
        pair_copy(b).wait()

        def add(i, _):
            h = i // CHIPS
            c = i % CHIPS
            dx_v[s3, core, h, crow(c), :] += pr_v[slot, h, crow(c), :]
            return 0
        lax.fori_loop(0, 2 * CHIPS, add, 0)

        @pl.when(b < BLOCKS - 2)
        def _():
            pl.semaphore_signal(pair_free, inc=1, **to(peer))
        for c in r2_copies(b)[:2]:
            c.start()

    def rs2_direct(b):
        for c in r2_copies(b)[2:]:
            c.start()

    def r3_copies(b):
        mine, s3, ow = dx_v.at[b % 3, core], b % 3, b % 5
        return (remote(mine.at[0, crow(right_chip)], ow_v.at[ow, 0, 0], r3_send.at[s3], ow_recv.at[ow], right),
                remote(mine.at[1, crow(left_chip)], ow_v.at[ow, 1, 1], r3_send.at[s3], ow_recv.at[ow], left))

    def rs3(b):
        s3, mg = b % 3, b % 4
        wait_bytes(mg_v.at[mg], mg_recv.at[mg])
        dx_v[s3, core, 0, crow(right_chip), :] += mg_v[mg, 0]
        dx_v[s3, core, 1, crow(left_chip), :] += mg_v[mg, 1]
        for c in r3_copies(b):
            c.start()

    def rs4(b):
        ow = b % 5
        wait_bytes(ow_v.at[ow], ow_recv.at[ow])

        @pl.when(b >= 1)
        def _():
            out_copies(b - 1)[0].wait()
            out_copies(b - 1)[1].wait()
        for h in range(2):
            dy = dx_v[b % 3, core, h, crow(chip), :] + ow_v[ow, 0, h] + ow_v[ow, 1, h]
            a = own(b, h)[...].astype(F32)
            mean = jnp.mean(a, axis=-1, keepdims=True)
            cent = a - mean
            rstd = lax.rsqrt(jnp.mean(cent * cent, axis=-1, keepdims=True) + LN_EPS)
            xhat = cent * rstd
            gsrc_v[h:h + 1, :] += jnp.sum(dy * xhat, axis=0, keepdims=True)
            gsrc_v[2 + h:3 + h, :] += jnp.sum(dy, axis=0, keepdims=True)
            dxh = dy * gain_ref[h:h + 1, :]
            c1 = jnp.mean(dxh, axis=-1, keepdims=True)
            c2_ = jnp.mean(dxh * xhat, axis=-1, keepdims=True)
            da = rstd * (dxh - c1 - xhat * c2_)
            if h == 0:
                da_v[...] = da
            else:
                dg_v[b % 4] = da.astype(BF16)
        for c in out_copies(b):
            c.start()
        wait_bytes(ow_v.at[ow], r2_send.at[b % 3])
        wait_bytes(mg_v.at[b % 4], r3_send.at[b % 3])

    def out_copies(b):
        return (pltpu.make_async_copy(da_v, da1_ref.at[b], out_sem.at[0]),
                pltpu.make_async_copy(dg_v.at[b % 4], dgown_ref.at[b], out_sem.at[1]))

    def xin_copy(i):
        sl = pl.ds(pl.multiple_of(i * nc, nc), nc)
        return pltpu.make_async_copy(xall_ref.at[:, sl], e_v.at[:, sl], xin_sem.at[i])

    def dzin_copies(c, odd):
        at = pl.ds(pl.multiple_of(c * re, re), re)
        if odd:
            return [pltpu.make_async_copy(dzt_ref.at[at, pl.ds(k * cols, cols)], dz_v.at[pl.ds(k * re, re)], dzin_sem.at[1])
                    for k in range(BLOCKS)]
        return [pltpu.make_async_copy(dzt_ref.at[at, pl.ds(k * depth, depth)], (a_v, x_v)[k], dzin_sem.at[0])
                for k in range(2)]

    def de_copy(c, i):
        return pltpu.make_async_copy(
            z_v.at[pl.ds(pl.multiple_of(i * re, re), re)],
            de_ref.at[pl.ds(pl.multiple_of(c * re, re), re), pl.ds(pl.multiple_of(i * nc, nc), nc)], de_sem.at[i])

    def de_chunk(c, odd, extra=None):
        if odd:
            wait_bytes(dz_v, dzin_sem.at[1])
        else:
            wait_bytes(e_v.at[pl.ds(0, 2 * re)], dzin_sem.at[0])

        def part(i, _):
            sl = pl.ds(pl.multiple_of(i * nc, nc), nc)

            @pl.when(c == 0)
            def _():
                xin_copy(i).wait()

            @pl.when(c >= 1)
            def _():
                de_copy(c - 1, i).wait()
            if odd:
                val = jnp.dot(dz_v[:re, :], e_v[:cols, sl], preferred_element_type=F32)
                for k in range(1, BLOCKS):
                    val = val + jnp.dot(dz_v[k * re:k * re + re, :], e_v[k * cols:k * cols + cols, sl], preferred_element_type=F32)
            else:
                val = jnp.dot(a_v[...], e_v[:depth, sl], preferred_element_type=F32)
                val = val + jnp.dot(x_v[...], e_v[depth:, sl], preferred_element_type=F32)
            z_v[pl.ds(pl.multiple_of(i * re, re), re), :] = val
            de_copy(c, i).start()
            if extra is not None:
                @pl.when(jnp.logical_and(c == KEEP - 1, i == npart - 2))
                def _():
                    extra()
            return 0
        lax.fori_loop(0, npart, part, 0)

        @pl.when(c + 2 < KEEP)
        def _():
            for d in dzin_copies(c + 2, odd):
                d.start()

    def inside(b, fn, name='svc'):
        @pl.when(jnp.logical_and(b >= 0, b < BLOCKS))
        def _():
            with jax.named_scope(name):
                fn(b)

    def between(j, lo, hi, fn, name='svc'):
        @pl.when(jnp.logical_and(j >= lo, j <= hi))
        def _():
            with jax.named_scope(name):
                fn()

    def x_copy(b):
        return pltpu.make_async_copy(x_v, xall_ref.at[pl.ds(pl.multiple_of(b * cols, cols), cols)], x_sem)

    def dz_copy(b):
        return pltpu.make_async_copy(dz_v, dzt_ref.at[:, pl.ds(pl.multiple_of(b * cols, cols), cols)], dz_sem)

    def loop(k, fn):
        def body(i, _):
            fn(i)
            return 0
        lax.fori_loop(0, k, body, 0)

    with jax.named_scope('p_h'):
        ld_h.wait()
    in1(0, 0)
    in1(1, 0)
    with jax.named_scope('p_w'):
        ld_w.wait()
    ld_e[0].start()
    with jax.named_scope('p_proj'):
        project(own_v.at[0], own_v.at[1])
    with jax.named_scope('p_in2'):
        in2(0, 0)
    in1(1, 1)
    span(in1, 2, 3)
    with jax.named_scope('p_code'):
        wait_bytes(crcv_v.at[pl.ds(1, n - 1)], cd_send)
        wait_bytes(crcv_v.at[pl.ds(1, n - 1)], cd_recv)
    code = code_ref[...]
    for r in range(1, n):
        code = code + crcv_v[r]
    mask = (code >= 65536).astype(jnp.int32)
    local = code - mask * 65536 - me * rows
    tgt_v[0:BLOCKS, :] = jnp.where(jnp.logical_and(local >= 0, local < rows), local, -(1 << 24))
    maskf = mask.astype(F32)
    msk_v[...] = maskf
    per_col = jnp.sum(maskf, axis=0, keepdims=True)
    n0 = jnp.sum(per_col[:, :tok], axis=1, keepdims=True)
    n1 = jnp.sum(per_col[:, tok:], axis=1, keepdims=True)
    counts = jnp.concatenate([jnp.broadcast_to(n0, (1, tok)), jnp.broadcast_to(n1, (1, tok))], axis=1)
    wgt_v[...] = maskf / counts
    tot_v[0:1, :] = jnp.zeros((1, cols), F32)
    tot_v[1:2, :] = counts
    gsrc_v[...] = jnp.zeros_like(gsrc_v)
    with jax.named_scope('p_in3'):
        in3(0, 0)
    with jax.named_scope('p_fetch'):
        gather4(aall_ref.at[0, 0], h_send.at[0, 0], h_recv.at[0, 0])
        first = [a_copy(0, 0, kk, c) for kk in range(2) for c in range(CHIPS)]
        for c in first:
            c.start()
        wait_bytes(a_v.at[pl.ds(0, tok)], a_sem)
    with jax.named_scope('p_proj0'):
        project(a_v.at[pl.ds(0, tok)], a_v.at[pl.ds(tok, tok)])
    ld_e[1].start()
    ld_e[0].wait()

    def last_stage(b):
        rs4(b)
        dg1(b)

    def gather_b0():
        span(in2, 1, 2)
        span(in1, 3, 4)

    def gather_d0():
        ld_e[1].wait()
        span(in3, 1, 2)
        span(in2, 2, 3)
        span(in1, 4, 5)

    def gather_e0():
        span(in3, 2, 3)
        span(in2, 3, 4)
        span(in1, 5, 6)

    def gather_e1():
        span(in3, 3, 4)
        span(in2, 4, 6)
        span(in1, 6, 8)

    def gather_b2():
        span(in3, 4, 6)

    def gather_e2():
        span(in2, 6, 8)

    def gather_b3():
        span(in3, 6, 8)

    def step(t, _):
        j = t - 1
        def last_dg3():
            dg3(BLOCKS - 2)
            dg3(BLOCKS - 1)

        def block_wait():
            wait_bytes(a_v, a_sem)
        between(j, 0, BLOCKS - 2, block_wait, 'bwait')
        between(j, 1, BLOCKS, lambda: x_wait(j), 'xwait')

        def full_a():
            def body(i):
                dx_part(i, (j - 1) % 3)
                norm_part(i)
            loop(npart, body)
        between(j, -1, 0, lambda: loop(npart, norm_part), 'norm')
        between(j, 1, BLOCKS - 2, full_a, 'full_a')
        between(j, BLOCKS, BLOCKS, start_tail, 'start_tail')

        def last_a(i):
            dx_part(i, (j - 1) % 3)

            @pl.when(j == BLOCKS)
            def _():
                xin_copy(i).start()
        between(j, BLOCKS - 1, BLOCKS, lambda: loop(npart, last_a), 'last_a')
        between(j, BLOCKS + 1, BLOCKS + 3, lambda: de_chunk(2 * (j - BLOCKS) - 1, True, last_dg3), 'de_a')
        between(j, -1, BLOCKS - 2, lambda: x_copy(j + 1).start(), 'xstart')
        between(j, BLOCKS, BLOCKS, start_odd, 'start_odd')
        inside(j - 1, rs1, 'rs1')
        between(j, -1, -1, gather_b0, 'gb0')
        between(j, 1, 1, gather_b2, 'gb2')
        between(j, 2, 2, gather_b3, 'gb3')
        between(j, 1, BLOCKS - 3, lambda: fetch_block(j + 2), 'fetch')
        between(j, BLOCKS, BLOCKS, lambda: rs3(BLOCKS - 3), 'rs3')
        def late_stages():
            def body(b, _):
                last_stage(b)
                return 0
            lax.fori_loop(j - 4, 2 * j - BLOCKS - 4, body, 0)
        between(j, BLOCKS + 1, BLOCKS + 2, late_stages, 'rs4late')
        inside(j - 2, rs2_direct, 'rs2d')
        inside(j, join_stats, 'join')
        between(j, 1, BLOCKS - 1, lambda: dz_copy(j - 1).wait(), 'dzwait')
        between(j, BLOCKS, BLOCKS + 2, lambda: de_chunk(2 * (j - BLOCKS), False), 'de_d')

        def start_stats():
            ms_v[0] = jnp.full((8, cols), -3.0e38, F32)
            ms_v[1] = jnp.zeros((8, cols), F32)
            ms_v[2] = jnp.zeros((8, cols), F32)
            tgt_v[pl.ds(9, 1), :] = tgt_v[pl.ds(j + 1, 1), :]
        between(j, -1, BLOCKS - 2, start_stats)

        def first_d(i):
            d_body(i, False, True)

            @pl.when(i == 0)
            def _():
                gather_d0()
        between(j, -1, -1, lambda: loop(nr, first_d), 'only_z')
        def mid_d(i):
            d_body(i, True, True)

            @pl.when(i == 0)
            def _():
                between(j, 0, 0, lambda: fetch_block(2), 'fetch')
        between(j, 0, BLOCKS - 2, lambda: loop(nr, mid_d), 'full_d')
        between(j, BLOCKS - 1, BLOCKS - 1, lambda: loop(nr, lambda i: d_body(i, True, False)), 'back')
        between(j, -1, -1, lambda: fetch_block(1), 'fetch')
        between(j, -1, BLOCKS - 2, lambda: send_stats(j + 1), 'stats')
        inside(j, lambda b: dz_copy(b).start(), 'dzstart')
        between(j, 2, BLOCKS - 2, lambda: rs3(j - 2), 'rs3')
        between(j, BLOCKS, BLOCKS + 1, lambda: rs3(j - 2), 'rs3')
        between(j, 3, BLOCKS - 1, lambda: last_stage(j - 3), 'rs4g1')
        between(j, 4, BLOCKS + 2, lambda: dg2(j - 4), 'dg2')
        between(j, -1, -1, gather_e0, 'ge0')
        between(j, 0, 0, gather_e1, 'ge1')
        between(j, 1, 1, gather_e2, 'ge2')
        between(j, 5, BLOCKS + 2, lambda: dg3(j - 5), 'dg3')
        inside(j - 1, rs2, 'rs2')
        between(j, BLOCKS + 2, BLOCKS + 2, lambda: dg2(BLOCKS - 1), 'dg2last')
        between(j, BLOCKS + 2, BLOCKS + 2, gb_start, 'gbstart')
        return 0

    def gb_copy(r):
        return remote(gsrc_v, grcv_v.at[r], gb_send, gb_recv, (me + r) % n)

    def gb_start():
        for r in range(1, n):
            gb_copy(r).start()

    def start_tail():
        dz_copy(BLOCKS - 1).wait()
        for d in dzin_copies(0, False):
            d.start()

    def start_odd():
        for d in dzin_copies(1, True):
            d.start()

    def x_wait(j):
        @pl.when(j <= BLOCKS - 1)
        def _():
            x_copy(j).wait()

    def first_x(j):
        x_copy(j).wait()

    def step_outer(t, c):
        @pl.when(t == 1)
        def _():
            first_x(0)
        return step(t, c)

    lax.fori_loop(0, BLOCKS + 5, step_outer, 0)

    with jax.named_scope('e_g4'):
        for b in range(BLOCKS):
            gather4(dgall_ref.at[b], g_send.at[b], g_recv.at[b])
    with jax.named_scope('e_out'):
        for c in out_copies(BLOCKS - 1):
            c.wait()
    with jax.named_scope('e_de'):
        for i in range(npart):
            de_copy(KEEP - 1, i).wait()
    with jax.named_scope('e_gb'):
        wait_bytes(grcv_v.at[pl.ds(1, n - 1)], gb_send)
        wait_bytes(grcv_v.at[pl.ds(1, n - 1)], gb_recv)
    with jax.named_scope('e_sum'):
        acc = gsrc_v[...]
        for r in range(1, n):
            acc = acc + grcv_v[r]
        dgb_ref[...] = acc
        total_ref[...] = jnp.broadcast_to(jnp.sum(tot_v[0:1, :], axis=1, keepdims=True), total_ref.shape)


def stream(n, hidden, w_two, gain, bias, embed, code):
    tokens, depth = hidden.shape
    rows = embed.shape[0]
    q = tokens // BLOCKS
    half = CHIPS * q
    tok = 2 * half
    cols = 2 * tok
    nc = depth // 4
    rc, sub = rows // 2, rows // 8
    assert BLOCKS * cols == rows == 2 * depth and nc == cols
    dims = (n, q, depth, rows, rc, nc, sub)
    any_spec = pl.BlockSpec(memory_space=pl.ANY)
    vmem = pl.BlockSpec(memory_space=pltpu.VMEM)
    dma = pltpu.SemaphoreType.DMA
    sds = jax.ShapeDtypeStruct
    return pl.pallas_call(
        functools.partial(stream_kernel, dims),
        out_shape=(sds((BLOCKS, 2, 2, CHIPS, q, depth), BF16), sds((BLOCKS * cols, depth), BF16),
                   sds((rows, BLOCKS * cols), BF16), sds((BLOCKS, 2, CHIPS, q, depth), BF16),
                   sds((BLOCKS, q, depth), F32), sds((BLOCKS, q, depth), BF16),
                   sds((BLOCKS, cols), F32), sds((8, 128), F32), sds((8, depth), F32),
                   sds((KEEP * (rows // BLOCKS), depth), F32)),
        in_specs=[any_spec, any_spec, vmem, vmem, any_spec, vmem],
        out_specs=(any_spec,) * 6 + (vmem,) * 3 + (any_spec,),
        scratch_shapes=[
            pltpu.VMEM((rows, depth), BF16),
            pltpu.VMEM((cols, depth), BF16), pltpu.VMEM((cols, depth), BF16),
            pltpu.VMEM((rows, cols), F32), pltpu.VMEM((rows, cols), BF16),
            pltpu.VMEM((3, 2, 2, half, depth), F32), pltpu.VMEM((2, 2, half, depth), F32),
            pltpu.VMEM((4, 2, q, depth), F32), pltpu.VMEM((5, 2, 2, q, depth), F32),
            pltpu.VMEM((2, tokens, depth), BF16),
            pltpu.VMEM((4, q, depth), BF16), pltpu.VMEM((q, depth), F32),
            pltpu.VMEM((2, 8, cols), F32), pltpu.VMEM((2, n, 8, cols), F32),
            pltpu.VMEM((n, BLOCKS, cols), jnp.int32), pltpu.VMEM((16, cols), jnp.int32),
            pltpu.VMEM((BLOCKS, cols), F32), pltpu.VMEM((BLOCKS, cols), F32),
            pltpu.VMEM((3, 8, cols), F32), pltpu.VMEM((8, cols), F32), pltpu.VMEM((8, cols), F32),
            pltpu.VMEM((8, depth), F32), pltpu.VMEM((n, 8, depth), F32),
            dma((4,)), dma((4, 2, 3)), dma((BLOCKS, 2, 4)), dma((4, 2)), dma((BLOCKS, 3)), dma((BLOCKS, 4)),
            dma((BLOCKS,)), dma((2,)), dma((2,)), dma((2,)), dma((2,)), dma((3,)), dma((3,)),
            dma((4,)), dma((5,)), pltpu.SemaphoreType.REGULAR,
            dma, dma, dma, dma, dma, dma((2,)), dma, dma,
            dma((depth // nc,)), dma((2,)), dma((depth // nc,)),
        ],
        compiler_params=pltpu.CompilerParams(collective_id=0, has_side_effects=True, vmem_limit_bytes=67043328),
        name='stream',
    )(hidden, w_two, gain, bias, embed, code)


def dense_kernel(part_ref, dzt_ref, xall_ref, aall_ref, gall_ref, da_ref, go_ref, w_ref, loss_hbm, sum_hbm, dgb_hbm,
                 de_ref, dw_ref, dh_ref, tl_ref, total_ref, gs_ref, gb_ref,
                 da_v, go_v, w_v, g_v, x_v, h_v, dw_v, dz_v, de_v, st_v, w_sem, g_sem, x_sem, h_sem, dw_sem, dz_sem, de_sem, in_sem, out_sem, a_sem, loss_ref, sum_ref, dgb_ref, s_sem):
    depth = x_v.shape[1]
    nc, wb = depth // 4, depth // BLOCKS
    re = dzt_ref.shape[0] // BLOCKS
    xr = x_v.shape[0] // BLOCKS
    todo = BLOCKS - KEEP
    pieces = BLOCKS + 8 * todo
    pr = KEEP * re // pieces

    def at(i, size):
        return pl.ds(pl.multiple_of(i * size, size), size)

    def w_copy(i):
        return pltpu.make_async_copy(w_ref.at[at(i, nc)], w_v.at[at(i, nc)], w_sem.at[i])

    def h_copy(i):
        return pltpu.make_async_copy(aall_ref.at[:, 0:h_v.shape[2], at(i, wb)], h_v.at[i % 2], h_sem.at[i % 2])

    def dw_copy(i):
        return pltpu.make_async_copy(dw_v.at[i % 2], dw_ref.at[at(i, wb)], dw_sem.at[i % 2])

    def x_copy(i):
        return pltpu.make_async_copy(xall_ref.at[at(i, xr)], x_v.at[at(i, xr)], x_sem.at[i])

    def dz_copy(c):
        return pltpu.make_async_copy(dzt_ref.at[at(KEEP + c, re)], dz_v.at[c % 2], dz_sem.at[c % 2])

    def de_copy(u):
        return pltpu.make_async_copy(de_v.at[u % 2], de_ref.at[at(KEEP + u // 4, re), at(u % 4, nc)], de_sem.at[u % 2])

    def pin(t):
        return pltpu.make_async_copy(part_ref.at[at(t, pr)], st_v.at[t % 4], in_sem.at[t % 4])

    def pout(t):
        return pltpu.make_async_copy(st_v.at[t % 4], de_ref.at[at(t, pr)], out_sem.at[t % 4])

    def carry(t):
        pin(t).wait()
        pout(t).start()

        @pl.when(t >= 2)
        def _():
            pout(t - 2).wait()

        @pl.when(t + 2 < pieces)
        def _():
            pin(t + 2).start()

    g_load = pltpu.make_async_copy(gall_ref, g_v, g_sem)
    da_load = pltpu.make_async_copy(da_ref, da_v, a_sem.at[0])
    go_load = pltpu.make_async_copy(go_ref, go_v, a_sem.at[1])
    go_load.start()
    w_copy(0).start()
    small = [pltpu.make_async_copy(a, b, s_sem.at[i]) for i, (a, b) in
             enumerate(((loss_hbm, loss_ref), (sum_hbm, sum_ref), (dgb_hbm, dgb_ref)))]
    for c in small:
        c.start()
    da_load.start()
    for i in range(1, 4):
        w_copy(i).start()
    g_load.start()
    h_copy(0).start()
    h_copy(1).start()
    pin(0).start()
    pin(1).start()

    go_load.wait()
    da_load.wait()

    def hidden_part(i, _):
        w_copy(i).wait()
        sl = at(i, nc)
        back = lax.dot_general(go_v[...], w_v[sl, :], (((1,), (1,)), ((), ())), preferred_element_type=F32)
        dh_ref[:, sl] = (da_v[:, sl] + back).astype(BF16)
        return 0
    with jax.named_scope('k2_dh'):
        lax.fori_loop(0, 4, hidden_part, 0)
    for c in small:
        c.wait()
    gs_ref[...] = dgb_ref[0:2, :]
    gb_ref[...] = dgb_ref[2:4, :]
    total_ref[0] = sum_ref[0, 0]
    me = lax.axis_index('tp')
    lanes = loss_ref.shape[1]
    q = lanes // 2 // (2 * CHIPS)
    place = (me % 2) * CHIPS + me // 2
    for h in range(2):
        turned = pltpu.roll(loss_ref[...], (lanes - h * (lanes // 2) - place * q) % lanes, 1)
        tl_ref[h:h + 1, :] = jnp.concatenate([turned[b:b + 1, :q] for b in range(BLOCKS)], axis=1)
    with jax.named_scope('k2_g'):
        g_load.wait()

    def dw_part(i, _):
        h_copy(i).wait()
        carry(i)

        @pl.when(i < BLOCKS // 2)
        def _():
            x_copy(2 * i).start()
            x_copy(2 * i + 1).start()

        @pl.when(i == BLOCKS // 2)
        def _():
            dz_copy(0).start()

        @pl.when(i == BLOCKS // 2 + 2)
        def _():
            dz_copy(1).start()
        @pl.when(i >= 2)
        def _():
            dw_copy(i - 2).wait()
        h = h_v[i % 2].reshape(g_v.shape[0], wb)
        dw_v[i % 2] = lax.dot_general(h, g_v[...], (((0,), (0,)), ((), ())), preferred_element_type=F32)
        dw_copy(i).start()

        @pl.when(i + 2 < BLOCKS)
        def _():
            h_copy(i + 2).start()
        return 0
    with jax.named_scope('k2_dw'):
        lax.fori_loop(0, BLOCKS, dw_part, 0)
    with jax.named_scope('k2_x'):
        for i in range(BLOCKS):
            x_copy(i).wait()

    def de_part(u, _):
        c = u // 4

        @pl.when(u % 4 == 0)
        def _():
            dz_copy(c).wait()
        carry(BLOCKS + 2 * u)

        @pl.when(u >= 2)
        def _():
            de_copy(u - 2).wait()
        de_v[u % 2] = jnp.dot(dz_v[c % 2], x_v[:, at(u % 4, nc)], preferred_element_type=F32)
        de_copy(u).start()
        carry(BLOCKS + 2 * u + 1)

        @pl.when(jnp.logical_and(u % 4 == 3, c + 2 < todo))
        def _():
            dz_copy(c + 2).start()
        return 0
    with jax.named_scope('k2_de'):
        lax.fori_loop(0, 4 * todo, de_part, 0)
    for i in (BLOCKS - 2, BLOCKS - 1):
        dw_copy(i).wait()
    for i in (4 * todo - 2, 4 * todo - 1):
        de_copy(i).wait()
    for t in (pieces - 2, pieces - 1):
        pout(t).wait()


def dense(part, dzt, xall, aall, gall, da1, dgown, w_two, loss, total_loss, dgb):
    rows, kk = dzt.shape
    depth = xall.shape[1]
    total, tokens = gall.shape[0], da1.shape[0]
    re, wb, nc = rows // BLOCKS, depth // BLOCKS, depth // 4
    pieces = BLOCKS + 8 * (BLOCKS - KEEP)
    sds = jax.ShapeDtypeStruct
    dma = pltpu.SemaphoreType.DMA
    any_spec = pl.BlockSpec(memory_space=pl.ANY)
    vmem = pl.BlockSpec(memory_space=pltpu.VMEM)
    return pl.pallas_call(
        dense_kernel,
        out_shape=(sds((rows, depth), F32), sds((depth, depth), F32), sds((tokens, depth), BF16), sds((2, tokens), F32),
                   sds((1,), F32), sds((2, depth), F32), sds((2, depth), F32)),
        in_specs=[any_spec] * 11,
        out_specs=(any_spec, any_spec, vmem, vmem, pl.BlockSpec(memory_space=pltpu.SMEM), vmem, vmem),
        scratch_shapes=[pltpu.VMEM((tokens, depth), F32), pltpu.VMEM((tokens, depth), BF16), pltpu.VMEM((depth, depth), BF16), pltpu.VMEM((total, depth), BF16), pltpu.VMEM((kk, depth), BF16),
                        pltpu.VMEM((2, BLOCKS, total // BLOCKS, wb), BF16), pltpu.VMEM((2, wb, depth), F32),
                        pltpu.VMEM((2, re, kk), BF16), pltpu.VMEM((2, re, nc), F32),
                        pltpu.VMEM((4, KEEP * re // pieces, depth), F32),
                        dma((4,)), dma, dma((BLOCKS,)), dma((2,)), dma((2,)), dma((2,)), dma((2,)), dma((4,)), dma((4,)), dma((2,)), pltpu.VMEM(loss.shape, F32), pltpu.VMEM(total_loss.shape, F32),
                        pltpu.VMEM(dgb.shape, F32), dma((3,))],
        compiler_params=pltpu.CompilerParams(vmem_limit_bytes=67043328),
        name='dense',
    )(part, dzt, xall, aall, gall, da1, dgown, w_two, loss, total_loss, dgb)


def solution(mesh):
    n = mesh.shape['tp']
    tok_spec = P(('dp', 'tp'), None)
    row_spec = P(None, ('dp', 'tp'))

    def device_step(hidden, w_two, ln_scale, ln_shift, embed, targets, loss_mask):
        tokens, depth = hidden.shape
        q = tokens // BLOCKS
        me = lax.axis_index('tp')
        code = (targets + 65536 * loss_mask).reshape(2, BLOCKS, q).transpose(1, 0, 2)
        place = (me % 2) * CHIPS + me // 2
        seat = lax.broadcasted_iota(jnp.int32, (1, 1, 2 * CHIPS, 1), 2) == place
        code = jnp.where(seat, code[:, :, None, :], 0).reshape(BLOCKS, 2 * 2 * CHIPS * q)
        aall, xall, dzt, dgall, da1, dgown, loss, total, dgb, part = stream(
            n, hidden, w_two, ln_scale, ln_shift, embed, code)
        d_embed, d_w, d_hidden, token_loss, total_loss, d_scale, d_shift = dense(
            part, dzt, xall, aall.reshape(BLOCKS, 2 * n * q, depth), dgall.reshape(n * tokens, depth),
            da1.reshape(tokens, depth), dgown.reshape(tokens, depth), w_two, loss, total, dgb)
        return token_loss, total_loss, d_hidden, d_embed, d_w, d_scale, d_shift

    return jax.shard_map(device_step, mesh=mesh,
                         in_specs=(tok_spec, P(), P(), P(), P('tp', None), row_spec, row_spec),
                         out_specs=(row_spec, P('dp'), tok_spec, tok_spec, P('dp', None), P('dp', None), P('dp', None)),
                         check_vma=False)
```
